8 devices in a mesh: col: 4 (over z, y, x), row: 2 (over core).
Axes of the slice: x: 2, y: 2, z: 1, core: 2. Of those that a mesh axis runs over, the one named last changes fastest.
Arguments:
- x_in: bfloat16 [1, 96, 768, 256], P(None, 'row', 'col')
- a_pre: bfloat16 [1, 96, 768, 256], P(None, 'row', 'col')
- g_out: bfloat16 [1, 96, 768, 256], P(None, 'row', 'col')
- w_one: bfloat16 [3, 3, 256, 256], replicated
- w_two: bfloat16 [3, 3, 256, 256], replicated
Outputs:
- output 1: bfloat16 [1, 96, 768, 256], P(None, 'row', 'col')
- output 2: float32 [3, 3, 256, 256], replicated
- output 3: float32 [3, 3, 256, 256], replicated
All inputs are finite; a program needn't handle non-finite values.
Results may differ from the reference program's by a relative error of at most 0.001.
Values are sent between devices in bfloat16 or wider.
A program may use at most 1 GiB of HBM per device.

```python
import jax
import jax.numpy as jnp
from jax import lax

IMAGES = 1
CHANNELS = 256
TILE_ROWS = 48
TILE_COLS = 192
IMG_HEIGHT = 96
IMG_WIDTH = 768

FRAME_PAD = ((0, 0), (1, 1), (1, 1), (0, 0))


def conv_same(image_in, kernel):
    return lax.conv_general_dilated(image_in, kernel, (1, 1), "SAME", dimension_numbers=("NHWC", "HWIO", "NHWC"))


def gelu_slope(pre_act):
    tanh_scale = 0.7978845608028654
    cube_coef = 0.044715
    tanh_val = jnp.tanh(tanh_scale * (pre_act + cube_coef * pre_act * pre_act * pre_act))
    return 0.5 * (1.0 + tanh_val) + 0.5 * pre_act * (1.0 - tanh_val * tanh_val) * tanh_scale * (1.0 + 3.0 * cube_coef * pre_act * pre_act)


def tap_grads(left_pad, right_img):
    row_count = right_img.shape[1]
    col_count = right_img.shape[2]
    return jnp.stack([jnp.stack([jnp.einsum("bhwi,bhwo->io", left_pad[:, tap_row:tap_row + row_count, tap_col:tap_col + col_count], right_img) for tap_col in range(3)]) for tap_row in range(3)])


def edge_weight(boost):
    row_pos = jnp.arange(IMG_HEIGHT) % TILE_ROWS
    col_pos = jnp.arange(IMG_WIDTH) % TILE_COLS
    row_edge = (row_pos == 0) | (row_pos == TILE_ROWS - 1)
    col_edge = (col_pos == 0) | (col_pos == TILE_COLS - 1)
    on_edge = (row_edge[:, None] | col_edge[None, :]).astype(jnp.float32)
    return (1.0 + boost * on_edge)[None, :, :, None]


def setup_inputs(seed: int = 0) -> dict:
    key = jax.random.key(seed)
    key_x, key_a, key_g, key_one, key_two = jax.random.split(key, 5)
    img_shape = (IMAGES, IMG_HEIGHT, IMG_WIDTH, CHANNELS)
    fan_scale = (9 * CHANNELS) ** -0.5
    x_in = jax.random.normal(key_x, img_shape, jnp.float32).astype(jnp.bfloat16)
    a_pre = jax.random.normal(key_a, img_shape, jnp.float32).astype(jnp.bfloat16)
    g_out = (jax.random.normal(key_g, img_shape, jnp.float32) * edge_weight(2.0)).astype(jnp.bfloat16)
    w_one = (jax.random.normal(key_one, (3, 3, CHANNELS, CHANNELS), jnp.float32) * fan_scale).astype(jnp.bfloat16)
    w_two = (jax.random.normal(key_two, (3, 3, CHANNELS, CHANNELS), jnp.float32) * fan_scale).astype(jnp.bfloat16)
    return {"x_in": x_in, "a_pre": a_pre, "g_out": g_out, "w_one": w_one, "w_two": w_two}


def reference(x_in, a_pre, g_out, w_one, w_two):
    w_one_f = w_one.astype(jnp.float32)
    w_two_f = w_two.astype(jnp.float32)

    def conv_first(image_in):
        return conv_same(image_in, w_one_f)

    def conv_second(image_in):
        return conv_same(image_in, w_two_f)

    def one_image(packed):
        x_img, a_img, g_img = packed
        x_val = x_img[None].astype(jnp.float32)
        a_val = a_img[None].astype(jnp.float32)
        g_val = g_img[None].astype(jnp.float32)
        z_act = jax.nn.gelu(a_val, approximate=True).astype(jnp.bfloat16).astype(jnp.float32)
        d_z = jax.vjp(conv_second, z_act)[1](g_val)[0]
        d_w2 = tap_grads(jnp.pad(z_act, FRAME_PAD), g_val)
        d_a = (d_z * gelu_slope(a_val)).astype(jnp.bfloat16).astype(jnp.float32)
        conv_grad = jax.vjp(conv_first, x_val)[1](d_a)[0]
        d_w1 = tap_grads(jnp.pad(x_val, FRAME_PAD), d_a)
        d_x = (conv_grad + g_val).astype(jnp.bfloat16)
        return d_x[0], d_w1, d_w2

    d_x, w1_parts, w2_parts = lax.map(one_image, (x_in, a_pre, g_out))
    return d_x, jnp.sum(w1_parts, axis=0), jnp.sum(w2_parts, axis=0)
```

```python
import functools

import jax
import jax.numpy as jnp
from jax import lax
from jax.experimental import pallas as pl
from jax.experimental.pallas import tpu as pltpu
from jax.sharding import PartitionSpec as P

MESH = pl.DeviceIdType.MESH
F32 = jnp.float32
BF16 = jnp.bfloat16
CH = 256
ROWS = 48
COLS = 192
PIX = ROWS * COLS
STEP = 4
SPAN = STEP * COLS
CHUNKS = ROWS // STEP
TAPS = 9
BASE_ONE = TAPS + CHUNKS
LAST_TICK = 2 * (TAPS + CHUNKS)
LAGS = (0, 2, 4, 6, 8, 10)


def gelu_slope(pre_act):
    tanh_scale = 0.7978845608028654
    cube_coef = 0.044715
    tanh_val = jnp.tanh(tanh_scale * (pre_act + cube_coef * pre_act * pre_act * pre_act))
    return 0.5 * (1.0 + tanh_val) + 0.5 * pre_act * (1.0 - tanh_val * tanh_val) * tanh_scale * (1.0 + 3.0 * cube_coef * pre_act * pre_act)


def kernel(n_row, n_col, x_hbm, a_hbm, g_hbm, w1_hbm, w2_hbm, dx_hbm, dw1_hbm, dw2_hbm,
           g0, g1, g2, d0, d1, d2, zt, xt, av, w1, w2, acc, res, r0, r1, r2, dza, dzb,
           lhg, rhg, lhd, rhd, clg, crg, cld, crd,
           in_sem, out_sem, dw_sem, hs_sem, hr_sem, as_sem, ar_sem):
    row = lax.axis_index("row")
    col = lax.axis_index("col")
    bx = lax.rem(col, 2)
    by = lax.div(col, 2)
    other = 1 - row
    col_x = col + 1 - 2 * bx
    col_y = col + 2 - 4 * by
    has_left = col > 0
    has_right = col < n_col - 1

    a_copies = [pltpu.make_async_copy(a_hbm.at[pl.ds(12 * q, 12)], av.at[pl.ds(12 * q, 12)], in_sem.at[q]) for q in range(4)]
    g_copy = pltpu.make_async_copy(g_hbm, g1.at[pl.ds(1, ROWS)], in_sem.at[4])
    x_copy = pltpu.make_async_copy(x_hbm, d1.at[pl.ds(1, ROWS)], in_sem.at[5])
    w2_copy = pltpu.make_async_copy(w2_hbm, w2, in_sem.at[6])
    w1_copy = pltpu.make_async_copy(w1_hbm, w1, in_sem.at[7])
    a_copies[0].start()
    g_copy.start()
    for q in range(1, 4):
        a_copies[q].start()
    x_copy.start()
    w2_copy.start()
    w1_copy.start()

    for buf in (lhg, rhg, lhd, rhd):
        buf[...] = jnp.zeros_like(buf)
    for buf in (g1, d1):
        buf[0] = jnp.zeros((COLS, CH), BF16)
        buf[ROWS + 1] = jnp.zeros((COLS, CH), BF16)

    barrier = pltpu.get_barrier_semaphore()
    for dc in range(n_col):
        for dr in range(n_row):
            if dc or dr:
                pl.semaphore_signal(barrier, inc=1, device_id={"col": lax.rem(col + dc, n_col), "row": lax.rem(row + dr, n_row)}, device_id_type=MESH)
    pl.semaphore_wait(barrier, n_col * n_row - 1)

    def frame_copies(which, plane, cl, cr, lh, rh):
        def remote(src, dst, k, dev):
            return pltpu.make_async_remote_copy(src_ref=src, dst_ref=dst, send_sem=hs_sem.at[which, k], recv_sem=hr_sem.at[which, k], device_id=dev, device_id_type=MESH)

        left = jnp.maximum(col - 1, 0)
        right = jnp.minimum(col + 1, n_col - 1)
        src8 = pl.multiple_of(40 * other, 8)
        dst8 = pl.multiple_of(56 * row, 8)
        pair = remote(plane.at[ROWS - (ROWS - 1) * row], plane.at[(ROWS + 1) * row], 0, {"col": col, "row": other})
        to_left = [remote(cl, rh.at[pl.ds(8, ROWS)], 1, {"col": left, "row": row}), remote(cl.at[pl.ds(src8, 8)], rh.at[pl.ds(dst8, 8)], 2, {"col": left, "row": other})]
        to_right = [remote(cr, lh.at[pl.ds(8, ROWS)], 3, {"col": right, "row": row}), remote(cr.at[pl.ds(src8, 8)], lh.at[pl.ds(dst8, 8)], 4, {"col": right, "row": other})]
        return pair, to_left, to_right

    def frame_send(copies):
        pair, to_left, to_right = copies
        pair.start()

        @pl.when(has_left)
        def _():
            for c in to_left:
                c.start()

        @pl.when(has_right)
        def _():
            for c in to_right:
                c.start()

    def frame_wait(copies):
        pair, to_left, to_right = copies
        pair.wait_recv()

        @pl.when(has_right)
        def _():
            for c in to_left:
                c.wait_recv()

        @pl.when(has_left)
        def _():
            for c in to_right:
                c.wait_recv()

    def frame_done(copies):
        pair, to_left, to_right = copies
        pair.wait_send()

        @pl.when(has_left)
        def _():
            for c in to_left:
                c.wait_send()

        @pl.when(has_right)
        def _():
            for c in to_right:
                c.wait_send()

    def unit_copies(u, j):
        half = 128 * row
        p_base, q_base = half, half + 64
        p_mine, q_mine = p_base + 32 * bx, q_base + 32 * by
        p_last, q_last = p_mine + 16 * by, q_mine + 16 * bx

        def rows(ref, start, size):
            return ref.at[u, pl.ds(pl.multiple_of(start, 16), size)]

        def remote(src, dst, k, dev):
            return pltpu.make_async_remote_copy(src_ref=src, dst_ref=dst, send_sem=as_sem.at[u, k], recv_sem=ar_sem.at[u, k], device_id=dev, device_id_type=MESH)

        core = {"col": col, "row": other}
        dev_x = {"col": col_x, "row": row}
        dev_y = {"col": col_y, "row": row}
        if j == 0:
            return [remote(rows(acc, 128 * other, 128), r0.at[u], 0, core)]
        if j == 1:
            return [remote(rows(acc, p_base + 32 * (1 - bx), 32), rows(r1, 0, 32), 1, dev_x), remote(rows(acc, q_base + 32 * (1 - by), 32), rows(r1, 32, 32), 2, dev_y)]
        if j == 2:
            return [remote(rows(acc, p_mine + 16 * (1 - by), 16), rows(r2, 0, 16), 3, dev_y), remote(rows(acc, q_mine + 16 * (1 - bx), 16), rows(r2, 16, 16), 4, dev_x)]
        if j == 3:
            return [remote(rows(res, p_last, 16), rows(res, p_last, 16), 5, dev_y), remote(rows(res, q_last, 16), rows(res, q_last, 16), 6, dev_x)]
        if j == 4:
            return [remote(rows(res, p_mine, 32), rows(res, p_mine, 32), 7, dev_x), remote(rows(res, q_mine, 32), rows(res, q_mine, 32), 8, dev_y)]
        return [remote(rows(res, half, 128), rows(res, half, 128), 9, core)]

    def add_rows(dst, u, start, size, src, src_start):
        at = pl.ds(pl.multiple_of(start, 16), size)
        dst[u, at, :] = acc[u, at, :] + src[u, pl.ds(src_start, size), :]

    def tap_of(v):
        tap_row = jnp.where(v < 1, 1, jnp.where(v < 3, 2 * (v - 1), lax.rem(v, 3)))
        tap_col = jnp.where(v < 3, 1, jnp.where(v < 6, 0, 2))
        return 3 * tap_row + tap_col

    def result_copy(u, first):
        if first:
            return pltpu.make_async_copy(res.at[u], dw2_hbm.at[tap_of(u)], dw_sem.at[u])
        return pltpu.make_async_copy(res.at[u], dw1_hbm.at[tap_of(u - TAPS)], dw_sem.at[u])

    def stage(u, j):
        for c in unit_copies(u, j - 1):
            c.wait_recv()
        half = 128 * row
        if j == 1:
            add_rows(acc, u, half, 128, r0, 0)
        elif j == 2:
            add_rows(acc, u, half + 32 * bx, 32, r1, 0)
            add_rows(acc, u, half + 64 + 32 * by, 32, r1, 32)
        elif j == 3:
            add_rows(res, u, half + 32 * bx + 16 * by, 16, r2, 0)
            add_rows(res, u, half + 64 + 32 * by + 16 * bx, 16, r2, 16)
        if j < 6:
            for c in unit_copies(u, j):
                c.start()
        else:
            for k in range(6):
                for c in unit_copies(u, k):
                    c.wait_send()

            @pl.when(u < TAPS)
            def _():
                result_copy(u, True).start()

            @pl.when(u >= TAPS)
            def _():
                result_copy(u, False).start()

    def tick(s):
        for j in range(6, 0, -1):
            late = s - 2 - LAGS[j - 1]
            is_one = late >= BASE_ONE
            q = jnp.where(is_one, late - BASE_ONE, late)
            in_pair = lax.rem(jnp.maximum(q, 0), 3)
            v = 2 * lax.div(jnp.maximum(q, 0), 3) + in_pair

            @pl.when((q >= 0) & (in_pair < 2) & (v < TAPS))
            def _():
                stage(jnp.where(is_one, TAPS, 0) + v, j)

    def send_first(u):
        for c in unit_copies(u, 0):
            c.start()

    def tap_sum(lhs_t, plane, tap_row):
        total = None
        for q in range(CHUNKS):
            part = jnp.dot(lhs_t[:, SPAN * q:SPAN * (q + 1)], plane[pl.ds(2 - tap_row + STEP * q, STEP)].reshape(SPAN, CH), preferred_element_type=F32)
            total = part if total is None else total + part
        return total

    def shift_rows(center, minus, plus, lh, rh, first, count):
        for k in range(count):
            r = first + k
            v = center[r]
            minus[r] = jnp.concatenate([lh[pl.ds(r + 7, 1), :].astype(BF16), v[:COLS - 1]], axis=0)
            plus[r] = jnp.concatenate([v[1:], rh[pl.ds(r + 7, 1), :].astype(BF16)], axis=0)

    def conv_chunk(planes, w, i):
        total = None
        for k in range(TAPS):
            lhs = planes[k % 3][pl.ds(STEP * i + 2 - k // 3, STEP)].reshape(SPAN, CH)
            part = lax.dot_general(lhs, w[k], (((1,), (1,)), ((), ())), preferred_element_type=F32)
            total = part if total is None else total + part
        return total

    def z_chunk(i):
        z = jax.nn.gelu(av[pl.ds(STEP * i, STEP)].reshape(SPAN, CH).astype(F32), approximate=True).astype(BF16)
        zt[:, pl.ds(pl.multiple_of(SPAN * i, SPAN), SPAN)] = z.T

    def x_chunk(i):
        xt[:, pl.ds(pl.multiple_of(SPAN * i, SPAN), SPAN)] = d1[pl.ds(1 + STEP * i, STEP)].reshape(SPAN, CH).T

    def z_loop(lo, hi):
        lax.fori_loop(lo, hi, lambda i, c: (z_chunk(i), c)[1], 0)

    a_copies[0].wait()
    z_loop(0, 3)
    g_copy.wait()

    def g_edge(i, c):
        for k in range(8):
            r = 8 * i + k
            clg[pl.ds(r, 1), :] = g1[r + 1, 0:8, :].astype(F32)[0:1]
            crg[pl.ds(r, 1), :] = g1[r + 1, COLS - 8:COLS, :].astype(F32)[7:8]
        return c

    lax.fori_loop(0, ROWS // 8, g_edge, 0)
    g_frame = frame_copies(0, g1, clg, crg, lhg, rhg)
    frame_send(g_frame)
    for q in range(1, 4):
        a_copies[q].wait()
    z_loop(3, CHUNKS)

    frame_wait(g_frame)
    acc[0] = tap_sum(zt, g1, 1)
    send_first(0)

    def w2_mid(i, c):
        shift_rows(g1, g2, g0, lhg, rhg, 25 * i, 25)
        acc[1 + i] = tap_sum(zt, g1, 2 * i)
        send_first(1 + i)
        tick(1 + i)
        return c

    lax.fori_loop(0, 2, w2_mid, 0)
    x_copy.wait()
    for side, plane in ((0, g0), (1, g2)):
        def w2_side(i, c, side=side, plane=plane):
            u = 3 + 3 * side + i
            x_chunk(6 * side + 2 * i)
            x_chunk(6 * side + 2 * i + 1)
            acc[u] = tap_sum(zt, plane, i)
            send_first(u)
            tick(u)
            return c

        lax.fori_loop(0, 3, w2_side, 0)

    w2_copy.wait()
    g_planes = (g0, g1, g2)

    def da_chunk(i, dz):
        a_val = av[pl.ds(STEP * i, STEP)].reshape(SPAN, CH).astype(F32)
        d_a = (dz[...] * gelu_slope(a_val)).astype(BF16).reshape(STEP, COLS, CH)
        d1[pl.ds(1 + STEP * i, STEP)] = d_a
        for k in range(STEP):
            cld[pl.ds(STEP * i + k, 1), :] = d_a[k, 0:8].astype(F32)[0:1]
            crd[pl.ds(STEP * i + k, 1), :] = d_a[k, COLS - 8:COLS].astype(F32)[7:8]

    dza[...] = conv_chunk(g_planes, w2, 0)
    tick(TAPS)

    def dz_pair(i, c):
        dzb[...] = conv_chunk(g_planes, w2, 2 * i + 1)
        da_chunk(2 * i, dza)
        tick(TAPS + 2 * i + 1)
        dza[...] = conv_chunk(g_planes, w2, 2 * i + 2)
        da_chunk(2 * i + 1, dzb)
        tick(TAPS + 2 * i + 2)
        return c

    lax.fori_loop(0, CHUNKS // 2 - 1, dz_pair, 0)
    dzb[...] = conv_chunk(g_planes, w2, CHUNKS - 1)
    da_chunk(CHUNKS - 2, dza)
    da_chunk(CHUNKS - 1, dzb)
    tick(TAPS + CHUNKS - 1)

    d_frame = frame_copies(1, d1, cld, crd, lhd, rhd)
    frame_send(d_frame)
    acc[TAPS] = tap_sum(xt, d1, 1)
    send_first(TAPS)
    tick(BASE_ONE)
    frame_wait(d_frame)

    def w1_mid(i, c):
        shift_rows(d1, d2, d0, lhd, rhd, 25 * i, 25)
        acc[TAPS + 1 + i] = tap_sum(xt, d1, 2 * i)
        send_first(TAPS + 1 + i)
        tick(BASE_ONE + 1 + i)
        return c

    lax.fori_loop(0, 2, w1_mid, 0)
    for side, plane in ((0, d0), (1, d2)):
        def w1_side(i, c, side=side, plane=plane):
            v = 3 + 3 * side + i
            acc[TAPS + v] = tap_sum(xt, plane, i)
            send_first(TAPS + v)
            tick(BASE_ONE + v)
            return c

        lax.fori_loop(0, 3, w1_side, 0)

    w1_copy.wait()
    d_planes = (d0, d1, d2)

    def dx_copy(i):
        return pltpu.make_async_copy(av.at[pl.ds(STEP * i, STEP)], dx_hbm.at[pl.ds(STEP * i, STEP)], out_sem.at[i])

    def dx_chunk(i, c):
        total = conv_chunk(d_planes, w1, i) + g1[pl.ds(1 + STEP * i, STEP)].reshape(SPAN, CH).astype(F32)
        av[pl.ds(STEP * i, STEP)] = total.astype(BF16).reshape(STEP, COLS, CH)
        dx_copy(i).start()
        tick(BASE_ONE + TAPS + i)
        return c

    lax.fori_loop(0, CHUNKS, dx_chunk, 0)

    lax.fori_loop(LAST_TICK, BASE_ONE + 2 + 12 + LAGS[-1] + 1, lambda s, c: (tick(s), c)[1], 0)
    frame_done(g_frame)
    frame_done(d_frame)
    lax.fori_loop(0, TAPS, lambda u, c: (result_copy(u, True).wait(), c)[1], 0)
    lax.fori_loop(TAPS, 2 * TAPS, lambda u, c: (result_copy(u, False).wait(), c)[1], 0)
    lax.fori_loop(0, CHUNKS, lambda i, c: (dx_copy(i).wait(), c)[1], 0)


def solution(mesh):
    n_row, n_col = mesh.shape["row"], mesh.shape["col"]

    def local_step(x_tile, a_tile, g_tile, w_one, w_two):
        units = 2 * TAPS
        hbm = pl.BlockSpec(memory_space=pl.ANY)
        wide = pltpu.VMEM((ROWS + 2, COLS, CH), BF16)
        frame = pltpu.VMEM((64, CH), F32)
        edge = pltpu.VMEM((ROWS, CH), F32)
        d_x, d_w1, d_w2 = pl.pallas_call(
            functools.partial(kernel, n_row, n_col),
            out_shape=(
                jax.ShapeDtypeStruct((ROWS, COLS, CH), BF16),
                jax.ShapeDtypeStruct((TAPS, CH, CH), F32),
                jax.ShapeDtypeStruct((TAPS, CH, CH), F32),
            ),
            in_specs=[hbm] * 5,
            out_specs=(hbm,) * 3,
            scratch_shapes=[
                wide, wide, wide, wide, wide, wide,
                pltpu.VMEM((CH, PIX), BF16),
                pltpu.VMEM((CH, PIX), BF16),
                pltpu.VMEM((ROWS, COLS, CH), BF16),
                pltpu.VMEM((TAPS, CH, CH), BF16),
                pltpu.VMEM((TAPS, CH, CH), BF16),
                pltpu.VMEM((units, CH, CH), F32),
                pltpu.VMEM((units, CH, CH), F32),
                pltpu.VMEM((units, 128, CH), F32),
                pltpu.VMEM((units, 64, CH), F32),
                pltpu.VMEM((units, 32, CH), F32),
                pltpu.VMEM((SPAN, CH), F32),
                pltpu.VMEM((SPAN, CH), F32),
                frame, frame, frame, frame,
                edge, edge, edge, edge,
                pltpu.SemaphoreType.DMA((8,)),
                pltpu.SemaphoreType.DMA((CHUNKS,)),
                pltpu.SemaphoreType.DMA((units,)),
                pltpu.SemaphoreType.DMA((2, 5)),
                pltpu.SemaphoreType.DMA((2, 5)),
                pltpu.SemaphoreType.DMA((units, 10)),
                pltpu.SemaphoreType.DMA((units, 10)),
            ],
            compiler_params=pltpu.CompilerParams(collective_id=0, has_side_effects=True, vmem_limit_bytes=67043328),
        )(x_tile[0], a_tile[0], g_tile[0], w_one.reshape(TAPS, CH, CH), w_two.reshape(TAPS, CH, CH))
        shape = (3, 3, CH, CH)
        return d_x[None], d_w1.reshape(shape), d_w2.reshape(shape)

    tile_spec = P(None, "row", "col", None)
    return jax.shard_map(local_step, mesh=mesh, in_specs=(tile_spec, tile_spec, tile_spec, P(), P()), out_specs=(tile_spec, P(), P()), check_vma=False)
```

```python
import functools

import jax
import jax.numpy as jnp
from jax import lax
from jax.experimental import pallas as pl
from jax.experimental.pallas import tpu as pltpu
from jax.sharding import PartitionSpec as P

MESH = pl.DeviceIdType.MESH
F32 = jnp.float32
BF16 = jnp.bfloat16
CH = 256
ROWS = 48
COLS = 192
PIX = ROWS * COLS
STEP = 4
SPAN = STEP * COLS
CHUNKS = ROWS // STEP
TAPS = 9
TAP_ORDER = ((1, 1), (0, 1), (2, 1), (0, 0), (1, 0), (2, 0), (0, 2), (1, 2), (2, 2))
DZ_PLAN = (
    ((1, 8), (2, 6), (3, 3), (4, 0)),
    ((2, 7), (3, 4), (4, 1), (4, 2)),
    ((2, 8), (3, 5), (3, 6), (4, 3), (5, 0)),
    ((3, 7), (4, 4), (4, 5), (5, 1), (5, 2)),
    ((3, 8), (4, 6), (5, 3), (6, 0)),
    ((4, 7), (5, 4), (5, 5), (6, 1)),
)
W1_PLAN = (
    ((4, 8), (5, 6), (6, 2)),
    ((1, 9), (5, 7), (6, 3), (6, 4)),
    ((1, 10), (5, 8), (6, 5), (6, 6)),
)
DX_PLAN = (
    ((1, 17), (2, 15), (3, 12), (4, 9), (4, 10), (6, 7)),
    ((2, 16), (3, 13), (3, 14), (4, 11), (5, 9), (5, 10), (6, 8)),
    ((2, 17), (3, 15), (4, 12), (4, 13), (5, 11), (6, 9)),
    ((3, 16), (3, 17), (4, 14), (4, 15), (5, 12), (5, 13), (6, 10)),
    ((4, 16), (4, 17), (5, 14), (5, 15), (6, 11), (6, 12)),
    ((5, 16), (5, 17), (6, 13), (6, 14)),
    ((6, 15), (6, 16), (6, 17)),
)


def gelu_slope(a):
    scale = 0.7978845608028654
    square = (scale * 0.044715 * a) * a
    tanh_val = jnp.tanh(a * (scale + square))
    return (0.5 + 0.5 * tanh_val) + (0.5 * a * (1.0 - tanh_val * tanh_val)) * (scale + 3.0 * square)


def kernel(n_row, n_col, x_hbm, a_hbm, g_hbm, w1_hbm, w2_hbm, dx_hbm, dw1_hbm, dw2_hbm,
           planes, zt, xt, av, w1, w2, acc, res, r0, r1, r2, dza, dzb,
           lhg, rhg, lhd, rhd, clg, crg, cld, crd,
           in_sem, out_sem, dw_sem, hs_sem, hr_sem, as_sem, ar_sem):
    row = lax.axis_index("row")
    col = lax.axis_index("col")
    by = jnp.where(col >= 2, 1, 0)
    bx = col - 2 * by
    other = 1 - row
    g0, g1, g2, d0, d1, d2 = (planes.at[k] for k in range(6))
    col_x = col + 1 - 2 * bx
    col_y = col + 2 - 4 * by
    has_left = col > 0
    has_right = col < n_col - 1

    a_copies = [pltpu.make_async_copy(a_hbm.at[pl.ds(12 * q, 12)], av.at[pl.ds(12 * q, 12)], in_sem.at[q]) for q in range(4)]
    g_copy = pltpu.make_async_copy(g_hbm, g1.at[pl.ds(1, ROWS)], in_sem.at[4])
    x_copy = pltpu.make_async_copy(x_hbm, d1.at[pl.ds(1, ROWS)], in_sem.at[5])
    w2_copy = pltpu.make_async_copy(w2_hbm, w2, in_sem.at[6])
    w1_copy = pltpu.make_async_copy(w1_hbm, w1, in_sem.at[7])
    a_copies[0].start()
    g_copy.start()
    for q in range(1, 4):
        a_copies[q].start()
    x_copy.start()
    w2_copy.start()
    w1_copy.start()

    for buf in (lhg, rhg, lhd, rhd):
        buf[...] = jnp.zeros_like(buf)
    for buf in (g1, d1):
        buf[0] = jnp.zeros((COLS, CH), BF16)
        buf[ROWS + 1] = jnp.zeros((COLS, CH), BF16)

    barrier = pltpu.get_barrier_semaphore()
    for dc in range(n_col):
        for dr in range(n_row):
            if dc or dr:
                pl.semaphore_signal(barrier, inc=1, device_id={"col": lax.rem(col + dc, n_col), "row": lax.rem(row + dr, n_row)}, device_id_type=MESH)
    pl.semaphore_wait(barrier, n_col * n_row - 1)

    def frame_copies(which, plane, cl, cr, lh, rh):
        def remote(src, dst, k, dev):
            return pltpu.make_async_remote_copy(src_ref=src, dst_ref=dst, send_sem=hs_sem.at[which, k], recv_sem=hr_sem.at[which, k], device_id=dev, device_id_type=MESH)

        left = jnp.maximum(col - 1, 0)
        right = jnp.minimum(col + 1, n_col - 1)
        src8 = pl.multiple_of(40 * other, 8)
        dst8 = pl.multiple_of(56 * row, 8)
        pair = remote(plane.at[ROWS - (ROWS - 1) * row], plane.at[(ROWS + 1) * row], 0, {"col": col, "row": other})
        to_left = [remote(cl, rh.at[pl.ds(8, ROWS)], 1, {"col": left, "row": row}), remote(cl.at[pl.ds(src8, 8)], rh.at[pl.ds(dst8, 8)], 2, {"col": left, "row": other})]
        to_right = [remote(cr, lh.at[pl.ds(8, ROWS)], 3, {"col": right, "row": row}), remote(cr.at[pl.ds(src8, 8)], lh.at[pl.ds(dst8, 8)], 4, {"col": right, "row": other})]
        return pair, to_left, to_right

    def frame_send(copies):
        pair, to_left, to_right = copies
        pair.start()

        @pl.when(has_left)
        def _():
            for c in to_left:
                c.start()

        @pl.when(has_right)
        def _():
            for c in to_right:
                c.start()

    def frame_wait(copies):
        pair, to_left, to_right = copies
        pair.wait_recv()

        @pl.when(has_right)
        def _():
            for c in to_left:
                c.wait_recv()

        @pl.when(has_left)
        def _():
            for c in to_right:
                c.wait_recv()

    def frame_done(copies):
        pair, to_left, to_right = copies
        pair.wait_send()

        @pl.when(has_left)
        def _():
            for c in to_left:
                c.wait_send()

        @pl.when(has_right)
        def _():
            for c in to_right:
                c.wait_send()

    def unit_copies(u, j):
        half = 128 * row
        p_base, q_base = half, half + 64
        p_mine, q_mine = p_base + 32 * bx, q_base + 32 * by
        p_last, q_last = p_mine + 16 * by, q_mine + 16 * bx

        def rows(ref, start, size):
            return ref.at[u, pl.ds(pl.multiple_of(start, 16), size)]

        def remote(src, dst, k, dev):
            return pltpu.make_async_remote_copy(src_ref=src, dst_ref=dst, send_sem=as_sem.at[u, k], recv_sem=ar_sem.at[u, k], device_id=dev, device_id_type=MESH)

        core = {"col": col, "row": other}
        dev_x = {"col": col_x, "row": row}
        dev_y = {"col": col_y, "row": row}
        if j == 0:
            return [remote(rows(acc, 128 * other, 128), r0.at[u], 0, core)]
        if j == 1:
            return [remote(rows(acc, p_base + 32 * (1 - bx), 32), rows(r1, 0, 32), 1, dev_x), remote(rows(acc, q_base + 32 * (1 - by), 32), rows(r1, 32, 32), 2, dev_y)]
        if j == 2:
            return [remote(rows(acc, p_mine + 16 * (1 - by), 16), rows(r2, 0, 16), 3, dev_y), remote(rows(acc, q_mine + 16 * (1 - bx), 16), rows(r2, 16, 16), 4, dev_x)]
        if j == 3:
            return [remote(rows(res, p_last, 16), rows(res, p_last, 16), 5, dev_y), remote(rows(res, q_last, 16), rows(res, q_last, 16), 6, dev_x)]
        if j == 4:
            return [remote(rows(res, p_mine, 32), rows(res, p_mine, 32), 7, dev_x), remote(rows(res, q_mine, 32), rows(res, q_mine, 32), 8, dev_y)]
        return [remote(rows(res, half, 128), rows(res, half, 128), 9, core)]

    def add_rows(dst, u, start, size, src, src_start):
        at = pl.ds(pl.multiple_of(start, 16), size)
        dst[u, at, :] = acc[u, at, :] + src[u, pl.ds(src_start, size), :]

    def result_copy(u):
        out = dw2_hbm if u < TAPS else dw1_hbm
        tap_row, tap_col = TAP_ORDER[u % TAPS]
        return pltpu.make_async_copy(res.at[u], out.at[3 * tap_row + tap_col], dw_sem.at[u])

    def stage(u, j):
        for c in unit_copies(u, j - 1):
            c.wait_recv()
        half = 128 * row
        if j == 1:
            add_rows(acc, u, half, 128, r0, 0)
        elif j == 2:
            add_rows(acc, u, half + 32 * bx, 32, r1, 0)
            add_rows(acc, u, half + 64 + 32 * by, 32, r1, 32)
        elif j == 3:
            add_rows(res, u, half + 32 * bx + 16 * by, 16, r2, 0)
            add_rows(res, u, half + 64 + 32 * by + 16 * bx, 16, r2, 16)
        if j < 6:
            for c in unit_copies(u, j):
                c.start()
        else:
            for k in range(6):
                for c in unit_copies(u, k):
                    c.wait_send()

            result_copy(u).start()

    def run(plan):
        for j, u in plan:
            stage(u, j)

    def send_first(u):
        for c in unit_copies(u, 0):
            c.start()

    def tap_sum(lhs_t, plane, tap_row, fill=()):
        total = None
        blocks = SPAN // CH
        for q in range(CHUNKS):
            rhs = plane[pl.ds(2 - tap_row + STEP * q, STEP)].reshape(SPAN, CH)
            for m in range(blocks):
                for piece in fill[blocks * q + m::CHUNKS * blocks]:
                    piece()
                part = jnp.dot(lhs_t[blocks * q + m], rhs[CH * m:CH * (m + 1)], preferred_element_type=F32)
                total = part if total is None else total + part
        return total

    def shift_row(center, minus, plus, r, lh=None, rh=None):
        v = center[r]
        first = v[:1] if lh is None else lh[pl.ds(r + 7, 1), :].astype(BF16)
        last = v[:1] if rh is None else rh[pl.ds(r + 7, 1), :].astype(BF16)
        minus[r] = jnp.concatenate([first, v[:COLS - 1]], axis=0)
        plus[r] = jnp.concatenate([v[1:], last], axis=0)

    def mend_row(minus, plus, r, lh, rh):
        at = lax.broadcasted_iota(jnp.int32, (8, CH), 0)
        minus[r, 0:8] = jnp.where(at == 0, lh[pl.ds(r + 7, 1), :], minus[r, 0:8].astype(F32)).astype(BF16)
        plus[r, COLS - 8:COLS] = jnp.where(at == 7, rh[pl.ds(r + 7, 1), :], plus[r, COLS - 8:COLS].astype(F32)).astype(BF16)

    def conv_pair(planes, w, i, fill=()):
        totals = [None, None]
        for k in range(TAPS):
            for n in range(2):
                lhs = planes[k % 3][pl.ds(STEP * (2 * i + n) + 2 - k // 3, STEP)].reshape(SPAN, CH)
                part = lax.dot_general(lhs, w[k], (((1,), (1,)), ((), ())), preferred_element_type=F32)
                totals[n] = part if k == 0 else totals[n] + part
            for piece in fill[len(fill) * k // TAPS:len(fill) * (k + 1) // TAPS]:
                piece()
        return totals

    def z_chunk(i):
        z = jax.nn.gelu(av[pl.ds(STEP * i, STEP)].reshape(SPAN, CH).astype(F32), approximate=True).astype(BF16)
        for m in range(SPAN // CH):
            zt[SPAN // CH * i + m] = z[CH * m:CH * (m + 1)].T

    def x_chunk(i):
        x = d1[pl.ds(1 + STEP * i, STEP)].reshape(SPAN, CH)
        for m in range(SPAN // CH):
            xt[SPAN // CH * i + m] = x[CH * m:CH * (m + 1)].T

    def z_loop(lo, hi):
        lax.fori_loop(lo, hi, lambda i, c: (z_chunk(i), c)[1], 0)

    a_copies[0].wait()
    z_loop(0, 3)
    g_copy.wait()

    def g_edge(i, c):
        for k in range(8):
            r = 8 * i + k
            clg[pl.ds(r, 1), :] = g1[r + 1, 0:8, :].astype(F32)[0:1]
            crg[pl.ds(r, 1), :] = g1[r + 1, COLS - 8:COLS, :].astype(F32)[7:8]
        return c

    lax.fori_loop(0, ROWS // 8, g_edge, 0)
    g_frame = frame_copies(0, g1, clg, crg, lhg, rhg)
    frame_send(g_frame)
    for q in range(1, 4):
        a_copies[q].wait()
    z_loop(3, CHUNKS)

    acc[0] = tap_sum(zt, g1, 1)
    send_first(0)
    frame_wait(g_frame)

    def w2_mid(i, c):
        acc[1 + i] = tap_sum(zt, g1, 2 * i, [functools.partial(shift_row, g1, g2, g0, 25 * i + k, lhg, rhg) for k in range(25)])
        send_first(1 + i)
        stage(i, 1)
        return c

    lax.fori_loop(0, 2, w2_mid, 0)
    x_copy.wait()

    def w2_left(i, c):
        x_chunk(2 * i)
        x_chunk(2 * i + 1)
        acc[3 + i] = tap_sum(zt, g0, i)
        send_first(3 + i)
        stage(2 + i, 1)
        stage(i, 2)
        return c

    def w2_right(i, c):
        x_chunk(6 + 2 * i)
        x_chunk(6 + 2 * i + 1)
        acc[6 + i] = tap_sum(zt, g2, i)
        send_first(6 + i)
        stage(5 + i, 1)
        stage(3 + i, 2)
        stage(i, 3)
        return c

    lax.fori_loop(0, 3, w2_left, 0)
    lax.fori_loop(0, 3, w2_right, 0)

    w2_copy.wait()
    g_planes = (g0, g1, g2)

    def da_chunk(i, dz):
        part = COLS // 3

        def one(k, third):
            r, at = STEP * i + k, part * third
            a_val = av[r, at:at + part].astype(F32)
            d_a = (dz[COLS * k + at:COLS * k + at + part] * gelu_slope(a_val)).astype(BF16)
            d1[1 + r, at:at + part] = d_a
            if third == 0:
                cld[pl.ds(r, 1), :] = d_a[0:8].astype(F32)[0:1]
            if third == 2:
                crd[pl.ds(r, 1), :] = d_a[part - 8:].astype(F32)[7:8]

        pieces = []
        for k in range(STEP):
            pieces += [functools.partial(one, k, third) for third in range(3)]
            pieces.append(functools.partial(shift_row, d1, d2, d0, 1 + STEP * i + k))
        return pieces

    def dz_store(pair):
        dza[...], dzb[...] = pair

    def run_at(i, plans):
        for k, plan in enumerate(plans):
            @pl.when(i == k)
            def _(plan=plan):
                run(plan)

    def dz_step(i, c):
        dz_store(conv_pair(g_planes, w2, i, da_chunk(2 * i - 2, dza) + da_chunk(2 * i - 1, dzb)))
        run_at(i - 1, DZ_PLAN[1:])
        return c

    dz_store(conv_pair(g_planes, w2, 0))
    run(DZ_PLAN[0])
    lax.fori_loop(1, CHUNKS // 2, dz_step, 0)

    d_frame = frame_copies(1, d1, cld, crd, lhd, rhd)
    acc[9] = tap_sum(xt, d1, 1, da_chunk(CHUNKS - 2, dza) + da_chunk(CHUNKS - 1, dzb))
    frame_send(d_frame)
    send_first(9)
    run(W1_PLAN[0])
    frame_wait(d_frame)
    shift_row(d1, d2, d0, 0)
    shift_row(d1, d2, d0, ROWS + 1)

    def w1_mid(i, c):
        acc[10 + i] = tap_sum(xt, d1, 2 * i, [functools.partial(mend_row, d2, d0, 25 * i + k, lhd, rhd) for k in range(25)])
        send_first(10 + i)
        run_at(i, W1_PLAN[1:])
        return c

    lax.fori_loop(0, 2, w1_mid, 0)

    def w1_left(i, c):
        acc[12 + i] = tap_sum(xt, d0, i)
        send_first(12 + i)
        stage(11 + i, 1)
        stage(9 + i, 2)
        return c

    def w1_right(i, c):
        acc[15 + i] = tap_sum(xt, d2, i)
        send_first(15 + i)
        stage(14 + i, 1)
        stage(12 + i, 2)
        stage(9 + i, 3)
        return c

    lax.fori_loop(0, 3, w1_left, 0)
    lax.fori_loop(0, 3, w1_right, 0)

    w1_copy.wait()
    d_planes = (d0, d1, d2)

    def dx_copy(i):
        at = pl.ds(2 * STEP * i, 2 * STEP)
        return pltpu.make_async_copy(av.at[at], dx_hbm.at[at], out_sem.at[i])

    def dx_step(i, c):
        for n, total in enumerate(conv_pair(d_planes, w1, i)):
            at = STEP * (2 * i + n)
            total = total + g1[pl.ds(1 + at, STEP)].reshape(SPAN, CH).astype(F32)
            av[pl.ds(at, STEP)] = total.astype(BF16).reshape(STEP, COLS, CH)
        dx_copy(i).start()
        run_at(i, DX_PLAN[:CHUNKS // 2])
        return c

    lax.fori_loop(0, CHUNKS // 2, dx_step, 0)
    run(DX_PLAN[CHUNKS // 2])

    frame_done(g_frame)
    frame_done(d_frame)
    for u in range(2 * TAPS):
        result_copy(u).wait()
    lax.fori_loop(0, CHUNKS // 2, lambda i, c: (dx_copy(i).wait(), c)[1], 0)


def solution(mesh):
    n_row, n_col = mesh.shape["row"], mesh.shape["col"]

    def local_step(x_tile, a_tile, g_tile, w_one, w_two):
        units = 2 * TAPS
        hbm = pl.BlockSpec(memory_space=pl.ANY)
        frame = pltpu.VMEM((64, CH), F32)
        edge = pltpu.VMEM((ROWS, CH), F32)
        d_x, d_w1, d_w2 = pl.pallas_call(
            functools.partial(kernel, n_row, n_col),
            out_shape=(
                jax.ShapeDtypeStruct((ROWS, COLS, CH), BF16),
                jax.ShapeDtypeStruct((TAPS, CH, CH), F32),
                jax.ShapeDtypeStruct((TAPS, CH, CH), F32),
            ),
            in_specs=[hbm] * 5,
            out_specs=(hbm,) * 3,
            scratch_shapes=[
                pltpu.VMEM((6, ROWS + 2, COLS, CH), BF16),
                pltpu.VMEM((PIX // CH, CH, CH), BF16),
                pltpu.VMEM((PIX // CH, CH, CH), BF16),
                pltpu.VMEM((ROWS, COLS, CH), BF16),
                pltpu.VMEM((TAPS, CH, CH), BF16),
                pltpu.VMEM((TAPS, CH, CH), BF16),
                pltpu.VMEM((units, CH, CH), F32),
                pltpu.VMEM((units, CH, CH), F32),
                pltpu.VMEM((units, 128, CH), F32),
                pltpu.VMEM((units, 64, CH), F32),
                pltpu.VMEM((units, 32, CH), F32),
                pltpu.VMEM((SPAN, CH), F32),
                pltpu.VMEM((SPAN, CH), F32),
                frame, frame, frame, frame,
                edge, edge, edge, edge,
                pltpu.SemaphoreType.DMA((8,)),
                pltpu.SemaphoreType.DMA((CHUNKS // 2,)),
                pltpu.SemaphoreType.DMA((units,)),
                pltpu.SemaphoreType.DMA((2, 5)),
                pltpu.SemaphoreType.DMA((2, 5)),
                pltpu.SemaphoreType.DMA((units, 10)),
                pltpu.SemaphoreType.DMA((units, 10)),
            ],
            compiler_params=pltpu.CompilerParams(collective_id=0, has_side_effects=True, vmem_limit_bytes=67043328),
        )(x_tile[0], a_tile[0], g_tile[0], w_one.reshape(TAPS, CH, CH), w_two.reshape(TAPS, CH, CH))
        shape = (3, 3, CH, CH)
        return d_x[None], d_w1.reshape(shape), d_w2.reshape(shape)

    tile_spec = P(None, "row", "col", None)
    return jax.shard_map(local_step, mesh=mesh, in_specs=(tile_spec, tile_spec, tile_spec, P(), P()), out_specs=(tile_spec, P(), P()), check_vma=False)
```

```python
import functools

import jax
import jax.numpy as jnp
from jax import lax
from jax.experimental import pallas as pl
from jax.experimental.pallas import tpu as pltpu
from jax.sharding import PartitionSpec as P

MESH = pl.DeviceIdType.MESH
F32 = jnp.float32
BF16 = jnp.bfloat16
CH = 256
ROWS = 48
COLS = 192
PIX = ROWS * COLS
PARTS = 12
STEP = 4
SPAN = STEP * COLS
CHUNKS = ROWS // STEP
TAPS = 9
TAP_ORDER = ((1, 1), (0, 1), (2, 1), (0, 0), (1, 0), (2, 0), (0, 2), (1, 2), (2, 2))
DZ_PLAN = (
    ((1, 8), (2, 6), (3, 3), (4, 0)),
    ((2, 7), (3, 4), (4, 1), (4, 2)),
    ((2, 8), (3, 5), (3, 6), (4, 3), (5, 0)),
    ((3, 7), (4, 4), (4, 5), (5, 1), (5, 2)),
    ((3, 8), (4, 6), (5, 3), (6, 0)),
    ((4, 7), (5, 4), (5, 5), (6, 1)),
)
W1_PLAN = (
    ((4, 8), (5, 6), (6, 2)),
    ((1, 9), (5, 7), (6, 3), (6, 4)),
    ((1, 10), (5, 8), (6, 5), (6, 6)),
)
DX_PLAN = (
    ((3, 13), (4, 11), (2, 15), (1, 17), (5, 9), (6, 7)),
    ((2, 16), (3, 14), (3, 15), (4, 12), (5, 10), (5, 11), (6, 8)),
    ((2, 17), (3, 16), (4, 13), (4, 14), (5, 12), (6, 9)),
    ((3, 17), (4, 15), (5, 13), (5, 14), (6, 10), (6, 11)),
    ((4, 16), (5, 15), (4, 17), (6, 12), (6, 13)),
    ((5, 16), (5, 17), (6, 14)),
    ((6, 15), (6, 16), (6, 17)),
)


def gelu_slope(a):
    scale = 0.7978845608028654
    square = (scale * 0.044715 * a) * a
    tanh_val = jnp.tanh(a * (scale + square))
    return (0.5 + 0.5 * tanh_val) + (0.5 * a * (1.0 - tanh_val * tanh_val)) * (scale + 3.0 * square)


def kernel(n_row, n_col, x_hbm, a_hbm, g_hbm, w1_hbm, w2_hbm, dx_hbm, dw1_hbm, dw2_hbm,
           planes, zt, xt, av, w1, w2, acc, res, r0, r1, r2, dzs,
           lhg, rhg, lhd, rhd, clg, crg, cld, crd,
           in_sem, out_sem, dw_sem, hs_sem, hr_sem, as_sem, ar_sem):
    row = lax.axis_index("row")
    col = lax.axis_index("col")
    by = jnp.where(col >= 2, 1, 0)
    bx = col - 2 * by
    other = 1 - row
    g0, g1, g2, d0, d1, d2 = (planes.at[k] for k in range(6))
    col_x = col + 1 - 2 * bx
    col_y = col + 2 - 4 * by
    has_left = col > 0
    has_right = col < n_col - 1

    a_copies = [pltpu.make_async_copy(a_hbm.at[pl.ds(12 * q, 12)], av.at[pl.ds(12 * q, 12)], in_sem.at[q]) for q in range(4)]
    g_copy = pltpu.make_async_copy(g_hbm, g1.at[pl.ds(1, ROWS)], in_sem.at[4])
    x_copy = pltpu.make_async_copy(x_hbm, d1.at[pl.ds(1, ROWS)], in_sem.at[5])
    w2_copy = pltpu.make_async_copy(w2_hbm, w2, in_sem.at[6])
    w1_copy = pltpu.make_async_copy(w1_hbm, w1, in_sem.at[7])
    a_copies[0].start()
    g_copy.start()
    for q in range(1, 4):
        a_copies[q].start()
    x_copy.start()
    w2_copy.start()
    w1_copy.start()

    for buf in (lhg, rhg, lhd, rhd):
        buf[...] = jnp.zeros_like(buf)
    for buf in (g1, d1):
        buf[0] = jnp.zeros((COLS, CH), BF16)
        buf[ROWS + 1] = jnp.zeros((COLS, CH), BF16)

    barrier = pltpu.get_barrier_semaphore()
    for dc in range(n_col):
        for dr in range(n_row):
            if dc or dr:
                pl.semaphore_signal(barrier, inc=1, device_id={"col": lax.rem(col + dc, n_col), "row": lax.rem(row + dr, n_row)}, device_id_type=MESH)
    pl.semaphore_wait(barrier, n_col * n_row - 1)

    def frame_copies(which, plane, cl, cr, lh, rh):
        def remote(src, dst, k, dev):
            return pltpu.make_async_remote_copy(src_ref=src, dst_ref=dst, send_sem=hs_sem.at[which, k], recv_sem=hr_sem.at[which, k], device_id=dev, device_id_type=MESH)

        left = jnp.maximum(col - 1, 0)
        right = jnp.minimum(col + 1, n_col - 1)
        src8 = pl.multiple_of(40 * other, 8)
        dst8 = pl.multiple_of(56 * row, 8)
        pair = remote(plane.at[ROWS - (ROWS - 1) * row], plane.at[(ROWS + 1) * row], 0, {"col": col, "row": other})
        to_left = [remote(cl, rh.at[pl.ds(8, ROWS)], 1, {"col": left, "row": row}), remote(cl.at[pl.ds(src8, 8)], rh.at[pl.ds(dst8, 8)], 2, {"col": left, "row": other})]
        to_right = [remote(cr, lh.at[pl.ds(8, ROWS)], 3, {"col": right, "row": row}), remote(cr.at[pl.ds(src8, 8)], lh.at[pl.ds(dst8, 8)], 4, {"col": right, "row": other})]
        return pair, to_left, to_right

    def frame_send(copies):
        pair, to_left, to_right = copies
        pair.start()

        @pl.when(has_left)
        def _():
            for c in to_left:
                c.start()

        @pl.when(has_right)
        def _():
            for c in to_right:
                c.start()

    def frame_wait(copies, columns_only=False):
        pair, to_left, to_right = copies
        if not columns_only:
            pair.wait_recv()

        @pl.when(has_right)
        def _():
            for c in to_left:
                c.wait_recv()

        @pl.when(has_left)
        def _():
            for c in to_right:
                c.wait_recv()

    def frame_done(copies):
        pair, to_left, to_right = copies
        pair.wait_send()

        @pl.when(has_left)
        def _():
            for c in to_left:
                c.wait_send()

        @pl.when(has_right)
        def _():
            for c in to_right:
                c.wait_send()

    def unit_copies(u, j):
        half = 128 * row
        p_base, q_base = half, half + 64
        p_mine, q_mine = p_base + 32 * bx, q_base + 32 * by
        p_last, q_last = p_mine + 16 * by, q_mine + 16 * bx

        def rows(ref, start, size):
            return ref.at[u, pl.ds(pl.multiple_of(start, 16), size)]

        def remote(src, dst, k, dev):
            return pltpu.make_async_remote_copy(src_ref=src, dst_ref=dst, send_sem=as_sem.at[u, k], recv_sem=ar_sem.at[u, k], device_id=dev, device_id_type=MESH)

        core = {"col": col, "row": other}
        dev_x = {"col": col_x, "row": row}
        dev_y = {"col": col_y, "row": row}
        if j == 0:
            return [remote(rows(acc, 128 * other, 128), r0.at[u], 0, core)]
        if j == 1:
            return [remote(rows(acc, p_base + 32 * (1 - bx), 32), rows(r1, 0, 32), 1, dev_x), remote(rows(acc, q_base + 32 * (1 - by), 32), rows(r1, 32, 32), 2, dev_y)]
        if j == 2:
            return [remote(rows(acc, p_mine + 16 * (1 - by), 16), rows(r2, 0, 16), 3, dev_y), remote(rows(acc, q_mine + 16 * (1 - bx), 16), rows(r2, 16, 16), 4, dev_x)]
        if j == 3:
            return [remote(rows(res, p_last, 16), rows(res, p_last, 16), 5, dev_y), remote(rows(res, q_last, 16), rows(res, q_last, 16), 6, dev_x)]
        if j == 4:
            return [remote(rows(res, p_mine, 32), rows(res, p_mine, 32), 7, dev_x), remote(rows(res, q_mine, 32), rows(res, q_mine, 32), 8, dev_y)]
        return [remote(rows(res, half, 128), rows(res, half, 128), 9, core)]

    def add_rows(dst, u, start, size, src, src_start):
        at = pl.ds(pl.multiple_of(start, 16), size)
        dst[u, at, :] = acc[u, at, :] + src[u, pl.ds(src_start, size), :]

    def result_copy(u):
        out = dw2_hbm if u < TAPS else dw1_hbm
        tap_row, tap_col = TAP_ORDER[u % TAPS]
        return pltpu.make_async_copy(res.at[u], out.at[3 * tap_row + tap_col], dw_sem.at[u])

    def stage(u, j):
        for c in unit_copies(u, j - 1):
            c.wait_recv()
        half = 128 * row
        if j == 1:
            add_rows(acc, u, half, 128, r0, 0)
        elif j == 2:
            add_rows(acc, u, half + 32 * bx, 32, r1, 0)
            add_rows(acc, u, half + 64 + 32 * by, 32, r1, 32)
        elif j == 3:
            add_rows(res, u, half + 32 * bx + 16 * by, 16, r2, 0)
            add_rows(res, u, half + 64 + 32 * by + 16 * bx, 16, r2, 16)
        if j < 6:
            for c in unit_copies(u, j):
                c.start()
        else:
            for k in range(6):
                for c in unit_copies(u, k):
                    c.wait_send()

            result_copy(u).start()

    def run(plan):
        for j, u in plan:
            stage(u, j)

    def send_first(u):
        for c in unit_copies(u, 0):
            c.start()

    def tap_sum(lhs_t, plane, tap_row, fill=(), before=None):
        total = None
        blocks = SPAN // CH
        for q in range(CHUNKS):
            rhs = plane[pl.ds(2 - tap_row + STEP * q, STEP)].reshape(SPAN, CH)
            for m in range(blocks):
                for piece in fill[blocks * q + m::CHUNKS * blocks]:
                    piece()
                if before is not None and before[blocks * q + m] is not None:
                    before[blocks * q + m]()
                part = jnp.dot(lhs_t[blocks * q + m], rhs[CH * m:CH * (m + 1)], preferred_element_type=F32)
                total = part if total is None else total + part
        return total

    def shift_row(center, minus, plus, r, lh=None, rh=None):
        v = center[r]
        first = v[:1] if lh is None else lh[pl.ds(r + 7, 1), :].astype(BF16)
        last = v[:1] if rh is None else rh[pl.ds(r + 7, 1), :].astype(BF16)
        minus[r] = jnp.concatenate([first, v[:COLS - 1]], axis=0)
        plus[r] = jnp.concatenate([v[1:], last], axis=0)

    def mend_row(minus, plus, r, lh, rh):
        at = lax.broadcasted_iota(jnp.int32, (8, CH), 0)
        minus[r, 0:8] = jnp.where(at == 0, lh[pl.ds(r + 7, 1), :], minus[r, 0:8].astype(F32)).astype(BF16)
        plus[r, COLS - 8:COLS] = jnp.where(at == 7, rh[pl.ds(r + 7, 1), :], plus[r, COLS - 8:COLS].astype(F32)).astype(BF16)

    def conv_pair(planes, w, i, fill=()):
        totals = [None, None]
        for k in range(TAPS):
            for n in range(2):
                lhs = planes[k % 3][pl.ds(STEP * (2 * i + n) + 2 - k // 3, STEP)].reshape(SPAN, CH)
                part = lax.dot_general(lhs, w[k], (((1,), (1,)), ((), ())), preferred_element_type=F32)
                totals[n] = part if k == 0 else totals[n] + part
            for piece in fill[len(fill) * k // TAPS:len(fill) * (k + 1) // TAPS]:
                piece()
        return totals

    def z_pieces(i):
        def one(m):
            for half in range(2):
                at = CH * m + 128 * half
                z = jax.nn.gelu(av[pl.ds(STEP * i, STEP)].reshape(SPAN, CH)[at:at + 128].astype(F32), approximate=True).astype(BF16)
                zt[SPAN // CH * i + m, :, 128 * half:128 * half + 128] = z.T

        return [functools.partial(one, m) for m in range(SPAN // CH)]

    def z_chunk(i):
        z = jax.nn.gelu(av[pl.ds(STEP * i, STEP)].reshape(SPAN, CH).astype(F32), approximate=True).astype(BF16)
        for m in range(SPAN // CH):
            zt[SPAN // CH * i + m] = z[CH * m:CH * (m + 1)].T

    def x_chunk(i):
        x = d1[pl.ds(1 + STEP * i, STEP)].reshape(SPAN, CH)
        for m in range(SPAN // CH):
            xt[SPAN // CH * i + m] = x[CH * m:CH * (m + 1)].T

    def z_loop(lo, hi):
        lax.fori_loop(lo, hi, lambda i, c: (z_chunk(i), c)[1], 0)

    a_copies[0].wait()
    z_loop(0, 3)
    g_copy.wait()

    def g_edge(i, c):
        for k in range(8):
            r = 8 * i + k
            clg[pl.ds(r, 1), :] = g1[r + 1, 0:8, :].astype(F32)[0:1]
            crg[pl.ds(r, 1), :] = g1[r + 1, COLS - 8:COLS, :].astype(F32)[7:8]
        return c

    lax.fori_loop(0, ROWS // 8, g_edge, 0)
    g_frame = frame_copies(0, g1, clg, crg, lhg, rhg)
    frame_send(g_frame)
    for q in range(1, 4):
        a_copies[q].wait()

    acc[0] = tap_sum(zt, g1, 1, before=[piece for i in range(CHUNKS) for piece in (z_pieces(i) if i >= 3 else [None] * 3)])
    send_first(0)
    frame_wait(g_frame)

    for i in range(2):
        @pl.when(row >= 0)
        def _(i=i):
            acc[1 + i] = tap_sum(zt, g1, 2 * i, [functools.partial(shift_row, g1, g2, g0, 25 * i + k, lhg, rhg) for k in range(25)])

        send_first(1 + i)
        stage(i, 1)

    x_copy.wait()

    def w2_left(i, c):
        x_chunk(2 * i)
        x_chunk(2 * i + 1)
        acc[3 + i] = tap_sum(zt, g0, i)
        send_first(3 + i)
        stage(2 + i, 1)
        stage(i, 2)
        return c

    def w2_right(i, c):
        x_chunk(6 + 2 * i)
        x_chunk(6 + 2 * i + 1)
        acc[6 + i] = tap_sum(zt, g2, i)
        send_first(6 + i)
        stage(5 + i, 1)
        stage(3 + i, 2)
        stage(i, 3)
        return c

    lax.fori_loop(0, 3, w2_left, 0)
    lax.fori_loop(0, 3, w2_right, 0)

    w2_copy.wait()
    g_planes = (g0, g1, g2)

    def da_chunk(i, dz):
        part = COLS // PARTS

        def one(k, third):
            r, at = STEP * i + k, part * third
            a_val = av[r, at:at + part].astype(F32)
            d_a = (dz[COLS * k + at:COLS * k + at + part] * gelu_slope(a_val)).astype(BF16)
            d1[1 + r, at:at + part] = d_a
            if third == 0:
                cld[pl.ds(r, 1), :] = d_a[0:8].astype(F32)[0:1]
            if third == PARTS - 1:
                crd[pl.ds(r, 1), :] = d_a[part - 8:].astype(F32)[7:8]

        pieces = []
        for k in range(STEP):
            pieces += [functools.partial(one, k, third) for third in range(PARTS)]
            pieces.append(functools.partial(shift_row, d1, d2, d0, 1 + STEP * i + k))
        return pieces

    dza, dzb = dzs.at[0], dzs.at[1]

    def dz_store(pair):
        dza[...], dzb[...] = pair

    def run_at(i, plans):
        for k, plan in enumerate(plans):
            @pl.when(i == k)
            def _(plan=plan):
                run(plan)

    def dz_step(i, c):
        dz_store(conv_pair(g_planes, w2, i, da_chunk(2 * i - 2, dza) + da_chunk(2 * i - 1, dzb)))
        run_at(i - 1, DZ_PLAN[1:])
        return c

    dz_store(conv_pair(g_planes, w2, 0))
    run(DZ_PLAN[0])
    lax.fori_loop(1, CHUNKS // 2, dz_step, 0)

    d_frame = frame_copies(1, d1, cld, crd, lhd, rhd)
    def da_last(i, c):
        for piece in da_chunk(CHUNKS - 2 + i, dzs.at[i]):
            piece()
        return c

    lax.fori_loop(0, 2, da_last, 0)
    frame_send(d_frame)
    acc[9] = tap_sum(xt, d1, 1)
    send_first(9)
    run(W1_PLAN[0])
    d_frame[0].wait_recv()

    def w1_mid(i, c):
        acc[10 + i] = tap_sum(xt, d1, 2 * i)
        send_first(10 + i)
        run_at(i, W1_PLAN[1:])
        return c

    lax.fori_loop(0, 2, w1_mid, 0)
    frame_wait(d_frame, True)
    shift_row(d1, d2, d0, 0, lhd, rhd)
    shift_row(d1, d2, d0, ROWS + 1, lhd, rhd)

    def mend(i, c):
        for k in range(8):
            mend_row(d2, d0, 1 + 8 * i + k, lhd, rhd)
        return c

    lax.fori_loop(0, ROWS // 8, mend, 0)

    def w1_left(i, c):
        acc[12 + i] = tap_sum(xt, d0, i)
        send_first(12 + i)
        stage(11 + i, 1)
        stage(9 + i, 2)

        @pl.when(i == 2)
        def _():
            stage(9, 3)

        return c

    def w1_right(i, c):
        acc[15 + i] = tap_sum(xt, d2, i)
        send_first(15 + i)
        stage(12 + i, 2)
        stage(14 + i, 1)
        stage(10 + i, 3)

        @pl.when(i >= 1)
        def _():
            stage(8 + i, 4)

        return c

    lax.fori_loop(0, 3, w1_left, 0)
    lax.fori_loop(0, 3, w1_right, 0)

    w1_copy.wait()
    d_planes = (d0, d1, d2)

    def dx_copy(i):
        at = pl.ds(2 * STEP * i, 2 * STEP)
        return pltpu.make_async_copy(av.at[at], dx_hbm.at[at], out_sem.at[i])

    def dx_step(i, c):
        for n, total in enumerate(conv_pair(d_planes, w1, i)):
            at = STEP * (2 * i + n)
            total = total + g1[pl.ds(1 + at, STEP)].reshape(SPAN, CH).astype(F32)
            av[pl.ds(at, STEP)] = total.astype(BF16).reshape(STEP, COLS, CH)
        dx_copy(i).start()
        run_at(i, DX_PLAN[:CHUNKS // 2])
        return c

    lax.fori_loop(0, CHUNKS // 2, dx_step, 0)
    run(DX_PLAN[CHUNKS // 2])

    frame_done(g_frame)
    frame_done(d_frame)
    for u in range(2 * TAPS):
        result_copy(u).wait()
    lax.fori_loop(0, CHUNKS // 2, lambda i, c: (dx_copy(i).wait(), c)[1], 0)


def solution(mesh):
    n_row, n_col = mesh.shape["row"], mesh.shape["col"]

    def local_step(x_tile, a_tile, g_tile, w_one, w_two):
        units = 2 * TAPS
        hbm = pl.BlockSpec(memory_space=pl.ANY)
        frame = pltpu.VMEM((64, CH), F32)
        edge = pltpu.VMEM((ROWS, CH), F32)
        d_x, d_w1, d_w2 = pl.pallas_call(
            functools.partial(kernel, n_row, n_col),
            out_shape=(
                jax.ShapeDtypeStruct((ROWS, COLS, CH), BF16),
                jax.ShapeDtypeStruct((TAPS, CH, CH), F32),
                jax.ShapeDtypeStruct((TAPS, CH, CH), F32),
            ),
            in_specs=[hbm] * 5,
            out_specs=(hbm,) * 3,
            scratch_shapes=[
                pltpu.VMEM((6, ROWS + 2, COLS, CH), BF16),
                pltpu.VMEM((PIX // CH, CH, CH), BF16),
                pltpu.VMEM((PIX // CH, CH, CH), BF16),
                pltpu.VMEM((ROWS, COLS, CH), BF16),
                pltpu.VMEM((TAPS, CH, CH), BF16),
                pltpu.VMEM((TAPS, CH, CH), BF16),
                pltpu.VMEM((units, CH, CH), F32),
                pltpu.VMEM((units, CH, CH), F32),
                pltpu.VMEM((units, 128, CH), F32),
                pltpu.VMEM((units, 64, CH), F32),
                pltpu.VMEM((units, 32, CH), F32),
                pltpu.VMEM((2, SPAN, CH), F32),
                frame, frame, frame, frame,
                edge, edge, edge, edge,
                pltpu.SemaphoreType.DMA((8,)),
                pltpu.SemaphoreType.DMA((CHUNKS // 2,)),
                pltpu.SemaphoreType.DMA((units,)),
                pltpu.SemaphoreType.DMA((2, 5)),
                pltpu.SemaphoreType.DMA((2, 5)),
                pltpu.SemaphoreType.DMA((units, 10)),
                pltpu.SemaphoreType.DMA((units, 10)),
            ],
            compiler_params=pltpu.CompilerParams(collective_id=0, has_side_effects=True, vmem_limit_bytes=67043328),
        )(x_tile[0], a_tile[0], g_tile[0], w_one.reshape(TAPS, CH, CH), w_two.reshape(TAPS, CH, CH))
        shape = (3, 3, CH, CH)
        return d_x[None], d_w1.reshape(shape), d_w2.reshape(shape)

    tile_spec = P(None, "row", "col", None)
    return jax.shard_map(local_step, mesh=mesh, in_specs=(tile_spec, tile_spec, tile_spec, P(), P()), out_specs=(tile_spec, P(), P()), check_vma=False)
```

```python
import functools

import jax
import jax.numpy as jnp
from jax import lax
from jax.experimental import pallas as pl
from jax.experimental.pallas import tpu as pltpu
from jax.sharding import PartitionSpec as P

MESH = pl.DeviceIdType.MESH
F32 = jnp.float32
BF16 = jnp.bfloat16
CH = 256
ROWS = 48
COLS = 192
PIX = ROWS * COLS
VMEM_LIMIT = 53 * 2**20
PARTS = 12
STEP = 4
SPAN = STEP * COLS
CHUNKS = ROWS // STEP
TAPS = 9
TAP_ORDER = ((1, 1), (0, 1), (2, 1), (0, 0), (1, 0), (2, 0), (0, 2), (1, 2), (2, 2))
DZ_PLAN = (
    ((1, 8), (2, 6), (3, 3), (4, 0)),
    ((2, 7), (3, 4), (4, 1), (4, 2)),
    ((2, 8), (3, 5), (3, 6), (4, 3), (5, 0)),
    ((3, 7), (4, 4), (4, 5), (5, 1), (5, 2)),
    ((3, 8), (4, 6), (5, 3), (6, 0)),
    ((4, 7), (5, 4), (5, 5), (6, 1)),
)
W1_PLAN = (
    ((4, 8), (5, 6), (6, 2)),
    ((1, 9), (5, 7), (6, 3), (6, 4)),
    ((1, 10), (5, 8), (6, 5), (6, 6)),
)
DX_PLAN = (
    ((3, 13), (4, 11), (2, 15), (1, 17), (5, 9), (6, 7)),
    ((2, 16), (3, 14), (3, 15), (4, 12), (5, 10), (5, 11), (6, 8)),
    ((2, 17), (3, 16), (4, 13), (4, 14), (5, 12), (6, 9)),
    ((3, 17), (4, 15), (5, 13), (5, 14), (6, 10), (6, 11)),
    ((4, 16), (5, 15), (4, 17), (6, 12), (6, 13)),
    ((5, 16), (5, 17), (6, 14)),
    ((6, 15), (6, 16), (6, 17)),
)


def gelu_slope(a):
    scale = 0.7978845608028654
    square = (scale * 0.044715 * a) * a
    tanh_val = jnp.tanh(a * (scale + square))
    return (0.5 + 0.5 * tanh_val) + (0.5 * a * (1.0 - tanh_val * tanh_val)) * (scale + 3.0 * square)


def mark(scope, name):
    if scope is not None:
        scope.__exit__(None, None, None)
    if name is None:
        return None
    scope = jax.named_scope(name)
    scope.__enter__()
    return scope


def kernel(n_row, n_col, x_hbm, a_hbm, g_hbm, w1_hbm, w2_hbm, av, dw1, dw2,
           planes, zt, xt, w1, w2, acc, r0, r1, r2, dzs,
           lhg, rhg, lhd, rhd, clg, crg, cld, crd,
           in_sem, hs_sem, hr_sem, as_sem, ar_sem):
    row = lax.axis_index("row")
    col = lax.axis_index("col")
    by = jnp.where(col >= 2, 1, 0)
    bx = col - 2 * by
    other = 1 - row
    g0, g1, g2, d0, d1, d2 = (planes.at[k] for k in range(6))
    col_x = col + 1 - 2 * bx
    col_y = col + 2 - 4 * by
    has_left = col > 0
    has_right = col < n_col - 1

    scope = None
    scope = mark(scope, "p_start")
    a_copies = [pltpu.make_async_copy(a_hbm.at[pl.ds(12 * q, 12)], av.at[pl.ds(12 * q, 12)], in_sem.at[q]) for q in range(4)]
    g_copy = pltpu.make_async_copy(g_hbm, g1.at[pl.ds(1, ROWS)], in_sem.at[4])
    x_copy = pltpu.make_async_copy(x_hbm, d1.at[pl.ds(1, ROWS)], in_sem.at[5])
    w2_copy = pltpu.make_async_copy(w2_hbm, w2, in_sem.at[6])
    w1_copy = pltpu.make_async_copy(w1_hbm, w1, in_sem.at[7])
    a_copies[0].start()
    g_copy.start()
    for q in range(1, 4):
        a_copies[q].start()
    x_copy.start()
    w2_copy.start()
    w1_copy.start()

    for buf in (lhg, rhg, lhd, rhd):
        buf[...] = jnp.zeros_like(buf)
    for buf in (g1, d1):
        buf[0] = jnp.zeros((COLS, CH), BF16)
        buf[ROWS + 1] = jnp.zeros((COLS, CH), BF16)

    scope = mark(scope, "p_barrier")
    barrier = pltpu.get_barrier_semaphore()
    for dc in range(n_col):
        for dr in range(n_row):
            if dc or dr:
                pl.semaphore_signal(barrier, inc=1, device_id={"col": lax.rem(col + dc, n_col), "row": lax.rem(row + dr, n_row)}, device_id_type=MESH)
    pl.semaphore_wait(barrier, n_col * n_row - 1)

    def frame_copies(which, plane, cl, cr, lh, rh):
        def remote(src, dst, k, dev):
            return pltpu.make_async_remote_copy(src_ref=src, dst_ref=dst, send_sem=hs_sem.at[which, k], recv_sem=hr_sem.at[which, k], device_id=dev, device_id_type=MESH)

        left = jnp.maximum(col - 1, 0)
        right = jnp.minimum(col + 1, n_col - 1)
        src8 = pl.multiple_of(40 * other, 8)
        dst8 = pl.multiple_of(56 * row, 8)
        pair = remote(plane.at[ROWS - (ROWS - 1) * row], plane.at[(ROWS + 1) * row], 0, {"col": col, "row": other})
        to_left = [remote(cl, rh.at[pl.ds(8, ROWS)], 1, {"col": left, "row": row}), remote(cl.at[pl.ds(src8, 8)], rh.at[pl.ds(dst8, 8)], 2, {"col": left, "row": other})]
        to_right = [remote(cr, lh.at[pl.ds(8, ROWS)], 3, {"col": right, "row": row}), remote(cr.at[pl.ds(src8, 8)], lh.at[pl.ds(dst8, 8)], 4, {"col": right, "row": other})]
        return pair, to_left, to_right

    def frame_send(copies):
        pair, to_left, to_right = copies
        pair.start()

        @pl.when(has_left)
        def _():
            for c in to_left:
                c.start()

        @pl.when(has_right)
        def _():
            for c in to_right:
                c.start()

    def frame_wait(copies, columns_only=False):
        pair, to_left, to_right = copies
        if not columns_only:
            pair.wait_recv()

        @pl.when(has_right)
        def _():
            for c in to_left:
                c.wait_recv()

        @pl.when(has_left)
        def _():
            for c in to_right:
                c.wait_recv()

    def frame_done(copies):
        pair, to_left, to_right = copies
        pair.wait_send()

        @pl.when(has_left)
        def _():
            for c in to_left:
                c.wait_send()

        @pl.when(has_right)
        def _():
            for c in to_right:
                c.wait_send()

    def result_of(u, first):
        v = u if first else u - TAPS
        if isinstance(v, int):
            tap_row, tap_col = TAP_ORDER[v % TAPS]
        else:
            tap_row = jnp.where(v < 1, 1, jnp.where(v < 3, 2 * (v - 1), jnp.where(v < 6, v - 3, v - 6)))
            tap_col = jnp.where(v < 3, 1, jnp.where(v < 6, 0, 2))
        return dw2 if first else dw1, 3 * tap_row + tap_col

    def unit_copies(u, j, first):
        half = 128 * row
        p_base, q_base = half, half + 64
        p_mine, q_mine = p_base + 32 * bx, q_base + 32 * by
        p_last, q_last = p_mine + 16 * by, q_mine + 16 * bx

        result, tap = result_of(u, first)

        def rows(ref, start, size):
            return ref.at[u, pl.ds(pl.multiple_of(start, 16), size)]

        def done(start, size):
            return result.at[tap, pl.ds(pl.multiple_of(start, 16), size)]

        def remote(src, dst, k, dev):
            return pltpu.make_async_remote_copy(src_ref=src, dst_ref=dst, send_sem=as_sem.at[u, k], recv_sem=ar_sem.at[u, k], device_id=dev, device_id_type=MESH)

        core = {"col": col, "row": other}
        dev_x = {"col": col_x, "row": row}
        dev_y = {"col": col_y, "row": row}
        if j == 0:
            return [remote(rows(acc, 128 * other, 128), r0.at[u], 0, core)]
        if j == 1:
            return [remote(rows(acc, p_base + 32 * (1 - bx), 32), rows(r1, 0, 32), 1, dev_x), remote(rows(acc, q_base + 32 * (1 - by), 32), rows(r1, 32, 32), 2, dev_y)]
        if j == 2:
            return [remote(rows(acc, p_mine + 16 * (1 - by), 16), rows(r2, 0, 16), 3, dev_y), remote(rows(acc, q_mine + 16 * (1 - bx), 16), rows(r2, 16, 16), 4, dev_x)]
        if j == 3:
            return [remote(done(p_last, 16), done(p_last, 16), 5, dev_y), remote(done(q_last, 16), done(q_last, 16), 6, dev_x)]
        if j == 4:
            return [remote(done(p_mine, 32), done(p_mine, 32), 7, dev_x), remote(done(q_mine, 32), done(q_mine, 32), 8, dev_y)]
        return [remote(done(half, 128), done(half, 128), 9, core)]

    def add_rows(dst, where, u, start, size, src, src_start):
        at = pl.ds(pl.multiple_of(start, 16), size)
        dst[where, at, :] = acc[u, at, :] + src[u, pl.ds(src_start, size), :]

    def stage(u, j, first=None):
        first = u < TAPS if first is None else first
        result, tap = result_of(u, first)
        for c in unit_copies(u, j - 1, first):
            c.wait_recv()
        half = 128 * row
        if j == 1:
            add_rows(acc, u, u, half, 128, r0, 0)
        elif j == 2:
            add_rows(acc, u, u, half + 32 * bx, 32, r1, 0)
            add_rows(acc, u, u, half + 64 + 32 * by, 32, r1, 32)
        elif j == 3:
            add_rows(result, tap, u, half + 32 * bx + 16 * by, 16, r2, 0)
            add_rows(result, tap, u, half + 64 + 32 * by + 16 * bx, 16, r2, 16)
        if j < 6:
            for c in unit_copies(u, j, first):
                c.start()
        else:
            for k in range(6):
                for c in unit_copies(u, k, first):
                    c.wait_send()

    def run(plan):
        for j, u in plan:
            stage(u, j)

    def send_first(u):
        for c in unit_copies(u, 0, True):
            c.start()

    def tap_sum(lhs_t, plane, tap_row, fill=(), before=None):
        total = None
        blocks = SPAN // CH
        for q in range(CHUNKS):
            rhs = plane[pl.ds(2 - tap_row + STEP * q, STEP)].reshape(SPAN, CH)
            for m in range(blocks):
                for piece in fill[blocks * q + m::CHUNKS * blocks]:
                    piece()
                if before is not None and before[blocks * q + m] is not None:
                    before[blocks * q + m]()
                part = jnp.dot(lhs_t[blocks * q + m], rhs[CH * m:CH * (m + 1)], preferred_element_type=F32)
                total = part if total is None else total + part
        return total

    def shift_row(center, minus, plus, r, lh=None, rh=None):
        v = center[r]
        first = v[:1] if lh is None else lh[pl.ds(r + 7, 1), :].astype(BF16)
        last = v[:1] if rh is None else rh[pl.ds(r + 7, 1), :].astype(BF16)
        minus[r] = jnp.concatenate([first, v[:COLS - 1]], axis=0)
        plus[r] = jnp.concatenate([v[1:], last], axis=0)

    def mend_row(minus, plus, r, lh, rh):
        at = lax.broadcasted_iota(jnp.int32, (8, CH), 0)
        minus[r, 0:8] = jnp.where(at == 0, lh[pl.ds(r + 7, 1), :], minus[r, 0:8].astype(F32)).astype(BF16)
        plus[r, COLS - 8:COLS] = jnp.where(at == 7, rh[pl.ds(r + 7, 1), :], plus[r, COLS - 8:COLS].astype(F32)).astype(BF16)

    def conv_pair(planes, w, i, fill=()):
        totals = [None, None]
        for k in range(TAPS):
            for n in range(2):
                lhs = planes[k % 3][pl.ds(STEP * (2 * i + n) + 2 - k // 3, STEP)].reshape(SPAN, CH)
                part = lax.dot_general(lhs, w[k], (((1,), (1,)), ((), ())), preferred_element_type=F32)
                totals[n] = part if k == 0 else totals[n] + part
            for piece in fill[len(fill) * k // TAPS:len(fill) * (k + 1) // TAPS]:
                piece()
        return totals

    def z_pieces(i):
        def one(m):
            for half in range(2):
                at = CH * m + 128 * half
                z = jax.nn.gelu(av[pl.ds(STEP * i, STEP)].reshape(SPAN, CH)[at:at + 128].astype(F32), approximate=True).astype(BF16)
                zt[SPAN // CH * i + m, :, 128 * half:128 * half + 128] = z.T

        return [functools.partial(one, m) for m in range(SPAN // CH)]

    def z_chunk(i):
        z = jax.nn.gelu(av[pl.ds(STEP * i, STEP)].reshape(SPAN, CH).astype(F32), approximate=True).astype(BF16)
        for m in range(SPAN // CH):
            zt[SPAN // CH * i + m] = z[CH * m:CH * (m + 1)].T

    def x_chunk(i):
        x = d1[pl.ds(1 + STEP * i, STEP)].reshape(SPAN, CH)
        for m in range(SPAN // CH):
            xt[SPAN // CH * i + m] = x[CH * m:CH * (m + 1)].T

    def z_loop(lo, hi):
        lax.fori_loop(lo, hi, lambda i, c: (z_chunk(i), c)[1], 0)

    scope = mark(scope, "p_z1")
    a_copies[0].wait()
    z_loop(0, 3)
    scope = mark(scope, "p_gwait")
    g_copy.wait()

    def g_edge(i, c):
        for k in range(8):
            r = 8 * i + k
            clg[pl.ds(r, 1), :] = g1[r + 1, 0:8, :].astype(F32)[0:1]
            crg[pl.ds(r, 1), :] = g1[r + 1, COLS - 8:COLS, :].astype(F32)[7:8]
        return c

    lax.fori_loop(0, ROWS // 8, g_edge, 0)
    g_frame = frame_copies(0, g1, clg, crg, lhg, rhg)
    frame_send(g_frame)
    scope = mark(scope, "p_z2")
    for q in range(1, 4):
        a_copies[q].wait()

    scope = mark(scope, "p_s0")
    acc[0] = tap_sum(zt, g1, 1, before=[piece for i in range(CHUNKS) for piece in (z_pieces(i) if i >= 3 else [None] * 3)])
    send_first(0)
    scope = mark(scope, "p_fwg")
    frame_wait(g_frame)

    scope = mark(scope, "p_mid")
    for i in range(2):
        @pl.when(row >= 0)
        def _(i=i):
            acc[1 + i] = tap_sum(zt, g1, 2 * i, [functools.partial(shift_row, g1, g2, g0, 25 * i + k, lhg, rhg) for k in range(25)])

        send_first(1 + i)
        stage(i, 1)

    scope = mark(scope, "p_xw")
    x_copy.wait()

    def w2_left(i, c):
        x_chunk(2 * i)
        x_chunk(2 * i + 1)
        acc[3 + i] = tap_sum(zt, g0, i)
        send_first(3 + i)
        stage(2 + i, 1, True)
        stage(i, 2, True)
        return c

    def w2_right(i, c):
        x_chunk(6 + 2 * i)
        x_chunk(6 + 2 * i + 1)
        acc[6 + i] = tap_sum(zt, g2, i)
        send_first(6 + i)
        stage(5 + i, 1, True)
        stage(3 + i, 2, True)
        stage(i, 3, True)
        return c

    scope = mark(scope, "p_left")
    lax.fori_loop(0, 3, w2_left, 0)
    scope = mark(scope, "p_right")
    lax.fori_loop(0, 3, w2_right, 0)

    w2_copy.wait()
    g_planes = (g0, g1, g2)

    def da_chunk(i, dz):
        part = COLS // PARTS

        def one(k, third):
            r, at = STEP * i + k, part * third
            a_val = av[r, at:at + part].astype(F32)
            d_a = (dz[COLS * k + at:COLS * k + at + part] * gelu_slope(a_val)).astype(BF16)
            d1[1 + r, at:at + part] = d_a
            if third == 0:
                cld[pl.ds(r, 1), :] = d_a[0:8].astype(F32)[0:1]
            if third == PARTS - 1:
                crd[pl.ds(r, 1), :] = d_a[part - 8:].astype(F32)[7:8]

        pieces = []
        for k in range(STEP):
            pieces += [functools.partial(one, k, third) for third in range(PARTS)]
            pieces.append(functools.partial(shift_row, d1, d2, d0, 1 + STEP * i + k))
        return pieces

    dza, dzb = dzs.at[0], dzs.at[1]

    def dz_store(pair):
        dza[...], dzb[...] = pair

    def run_at(i, plans):
        for k, plan in enumerate(plans):
            @pl.when(i == k)
            def _(plan=plan):
                run(plan)

    def dz_step(i, c):
        dz_store(conv_pair(g_planes, w2, i, da_chunk(2 * i - 2, dza) + da_chunk(2 * i - 1, dzb)))
        run_at(i - 1, DZ_PLAN[1:])
        return c

    scope = mark(scope, "p_dz0")
    dz_store(conv_pair(g_planes, w2, 0))
    run(DZ_PLAN[0])
    scope = mark(scope, "p_dz")
    lax.fori_loop(1, CHUNKS // 2, dz_step, 0)

    d_frame = frame_copies(1, d1, cld, crd, lhd, rhd)
    def da_last(i, c):
        for piece in da_chunk(CHUNKS - 2 + i, dzs.at[i]):
            piece()
        return c

    scope = mark(scope, "p_dal")
    lax.fori_loop(0, 2, da_last, 0)
    frame_send(d_frame)
    scope = mark(scope, "p_s9")
    acc[9] = tap_sum(xt, d1, 1)
    send_first(9)
    scope = mark(scope, "p_s9plan")
    run(W1_PLAN[0])
    scope = mark(scope, "p_fwd0")
    d_frame[0].wait_recv()

    def w1_mid(i, c):
        acc[10 + i] = tap_sum(xt, d1, 2 * i)
        send_first(10 + i)
        run_at(i, W1_PLAN[1:])
        return c

    scope = mark(scope, "p_w1mid")
    lax.fori_loop(0, 2, w1_mid, 0)
    scope = mark(scope, "p_fwd1")
    frame_wait(d_frame, True)
    scope = mark(scope, "p_mend")
    shift_row(d1, d2, d0, 0, lhd, rhd)
    shift_row(d1, d2, d0, ROWS + 1, lhd, rhd)

    def mend(i, c):
        for k in range(8):
            mend_row(d2, d0, 1 + 8 * i + k, lhd, rhd)
        return c

    lax.fori_loop(0, ROWS // 8, mend, 0)

    def w1_left(i, c):
        acc[12 + i] = tap_sum(xt, d0, i)
        send_first(12 + i)
        stage(11 + i, 1, False)
        stage(9 + i, 2, False)

        @pl.when(i == 2)
        def _():
            stage(9, 3)

        return c

    def w1_right(i, c):
        acc[15 + i] = tap_sum(xt, d2, i)
        send_first(15 + i)
        stage(12 + i, 2, False)
        stage(14 + i, 1, False)
        stage(10 + i, 3, False)

        @pl.when(i >= 1)
        def _():
            stage(8 + i, 4, False)

        return c

    scope = mark(scope, "p_w1l")
    lax.fori_loop(0, 3, w1_left, 0)
    scope = mark(scope, "p_w1r")
    lax.fori_loop(0, 3, w1_right, 0)

    w1_copy.wait()
    d_planes = (d0, d1, d2)

    def dx_step(i, c):
        for n, total in enumerate(conv_pair(d_planes, w1, i)):
            at = STEP * (2 * i + n)
            total = total + g1[pl.ds(1 + at, STEP)].reshape(SPAN, CH).astype(F32)
            av[pl.ds(at, STEP)] = total.astype(BF16).reshape(STEP, COLS, CH)
        run_at(i, DX_PLAN[:CHUNKS // 2])
        return c

    scope = mark(scope, "p_dx")
    lax.fori_loop(0, CHUNKS // 2, dx_step, 0)
    scope = mark(scope, "p_tail")
    run(DX_PLAN[CHUNKS // 2])

    scope = mark(scope, "p_done")
    frame_done(g_frame)
    frame_done(d_frame)
    mark(scope, None)

def solution(mesh):
    n_row, n_col = mesh.shape["row"], mesh.shape["col"]

    def local_step(x_tile, a_tile, g_tile, w_one, w_two):
        units = 2 * TAPS
        hbm = pl.BlockSpec(memory_space=pl.ANY)
        frame = pltpu.VMEM((64, CH), F32)
        edge = pltpu.VMEM((ROWS, CH), F32)
        d_x, d_w1, d_w2 = pl.pallas_call(
            functools.partial(kernel, n_row, n_col),
            out_shape=(
                pltpu.VMEM((ROWS, COLS, CH), BF16),
                pltpu.VMEM((TAPS, CH, CH), F32),
                pltpu.VMEM((TAPS, CH, CH), F32),
            ),
            in_specs=[hbm] * 5,
            out_specs=(pl.BlockSpec(memory_space=pltpu.VMEM),) * 3,
            scratch_shapes=[
                pltpu.VMEM((6, ROWS + 2, COLS, CH), BF16),
                pltpu.VMEM((PIX // CH, CH, CH), BF16),
                pltpu.VMEM((PIX // CH, CH, CH), BF16),
                pltpu.VMEM((TAPS, CH, CH), BF16),
                pltpu.VMEM((TAPS, CH, CH), BF16),
                pltpu.VMEM((units, CH, CH), F32),
                pltpu.VMEM((units, 128, CH), F32),
                pltpu.VMEM((units, 64, CH), F32),
                pltpu.VMEM((units, 32, CH), F32),
                pltpu.VMEM((2, SPAN, CH), F32),
                frame, frame, frame, frame,
                edge, edge, edge, edge,
                pltpu.SemaphoreType.DMA((8,)),
                pltpu.SemaphoreType.DMA((2, 5)),
                pltpu.SemaphoreType.DMA((2, 5)),
                pltpu.SemaphoreType.DMA((units, 10)),
                pltpu.SemaphoreType.DMA((units, 10)),
            ],
            compiler_params=pltpu.CompilerParams(collective_id=0, has_side_effects=True, vmem_limit_bytes=VMEM_LIMIT),
        )(x_tile[0], a_tile[0], g_tile[0], w_one.reshape(TAPS, CH, CH), w_two.reshape(TAPS, CH, CH))
        shape = (3, 3, CH, CH)
        return d_x[None], d_w1.reshape(shape), d_w2.reshape(shape)

    tile_spec = P(None, "row", "col", None)
    return jax.shard_map(local_step, mesh=mesh, in_specs=(tile_spec, tile_spec, tile_spec, P(), P()), out_specs=(tile_spec, P(), P()), check_vma=False)
```

```python
import functools

import jax
import jax.numpy as jnp
from jax import lax
from jax.experimental import pallas as pl
from jax.experimental.pallas import tpu as pltpu
from jax.sharding import PartitionSpec as P

MESH = pl.DeviceIdType.MESH
F32 = jnp.float32
BF16 = jnp.bfloat16
CH = 256
ROWS = 48
COLS = 192
PIX = ROWS * COLS
VMEM_LIMIT = 53 * 2**20
PARTS = 12
STEP = 4
SPAN = STEP * COLS
CHUNKS = ROWS // STEP
TAPS = 9
TAP_ORDER = ((1, 1), (0, 1), (2, 1), (0, 0), (1, 0), (2, 0), (0, 2), (1, 2), (2, 2))
DZ_PLAN = (
    ((1, 8), (2, 6), (3, 3), (4, 0)),
    ((2, 7), (3, 4), (4, 1), (4, 2)),
    ((2, 8), (3, 5), (3, 6), (4, 3), (5, 0)),
    ((3, 7), (4, 4), (4, 5), (5, 1), (5, 2)),
    ((3, 8), (4, 6), (5, 3), (6, 0)),
    ((4, 7), (5, 4), (5, 5), (6, 1)),
)
W1_PLAN = (
    ((4, 8), (5, 6), (6, 2)),
    ((1, 9), (5, 7), (6, 3), (6, 4)),
    ((1, 10), (5, 8), (6, 5), (6, 6)),
)
DX_PLAN = (
    ((3, 13), (4, 11), (7, 17), (5, 9), (8, 15), (6, 7)),
    ((3, 14), (4, 12), (8, 16), (5, 10), (6, 8), (6, 9)),
    ((4, 13), (8, 17), (5, 11), (6, 10)),
    ((4, 14), (9, 15), (5, 12), (6, 11)),
    ((9, 16), (9, 17), (5, 13), (6, 12)),
    ((5, 14), (6, 13), (6, 15), (6, 16), (6, 17)),
    ((6, 14),),
)
DIRECT = 15


def gelu_slope(a):
    scale = 0.7978845608028654
    square = (scale * 0.044715 * a) * a
    tanh_val = jnp.tanh(a * (scale + square))
    return (0.5 + 0.5 * tanh_val) + (0.5 * a * (1.0 - tanh_val * tanh_val)) * (scale + 3.0 * square)


def mark(scope, name):
    if scope is not None:
        scope.__exit__(None, None, None)
    if name is None:
        return None
    scope = jax.named_scope(name)
    scope.__enter__()
    return scope


def kernel(n_row, n_col, x_hbm, a_hbm, g_hbm, w1_hbm, w2_hbm, av, dw1, dw2,
           planes, zt, xt, w1, w2, acc, r0, r1, r2, dzs,
           lhg, rhg, lhd, rhd, clg, crg, cld, crd,
           in_sem, hs_sem, hr_sem, as_sem, ar_sem):
    row = lax.axis_index("row")
    col = lax.axis_index("col")
    by = jnp.where(col >= 2, 1, 0)
    bx = col - 2 * by
    other = 1 - row
    g0, g1, g2, d0, d1, d2 = (planes.at[k] for k in range(6))
    col_x = col + 1 - 2 * bx
    col_y = col + 2 - 4 * by
    has_left = col > 0
    has_right = col < n_col - 1

    scope = None
    scope = mark(scope, "p_start")
    a_copies = [pltpu.make_async_copy(a_hbm.at[pl.ds(12 * q, 12)], av.at[pl.ds(12 * q, 12)], in_sem.at[q]) for q in range(4)]
    g_copy = pltpu.make_async_copy(g_hbm, g1.at[pl.ds(1, ROWS)], in_sem.at[4])
    x_copy = pltpu.make_async_copy(x_hbm, d1.at[pl.ds(1, ROWS)], in_sem.at[5])
    w2_copy = pltpu.make_async_copy(w2_hbm, w2, in_sem.at[6])
    w1_copy = pltpu.make_async_copy(w1_hbm, w1, in_sem.at[7])
    a_copies[0].start()
    g_copy.start()
    for q in range(1, 4):
        a_copies[q].start()
    x_copy.start()
    w2_copy.start()
    w1_copy.start()

    for buf in (lhg, rhg, lhd, rhd):
        buf[...] = jnp.zeros_like(buf)
    for buf in (g1, d1):
        buf[0] = jnp.zeros((COLS, CH), BF16)
        buf[ROWS + 1] = jnp.zeros((COLS, CH), BF16)

    scope = mark(scope, "p_barrier")
    barrier = pltpu.get_barrier_semaphore()
    for dc in range(n_col):
        for dr in range(n_row):
            if dc or dr:
                pl.semaphore_signal(barrier, inc=1, device_id={"col": lax.rem(col + dc, n_col), "row": lax.rem(row + dr, n_row)}, device_id_type=MESH)
    pl.semaphore_wait(barrier, n_col * n_row - 1)

    def frame_copies(which, plane, cl, cr, lh, rh):
        def remote(src, dst, k, dev):
            return pltpu.make_async_remote_copy(src_ref=src, dst_ref=dst, send_sem=hs_sem.at[which, k], recv_sem=hr_sem.at[which, k], device_id=dev, device_id_type=MESH)

        left = jnp.maximum(col - 1, 0)
        right = jnp.minimum(col + 1, n_col - 1)
        src8 = pl.multiple_of(40 * other, 8)
        dst8 = pl.multiple_of(56 * row, 8)
        pair = remote(plane.at[ROWS - (ROWS - 1) * row], plane.at[(ROWS + 1) * row], 0, {"col": col, "row": other})
        to_left = [remote(cl, rh.at[pl.ds(8, ROWS)], 1, {"col": left, "row": row}), remote(cl.at[pl.ds(src8, 8)], rh.at[pl.ds(dst8, 8)], 2, {"col": left, "row": other})]
        to_right = [remote(cr, lh.at[pl.ds(8, ROWS)], 3, {"col": right, "row": row}), remote(cr.at[pl.ds(src8, 8)], lh.at[pl.ds(dst8, 8)], 4, {"col": right, "row": other})]
        return pair, to_left, to_right

    def frame_send(copies):
        pair, to_left, to_right = copies
        pair.start()

        @pl.when(has_left)
        def _():
            for c in to_left:
                c.start()

        @pl.when(has_right)
        def _():
            for c in to_right:
                c.start()

    def frame_wait(copies, columns_only=False):
        pair, to_left, to_right = copies
        if not columns_only:
            pair.wait_recv()

        @pl.when(has_right)
        def _():
            for c in to_left:
                c.wait_recv()

        @pl.when(has_left)
        def _():
            for c in to_right:
                c.wait_recv()

    def frame_done(copies):
        pair, to_left, to_right = copies
        pair.wait_send()

        @pl.when(has_left)
        def _():
            for c in to_left:
                c.wait_send()

        @pl.when(has_right)
        def _():
            for c in to_right:
                c.wait_send()

    def result_of(u, first):
        v = u if first else u - TAPS
        if isinstance(v, int):
            tap_row, tap_col = TAP_ORDER[v % TAPS]
        else:
            tap_row = jnp.where(v < 1, 1, jnp.where(v < 3, 2 * (v - 1), jnp.where(v < 6, v - 3, v - 6)))
            tap_col = jnp.where(v < 3, 1, jnp.where(v < 6, 0, 2))
        return dw2 if first else dw1, 3 * tap_row + tap_col

    def unit_copies(u, j, first):
        half = 128 * row
        p_base, q_base = half, half + 64
        p_mine, q_mine = p_base + 32 * bx, q_base + 32 * by
        p_last, q_last = p_mine + 16 * by, q_mine + 16 * bx

        result, tap = result_of(u, first)

        def rows(ref, start, size):
            return ref.at[u, pl.ds(pl.multiple_of(start, 16), size)]

        def done(start, size):
            return result.at[tap, pl.ds(pl.multiple_of(start, 16), size)]

        def remote(src, dst, k, dev):
            return pltpu.make_async_remote_copy(src_ref=src, dst_ref=dst, send_sem=as_sem.at[u, k], recv_sem=ar_sem.at[u, k], device_id=dev, device_id_type=MESH)

        core = {"col": col, "row": other}
        dev_x = {"col": col_x, "row": row}
        dev_y = {"col": col_y, "row": row}
        if j == 0:
            return [remote(rows(acc, 128 * other, 128), r0.at[u], 0, core)]
        if j in (7, 8):
            mine = half + 32 * col
            peers = ((col_x, rows(r1, 0, 32)), (col_y, rows(r1, 32, 32)), (3 - col, rows(r2, 0, 32)))
            if j == 7:
                return [remote(rows(acc, half + 32 * peer, 32), slot, 1 + k, {"col": peer, "row": row}) for k, (peer, slot) in enumerate(peers)]
            return [remote(done(mine, 32), done(mine, 32), 4 + k, {"col": peer, "row": row}) for k, (peer, _) in enumerate(peers)]
        if j == 1:
            return [remote(rows(acc, p_base + 32 * (1 - bx), 32), rows(r1, 0, 32), 1, dev_x), remote(rows(acc, q_base + 32 * (1 - by), 32), rows(r1, 32, 32), 2, dev_y)]
        if j == 2:
            return [remote(rows(acc, p_mine + 16 * (1 - by), 16), rows(r2, 0, 16), 3, dev_y), remote(rows(acc, q_mine + 16 * (1 - bx), 16), rows(r2, 16, 16), 4, dev_x)]
        if j == 3:
            return [remote(done(p_last, 16), done(p_last, 16), 5, dev_y), remote(done(q_last, 16), done(q_last, 16), 6, dev_x)]
        if j == 4:
            return [remote(done(p_mine, 32), done(p_mine, 32), 7, dev_x), remote(done(q_mine, 32), done(q_mine, 32), 8, dev_y)]
        return [remote(done(half, 128), done(half, 128), 9, core)]

    def add_rows(dst, where, u, start, size, src, src_start):
        at = pl.ds(pl.multiple_of(start, 16), size)
        dst[where, at, :] = acc[u, at, :] + src[u, pl.ds(src_start, size), :]

    def stage(u, j, first=None):
        first = u < TAPS if first is None else first
        result, tap = result_of(u, first)
        direct = isinstance(u, int) and u >= DIRECT
        for c in unit_copies(u, {7: 0, 8: 7, 9: 8}.get(j, j - 1), first):
            c.wait_recv()
        half = 128 * row
        if j in (1, 7):
            add_rows(acc, u, u, half, 128, r0, 0)
        elif j == 2:
            add_rows(acc, u, u, half + 32 * bx, 32, r1, 0)
            add_rows(acc, u, u, half + 64 + 32 * by, 32, r1, 32)
        elif j == 3:
            add_rows(result, tap, u, half + 32 * bx + 16 * by, 16, r2, 0)
            add_rows(result, tap, u, half + 64 + 32 * by + 16 * bx, 16, r2, 16)
        elif j == 8:
            at = pl.ds(pl.multiple_of(half + 32 * col, 16), 32)
            result[tap, at, :] = (acc[u, at, :] + r1[u, 0:32, :]) + (r1[u, 32:64, :] + r2[u, 0:32, :])
        if j == 6:
            for k in (0, 7, 8, 5) if direct else range(6):
                for c in unit_copies(u, k, first):
                    c.wait_send()
        else:
            for c in unit_copies(u, {9: 5}.get(j, j), first):
                c.start()

    def run(plan):
        for j, u in plan:
            stage(u, j)

    def send_first(u):
        for c in unit_copies(u, 0, True):
            c.start()

    def tap_sum(lhs_t, plane, tap_row, fill=(), before=None):
        total = None
        blocks = SPAN // CH
        for q in range(CHUNKS):
            rhs = plane[pl.ds(2 - tap_row + STEP * q, STEP)].reshape(SPAN, CH)
            for m in range(blocks):
                for piece in fill[blocks * q + m::CHUNKS * blocks]:
                    piece()
                if before is not None and before[blocks * q + m] is not None:
                    before[blocks * q + m]()
                part = jnp.dot(lhs_t[blocks * q + m], rhs[CH * m:CH * (m + 1)], preferred_element_type=F32)
                total = part if total is None else total + part
        return total

    def shift_row(center, minus, plus, r, lh=None, rh=None):
        v = center[r]
        first = v[:1] if lh is None else lh[pl.ds(r + 7, 1), :].astype(BF16)
        last = v[:1] if rh is None else rh[pl.ds(r + 7, 1), :].astype(BF16)
        minus[r] = jnp.concatenate([first, v[:COLS - 1]], axis=0)
        plus[r] = jnp.concatenate([v[1:], last], axis=0)

    def mend_row(minus, plus, r, lh, rh):
        at = lax.broadcasted_iota(jnp.int32, (8, CH), 0)
        minus[r, 0:8] = jnp.where(at == 0, lh[pl.ds(r + 7, 1), :], minus[r, 0:8].astype(F32)).astype(BF16)
        plus[r, COLS - 8:COLS] = jnp.where(at == 7, rh[pl.ds(r + 7, 1), :], plus[r, COLS - 8:COLS].astype(F32)).astype(BF16)

    def conv_pair(planes, w, i, fill=()):
        totals = [None, None]
        for k in range(TAPS):
            for n in range(2):
                lhs = planes[k % 3][pl.ds(STEP * (2 * i + n) + 2 - k // 3, STEP)].reshape(SPAN, CH)
                part = lax.dot_general(lhs, w[k], (((1,), (1,)), ((), ())), preferred_element_type=F32)
                totals[n] = part if k == 0 else totals[n] + part
            for piece in fill[len(fill) * k // TAPS:len(fill) * (k + 1) // TAPS]:
                piece()
        return totals

    def z_pieces(i):
        def one(m):
            for half in range(2):
                at = CH * m + 128 * half
                z = jax.nn.gelu(av[pl.ds(STEP * i, STEP)].reshape(SPAN, CH)[at:at + 128].astype(F32), approximate=True).astype(BF16)
                zt[SPAN // CH * i + m, :, 128 * half:128 * half + 128] = z.T

        return [functools.partial(one, m) for m in range(SPAN // CH)]

    def z_chunk(i):
        z = jax.nn.gelu(av[pl.ds(STEP * i, STEP)].reshape(SPAN, CH).astype(F32), approximate=True).astype(BF16)
        for m in range(SPAN // CH):
            zt[SPAN // CH * i + m] = z[CH * m:CH * (m + 1)].T

    def x_chunk(i):
        x = d1[pl.ds(1 + STEP * i, STEP)].reshape(SPAN, CH)
        for m in range(SPAN // CH):
            xt[SPAN // CH * i + m] = x[CH * m:CH * (m + 1)].T

    def z_loop(lo, hi):
        lax.fori_loop(lo, hi, lambda i, c: (z_chunk(i), c)[1], 0)

    scope = mark(scope, "p_z1")
    a_copies[0].wait()
    z_loop(0, 3)
    scope = mark(scope, "p_gwait")
    g_copy.wait()

    def g_edge(i, c):
        for k in range(8):
            r = 8 * i + k
            clg[pl.ds(r, 1), :] = g1[r + 1, 0:8, :].astype(F32)[0:1]
            crg[pl.ds(r, 1), :] = g1[r + 1, COLS - 8:COLS, :].astype(F32)[7:8]
        return c

    lax.fori_loop(0, ROWS // 8, g_edge, 0)
    g_frame = frame_copies(0, g1, clg, crg, lhg, rhg)
    frame_send(g_frame)
    scope = mark(scope, "p_z2")
    for q in range(1, 4):
        a_copies[q].wait()

    scope = mark(scope, "p_s0")
    acc[0] = tap_sum(zt, g1, 1, before=[piece for i in range(CHUNKS) for piece in (z_pieces(i) if i >= 3 else [None] * 3)])
    send_first(0)
    scope = mark(scope, "p_fwg")
    frame_wait(g_frame)

    scope = mark(scope, "p_mid")
    for i in range(2):
        @pl.when(row >= 0)
        def _(i=i):
            acc[1 + i] = tap_sum(zt, g1, 2 * i, [functools.partial(shift_row, g1, g2, g0, 25 * i + k, lhg, rhg) for k in range(25)])

        send_first(1 + i)
        stage(i, 1)

    scope = mark(scope, "p_xw")
    x_copy.wait()

    def w2_left(i, c):
        x_chunk(2 * i)
        x_chunk(2 * i + 1)
        acc[3 + i] = tap_sum(zt, g0, i)
        send_first(3 + i)
        stage(2 + i, 1, True)
        stage(i, 2, True)
        return c

    def w2_right(i, c):
        x_chunk(6 + 2 * i)
        x_chunk(6 + 2 * i + 1)
        acc[6 + i] = tap_sum(zt, g2, i)
        send_first(6 + i)
        stage(5 + i, 1, True)
        stage(3 + i, 2, True)
        stage(i, 3, True)
        return c

    scope = mark(scope, "p_left")
    lax.fori_loop(0, 3, w2_left, 0)
    scope = mark(scope, "p_right")
    lax.fori_loop(0, 3, w2_right, 0)

    w2_copy.wait()
    g_planes = (g0, g1, g2)

    def da_chunk(i, dz):
        part = COLS // PARTS

        def one(k, third):
            r, at = STEP * i + k, part * third
            a_val = av[r, at:at + part].astype(F32)
            d_a = (dz[COLS * k + at:COLS * k + at + part] * gelu_slope(a_val)).astype(BF16)
            d1[1 + r, at:at + part] = d_a
            if third == 0:
                cld[pl.ds(r, 1), :] = d_a[0:8].astype(F32)[0:1]
            if third == PARTS - 1:
                crd[pl.ds(r, 1), :] = d_a[part - 8:].astype(F32)[7:8]

        pieces = []
        for k in range(STEP):
            pieces += [functools.partial(one, k, third) for third in range(PARTS)]
            pieces.append(functools.partial(shift_row, d1, d2, d0, 1 + STEP * i + k))
        return pieces

    dza, dzb = dzs.at[0], dzs.at[1]

    def dz_store(pair):
        dza[...], dzb[...] = pair

    def run_at(i, plans):
        for k, plan in enumerate(plans):
            @pl.when(i == k)
            def _(plan=plan):
                run(plan)

    def dz_step(i, c):
        dz_store(conv_pair(g_planes, w2, i, da_chunk(2 * i - 2, dza) + da_chunk(2 * i - 1, dzb)))
        run_at(i - 1, DZ_PLAN[1:])
        return c

    scope = mark(scope, "p_dz0")
    dz_store(conv_pair(g_planes, w2, 0))
    run(DZ_PLAN[0])
    scope = mark(scope, "p_dz")
    lax.fori_loop(1, CHUNKS // 2, dz_step, 0)

    d_frame = frame_copies(1, d1, cld, crd, lhd, rhd)
    def da_last(i, c):
        for piece in da_chunk(CHUNKS - 2 + i, dzs.at[i]):
            piece()
        return c

    scope = mark(scope, "p_dal")
    lax.fori_loop(0, 2, da_last, 0)
    frame_send(d_frame)
    scope = mark(scope, "p_s9")
    acc[9] = tap_sum(xt, d1, 1)
    send_first(9)
    scope = mark(scope, "p_s9plan")
    run(W1_PLAN[0])
    scope = mark(scope, "p_fwd0")
    d_frame[0].wait_recv()

    def w1_mid(i, c):
        acc[10 + i] = tap_sum(xt, d1, 2 * i)
        send_first(10 + i)
        run_at(i, W1_PLAN[1:])
        return c

    scope = mark(scope, "p_w1mid")
    lax.fori_loop(0, 2, w1_mid, 0)
    scope = mark(scope, "p_fwd1")
    frame_wait(d_frame, True)
    scope = mark(scope, "p_mend")
    shift_row(d1, d2, d0, 0, lhd, rhd)
    shift_row(d1, d2, d0, ROWS + 1, lhd, rhd)

    def mend(i, c):
        for k in range(8):
            mend_row(d2, d0, 1 + 8 * i + k, lhd, rhd)
        return c

    lax.fori_loop(0, ROWS // 8, mend, 0)

    def w1_left(i, c):
        acc[12 + i] = tap_sum(xt, d0, i)
        send_first(12 + i)
        stage(11 + i, 1, False)
        stage(9 + i, 2, False)

        @pl.when(i == 2)
        def _():
            stage(9, 3)

        return c

    def w1_right(i, c):
        acc[15 + i] = tap_sum(xt, d2, i)
        send_first(15 + i)
        stage(12 + i, 2, False)

        @pl.when(i == 0)
        def _():
            stage(14, 1)

        @pl.when(i >= 1)
        def _():
            stage(14 + i, 7, False)

        stage(10 + i, 3, False)

        @pl.when(i >= 1)
        def _():
            stage(8 + i, 4, False)

        return c

    scope = mark(scope, "p_w1l")
    lax.fori_loop(0, 3, w1_left, 0)
    scope = mark(scope, "p_w1r")
    lax.fori_loop(0, 3, w1_right, 0)

    w1_copy.wait()
    d_planes = (d0, d1, d2)

    def dx_step(i, c):
        for n, total in enumerate(conv_pair(d_planes, w1, i)):
            at = STEP * (2 * i + n)
            total = total + g1[pl.ds(1 + at, STEP)].reshape(SPAN, CH).astype(F32)
            av[pl.ds(at, STEP)] = total.astype(BF16).reshape(STEP, COLS, CH)
        run_at(i, DX_PLAN[:CHUNKS // 2])
        return c

    scope = mark(scope, "p_dx")
    lax.fori_loop(0, CHUNKS // 2, dx_step, 0)
    scope = mark(scope, "p_tail")
    run(DX_PLAN[CHUNKS // 2])

    scope = mark(scope, "p_done")
    frame_done(g_frame)
    frame_done(d_frame)
    mark(scope, None)

def write_out(*refs):
    sem = refs[-1]
    copies = [pltpu.make_async_copy(src, dst, sem.at[k]) for k, (src, dst) in enumerate(zip(refs[:3], refs[3:6]))]
    for c in copies:
        c.start()
    for c in copies:
        c.wait()


def solution(mesh):
    n_row, n_col = mesh.shape["row"], mesh.shape["col"]

    def local_step(x_tile, a_tile, g_tile, w_one, w_two):
        units = 2 * TAPS
        hbm = pl.BlockSpec(memory_space=pl.ANY)
        frame = pltpu.VMEM((64, CH), F32)
        edge = pltpu.VMEM((ROWS, CH), F32)
        d_x, d_w1, d_w2 = pl.pallas_call(
            functools.partial(kernel, n_row, n_col),
            out_shape=(
                pltpu.VMEM((ROWS, COLS, CH), BF16),
                pltpu.VMEM((TAPS, CH, CH), F32),
                pltpu.VMEM((TAPS, CH, CH), F32),
            ),
            in_specs=[hbm] * 5,
            out_specs=(pl.BlockSpec(memory_space=pltpu.VMEM),) * 3,
            scratch_shapes=[
                pltpu.VMEM((6, ROWS + 2, COLS, CH), BF16),
                pltpu.VMEM((PIX // CH, CH, CH), BF16),
                pltpu.VMEM((PIX // CH, CH, CH), BF16),
                pltpu.VMEM((TAPS, CH, CH), BF16),
                pltpu.VMEM((TAPS, CH, CH), BF16),
                pltpu.VMEM((units, CH, CH), F32),
                pltpu.VMEM((units, 128, CH), F32),
                pltpu.VMEM((units, 64, CH), F32),
                pltpu.VMEM((units, 32, CH), F32),
                pltpu.VMEM((2, SPAN, CH), F32),
                frame, frame, frame, frame,
                edge, edge, edge, edge,
                pltpu.SemaphoreType.DMA((8,)),
                pltpu.SemaphoreType.DMA((2, 5)),
                pltpu.SemaphoreType.DMA((2, 5)),
                pltpu.SemaphoreType.DMA((units, 10)),
                pltpu.SemaphoreType.DMA((units, 10)),
            ],
            compiler_params=pltpu.CompilerParams(collective_id=0, has_side_effects=True, vmem_limit_bytes=VMEM_LIMIT),
        )(x_tile[0], a_tile[0], g_tile[0], w_one.reshape(TAPS, CH, CH), w_two.reshape(TAPS, CH, CH))
        held = [pltpu.with_memory_space_constraint(r, pltpu.VMEM) for r in (d_x, d_w1, d_w2)]
        d_x, d_w1, d_w2 = pl.pallas_call(
            write_out,
            out_shape=tuple(jax.ShapeDtypeStruct(r.shape, r.dtype) for r in (d_x, d_w1, d_w2)),
            in_specs=[pl.BlockSpec(memory_space=pltpu.VMEM)] * 3,
            out_specs=(hbm,) * 3,
            scratch_shapes=[pltpu.SemaphoreType.DMA((3,))],
            compiler_params=pltpu.CompilerParams(vmem_limit_bytes=2**20),
        )(*held)
        shape = (3, 3, CH, CH)
        return d_x[None], d_w1.reshape(shape), d_w2.reshape(shape)

    tile_spec = P(None, "row", "col", None)
    return jax.shard_map(local_step, mesh=mesh, in_specs=(tile_spec, tile_spec, tile_spec, P(), P()), out_specs=(tile_spec, P(), P()), check_vma=False)
```

```python
import functools

import jax
import jax.numpy as jnp
from jax import lax
from jax.experimental import pallas as pl
from jax.experimental.pallas import tpu as pltpu
from jax.sharding import PartitionSpec as P

MESH = pl.DeviceIdType.MESH
F32 = jnp.float32
BF16 = jnp.bfloat16
CH = 256
ROWS = 48
COLS = 192
PIX = ROWS * COLS
VMEM_LIMIT = 56000 * 2**10
PARTS = 12
STEP = 4
SPAN = STEP * COLS
CHUNKS = ROWS // STEP
TAPS = 9
TAP_ORDER = ((1, 1), (0, 1), (2, 1), (0, 0), (1, 0), (2, 0), (0, 2), (1, 2), (2, 2))
DZ_PLAN = (
    ((1, 8), (2, 6), (3, 3), (4, 0)),
    ((2, 7), (3, 4), (4, 1), (4, 2)),
    ((2, 8), (3, 5), (3, 6), (4, 3), (5, 0)),
    ((3, 7), (4, 4), (5, 1), (5, 2)),
    ((3, 8), (4, 5), (5, 3), (6, 0)),
    ((4, 6), (5, 4), (6, 1)),
)
W1_PLAN = (
    ((4, 7), (4, 8), (5, 5), (6, 2)),
    ((1, 9), (5, 6), (6, 3), (6, 4)),
    ((1, 10), (5, 7), (6, 5)),
    ((1, 11), (2, 9), (2, 10), (5, 8), (6, 6)),
    (),
    ((2, 11), (1, 12), (3, 9), (6, 7)),
    ((3, 10), (1, 13), (6, 8)),
    ((3, 11), (2, 12), (1, 14), (4, 9)),
    ((2, 13), (1, 15), (4, 10)),
    ((3, 12), (2, 14), (7, 16), (4, 11)),
)
DX_PLAN = (
    ((3, 13), (2, 15), (7, 17), (5, 9), (5, 10)),
    ((3, 14), (4, 12), (8, 16), (3, 15), (5, 11), (6, 9)),
    ((4, 13), (8, 17), (6, 10)),
    ((4, 14), (4, 15), (5, 12), (6, 11)),
    ((9, 16), (9, 17), (5, 13), (6, 12)),
    ((5, 14), (5, 15), (6, 13), (6, 16), (6, 17), (6, 14), (6, 15)),
)
DIRECT = 16


def gelu_slope(a):
    scale = 0.7978845608028654
    square = (scale * 0.044715 * a) * a
    tanh_val = jnp.tanh(a * (scale + square))
    return (0.5 + 0.5 * tanh_val) + (0.5 * a * (1.0 - tanh_val * tanh_val)) * (scale + 3.0 * square)


def mark(scope, name):
    if scope is not None:
        scope.__exit__(None, None, None)
    if name is None:
        return None
    scope = jax.named_scope(name)
    scope.__enter__()
    return scope


def kernel(n_row, n_col, x_hbm, a_hbm, g_hbm, w1_hbm, w2_hbm, av, dw1, dw2,
           planes, zt, xt, w1, w2, acc, r0, r1, r2, dzs,
           lhg, rhg, lhd, rhd, clg, crg, cld, crd,
           in_sem, hs_sem, hr_sem, as_sem, ar_sem):
    row = lax.axis_index("row")
    col = lax.axis_index("col")
    by = jnp.where(col >= 2, 1, 0)
    bx = col - 2 * by
    other = 1 - row
    g0, g1, g2, d0, d1, d2 = (planes.at[k] for k in range(6))
    col_x = col + 1 - 2 * bx
    col_y = col + 2 - 4 * by
    has_left = col > 0
    has_right = col < n_col - 1

    scope = None
    scope = mark(scope, "p_start")
    a_copies = [pltpu.make_async_copy(a_hbm.at[pl.ds(12 * q, 12)], av.at[pl.ds(12 * q, 12)], in_sem.at[q]) for q in range(4)]
    g_copy = pltpu.make_async_copy(g_hbm, g1.at[pl.ds(1, ROWS)], in_sem.at[4])
    x_copy = pltpu.make_async_copy(x_hbm, d1.at[pl.ds(1, ROWS)], in_sem.at[5])
    w2_copy = pltpu.make_async_copy(w2_hbm, w2, in_sem.at[6])
    w1_copy = pltpu.make_async_copy(w1_hbm, w1, in_sem.at[7])
    a_copies[0].start()
    g_copy.start()
    for q in range(1, 4):
        a_copies[q].start()
    x_copy.start()
    w2_copy.start()
    w1_copy.start()

    for buf in (lhg, rhg, lhd, rhd):
        buf[...] = jnp.zeros_like(buf)
    for buf in (g1, d1):
        buf[0] = jnp.zeros((COLS, CH), BF16)
        buf[ROWS + 1] = jnp.zeros((COLS, CH), BF16)

    scope = mark(scope, "p_barrier")
    barrier = pltpu.get_barrier_semaphore()
    for dc in range(n_col):
        for dr in range(n_row):
            if dc or dr:
                pl.semaphore_signal(barrier, inc=1, device_id={"col": lax.rem(col + dc, n_col), "row": lax.rem(row + dr, n_row)}, device_id_type=MESH)
    pl.semaphore_wait(barrier, n_col * n_row - 1)

    def frame_copies(which, plane, cl, cr, lh, rh):
        def remote(src, dst, k, dev):
            return pltpu.make_async_remote_copy(src_ref=src, dst_ref=dst, send_sem=hs_sem.at[which, k], recv_sem=hr_sem.at[which, k], device_id=dev, device_id_type=MESH)

        left = jnp.maximum(col - 1, 0)
        right = jnp.minimum(col + 1, n_col - 1)
        src8 = pl.multiple_of(40 * other, 8)
        dst8 = pl.multiple_of(56 * row, 8)
        pair = remote(plane.at[ROWS - (ROWS - 1) * row], plane.at[(ROWS + 1) * row], 0, {"col": col, "row": other})
        to_left = [remote(cl, rh.at[pl.ds(8, ROWS)], 1, {"col": left, "row": row}), remote(cl.at[pl.ds(src8, 8)], rh.at[pl.ds(dst8, 8)], 2, {"col": left, "row": other})]
        to_right = [remote(cr, lh.at[pl.ds(8, ROWS)], 3, {"col": right, "row": row}), remote(cr.at[pl.ds(src8, 8)], lh.at[pl.ds(dst8, 8)], 4, {"col": right, "row": other})]
        return pair, to_left, to_right

    def frame_send(copies):
        pair, to_left, to_right = copies
        pair.start()

        @pl.when(has_left)
        def _():
            for c in to_left:
                c.start()

        @pl.when(has_right)
        def _():
            for c in to_right:
                c.start()

    def frame_wait(copies, columns_only=False):
        pair, to_left, to_right = copies
        if not columns_only:
            pair.wait_recv()

        @pl.when(has_right)
        def _():
            for c in to_left:
                c.wait_recv()

        @pl.when(has_left)
        def _():
            for c in to_right:
                c.wait_recv()

    def frame_done(copies):
        pair, to_left, to_right = copies
        pair.wait_send()

        @pl.when(has_left)
        def _():
            for c in to_left:
                c.wait_send()

        @pl.when(has_right)
        def _():
            for c in to_right:
                c.wait_send()

    def result_of(u, first):
        v = u if first else u - TAPS
        if isinstance(v, int):
            tap_row, tap_col = TAP_ORDER[v % TAPS]
        else:
            tap_row = jnp.where(v < 1, 1, jnp.where(v < 3, 2 * (v - 1), jnp.where(v < 6, v - 3, v - 6)))
            tap_col = jnp.where(v < 3, 1, jnp.where(v < 6, 0, 2))
        return dw2 if first else dw1, 3 * tap_row + tap_col

    def unit_copies(u, j, first):
        half = 128 * row
        p_base, q_base = half, half + 64
        p_mine, q_mine = p_base + 32 * bx, q_base + 32 * by
        p_last, q_last = p_mine + 16 * by, q_mine + 16 * bx

        result, tap = result_of(u, first)

        def rows(ref, start, size):
            return ref.at[u, pl.ds(pl.multiple_of(start, 16), size)]

        def done(start, size):
            return result.at[tap, pl.ds(pl.multiple_of(start, 16), size)]

        def remote(src, dst, k, dev):
            return pltpu.make_async_remote_copy(src_ref=src, dst_ref=dst, send_sem=as_sem.at[u, k], recv_sem=ar_sem.at[u, k], device_id=dev, device_id_type=MESH)

        core = {"col": col, "row": other}
        dev_x = {"col": col_x, "row": row}
        dev_y = {"col": col_y, "row": row}
        if j == 0:
            return [remote(rows(acc, 128 * other, 128), r0.at[u], 0, core)]
        if j in (7, 8):
            mine = half + 32 * col
            peers = ((col_x, rows(r1, 0, 32)), (col_y, rows(r1, 32, 32)), (3 - col, rows(r2, 0, 32)))
            if j == 7:
                return [remote(rows(acc, half + 32 * peer, 32), slot, 1 + k, {"col": peer, "row": row}) for k, (peer, slot) in enumerate(peers)]
            return [remote(done(mine, 32), done(mine, 32), 4 + k, {"col": peer, "row": row}) for k, (peer, _) in enumerate(peers)]
        if j == 1:
            return [remote(rows(acc, p_base + 32 * (1 - bx), 32), rows(r1, 0, 32), 1, dev_x), remote(rows(acc, q_base + 32 * (1 - by), 32), rows(r1, 32, 32), 2, dev_y)]
        if j == 2:
            return [remote(rows(acc, p_mine + 16 * (1 - by), 16), rows(r2, 0, 16), 3, dev_y), remote(rows(acc, q_mine + 16 * (1 - bx), 16), rows(r2, 16, 16), 4, dev_x)]
        if j == 3:
            return [remote(done(p_last, 16), done(p_last, 16), 5, dev_y), remote(done(q_last, 16), done(q_last, 16), 6, dev_x)]
        if j == 4:
            return [remote(done(p_mine, 32), done(p_mine, 32), 7, dev_x), remote(done(q_mine, 32), done(q_mine, 32), 8, dev_y)]
        return [remote(done(half, 128), done(half, 128), 9, core)]

    def add_rows(dst, where, u, start, size, src, src_start):
        at = pl.ds(pl.multiple_of(start, 16), size)
        dst[where, at, :] = acc[u, at, :] + src[u, pl.ds(src_start, size), :]

    def stage(u, j, first=None):
        first = u < TAPS if first is None else first
        result, tap = result_of(u, first)
        direct = isinstance(u, int) and u >= DIRECT
        with jax.named_scope(f"p_w{j}_{u}" if isinstance(u, int) else f"p_w{j}_dyn"):
            for c in unit_copies(u, {7: 0, 8: 7, 9: 8}.get(j, j - 1), first):
                c.wait_recv()
        half = 128 * row
        if j in (1, 7):
            add_rows(acc, u, u, half, 128, r0, 0)
        elif j == 2:
            add_rows(acc, u, u, half + 32 * bx, 32, r1, 0)
            add_rows(acc, u, u, half + 64 + 32 * by, 32, r1, 32)
        elif j == 3:
            add_rows(result, tap, u, half + 32 * bx + 16 * by, 16, r2, 0)
            add_rows(result, tap, u, half + 64 + 32 * by + 16 * bx, 16, r2, 16)
        elif j == 8:
            at = pl.ds(pl.multiple_of(half + 32 * col, 16), 32)
            result[tap, at, :] = (acc[u, at, :] + r1[u, 0:32, :]) + (r1[u, 32:64, :] + r2[u, 0:32, :])
        if j == 6:
            for k in (0, 7, 8, 5) if direct else range(6):
                for c in unit_copies(u, k, first):
                    c.wait_send()
        else:
            for c in unit_copies(u, {9: 5}.get(j, j), first):
                c.start()

    def run(plan):
        for j, u in plan:
            stage(u, j)

    def send_first(u):
        for c in unit_copies(u, 0, True):
            c.start()

    def tap_sum(lhs_t, plane, tap_row, fill=(), before=None):
        total = None
        blocks = SPAN // CH
        for q in range(CHUNKS):
            rhs = plane[pl.ds(2 - tap_row + STEP * q, STEP)].reshape(SPAN, CH)
            for m in range(blocks):
                for piece in fill[blocks * q + m::CHUNKS * blocks]:
                    piece()
                if before is not None and before[blocks * q + m] is not None:
                    before[blocks * q + m]()
                part = jnp.dot(lhs_t[blocks * q + m], rhs[CH * m:CH * (m + 1)], preferred_element_type=F32)
                total = part if total is None else total + part
        return total

    def shift_row(center, minus, plus, r, lh=None, rh=None):
        v = center[r]
        first = v[:1] if lh is None else lh[pl.ds(r + 7, 1), :].astype(BF16)
        last = v[:1] if rh is None else rh[pl.ds(r + 7, 1), :].astype(BF16)
        minus[r] = jnp.concatenate([first, v[:COLS - 1]], axis=0)
        plus[r] = jnp.concatenate([v[1:], last], axis=0)

    def mend_row(minus, plus, r, lh, rh):
        at = lax.broadcasted_iota(jnp.int32, (8, CH), 0)
        minus[r, 0:8] = jnp.where(at == 0, lh[pl.ds(r + 7, 1), :], minus[r, 0:8].astype(F32)).astype(BF16)
        plus[r, COLS - 8:COLS] = jnp.where(at == 7, rh[pl.ds(r + 7, 1), :], plus[r, COLS - 8:COLS].astype(F32)).astype(BF16)

    def conv_pair(planes, w, i, fill=()):
        totals = [None, None]
        for k in range(TAPS):
            for n in range(2):
                lhs = planes[k % 3][pl.ds(STEP * (2 * i + n) + 2 - k // 3, STEP)].reshape(SPAN, CH)
                part = lax.dot_general(lhs, w[k], (((1,), (1,)), ((), ())), preferred_element_type=F32)
                totals[n] = part if k == 0 else totals[n] + part
            for piece in fill[len(fill) * k // TAPS:len(fill) * (k + 1) // TAPS]:
                piece()
        return totals

    def z_pieces(i):
        def one(m):
            for half in range(2):
                at = CH * m + 128 * half
                z = jax.nn.gelu(av[pl.ds(STEP * i, STEP)].reshape(SPAN, CH)[at:at + 128].astype(F32), approximate=True).astype(BF16)
                zt[SPAN // CH * i + m, :, 128 * half:128 * half + 128] = z.T

        return [functools.partial(one, m) for m in range(SPAN // CH)]

    def z_chunk(i):
        z = jax.nn.gelu(av[pl.ds(STEP * i, STEP)].reshape(SPAN, CH).astype(F32), approximate=True).astype(BF16)
        for m in range(SPAN // CH):
            zt[SPAN // CH * i + m] = z[CH * m:CH * (m + 1)].T

    def x_chunk(i):
        x = d1[pl.ds(1 + STEP * i, STEP)].reshape(SPAN, CH)
        for m in range(SPAN // CH):
            xt[SPAN // CH * i + m] = x[CH * m:CH * (m + 1)].T

    def z_loop(lo, hi):
        lax.fori_loop(lo, hi, lambda i, c: (z_chunk(i), c)[1], 0)

    scope = mark(scope, "p_z1")
    a_copies[0].wait()
    z_loop(0, 3)
    scope = mark(scope, "p_gwait")
    g_copy.wait()

    def g_edge(i, c):
        for k in range(8):
            r = 8 * i + k
            clg[pl.ds(r, 1), :] = g1[r + 1, 0:8, :].astype(F32)[0:1]
            crg[pl.ds(r, 1), :] = g1[r + 1, COLS - 8:COLS, :].astype(F32)[7:8]
        return c

    lax.fori_loop(0, ROWS // 8, g_edge, 0)
    g_frame = frame_copies(0, g1, clg, crg, lhg, rhg)
    frame_send(g_frame)
    a_copies[1].wait()
    z_loop(3, 6)
    for q in range(2, 4):
        a_copies[q].wait()

    scope = mark(scope, "p_s0")
    acc[0] = tap_sum(zt, g1, 1, before=[piece for i in range(CHUNKS) for piece in (z_pieces(i) if i >= 6 else [None] * 3)])
    send_first(0)
    scope = mark(scope, "p_fwg")
    frame_wait(g_frame)

    scope = mark(scope, "p_mid")
    for i in range(2):
        @pl.when(row >= 0)
        def _(i=i):
            acc[1 + i] = tap_sum(zt, g1, 2 * i, [functools.partial(shift_row, g1, g2, g0, 25 * i + k, lhg, rhg) for k in range(25)])

        send_first(1 + i)
        stage(i, 1)

    scope = mark(scope, "p_xw")
    x_copy.wait()

    def w2_left(i, c):
        x_chunk(2 * i)
        x_chunk(2 * i + 1)
        acc[3 + i] = tap_sum(zt, g0, i)
        send_first(3 + i)
        stage(2 + i, 1, True)
        stage(i, 2, True)
        return c

    def w2_right(i, c):
        x_chunk(6 + 2 * i)
        x_chunk(6 + 2 * i + 1)
        acc[6 + i] = tap_sum(zt, g2, i)
        send_first(6 + i)
        stage(5 + i, 1, True)
        stage(3 + i, 2, True)
        stage(i, 3, True)
        return c

    scope = mark(scope, "p_left")
    lax.fori_loop(0, 3, w2_left, 0)
    scope = mark(scope, "p_right")
    lax.fori_loop(0, 3, w2_right, 0)

    w2_copy.wait()
    g_planes = (g0, g1, g2)

    def da_chunk(i, dz):
        part = COLS // PARTS

        def one(k, third):
            r, at = STEP * i + k, part * third
            a_val = av[r, at:at + part].astype(F32)
            d_a = (dz[COLS * k + at:COLS * k + at + part] * gelu_slope(a_val)).astype(BF16)
            d1[1 + r, at:at + part] = d_a
            if third == 0:
                cld[pl.ds(r, 1), :] = d_a[0:8].astype(F32)[0:1]
            if third == PARTS - 1:
                crd[pl.ds(r, 1), :] = d_a[part - 8:].astype(F32)[7:8]

        pieces = []
        for k in range(STEP):
            pieces += [functools.partial(one, k, third) for third in range(PARTS)]
            pieces.append(functools.partial(shift_row, d1, d2, d0, 1 + STEP * i + k))
        return pieces

    dza, dzb = dzs.at[0], dzs.at[1]

    def dz_store(pair):
        dza[...], dzb[...] = pair

    def run_at(i, plans):
        for k, plan in enumerate(plans):
            @pl.when(i == k)
            def _(plan=plan):
                run(plan)

    def dz_step(i, c):
        dz_store(conv_pair(g_planes, w2, i, da_chunk(2 * i - 2, dza) + da_chunk(2 * i - 1, dzb)))
        run_at(i - 1, DZ_PLAN[1:])
        return c

    scope = mark(scope, "p_dz0")
    dz_store(conv_pair(g_planes, w2, 0))
    run(DZ_PLAN[0])
    scope = mark(scope, "p_dz")
    lax.fori_loop(1, CHUNKS // 2, dz_step, 0)

    d_frame = frame_copies(1, d1, cld, crd, lhd, rhd)
    def da_last(i, c):
        for piece in da_chunk(CHUNKS - 2 + i, dzs.at[i]):
            piece()
        return c

    scope = mark(scope, "p_dal")
    lax.fori_loop(0, 2, da_last, 0)
    frame_send(d_frame)
    scope = mark(scope, "p_s9")
    acc[9] = tap_sum(xt, d1, 1)
    send_first(9)
    scope = mark(scope, "p_s9plan")
    run(W1_PLAN[0])
    scope = mark(scope, "p_fwd0")
    d_frame[0].wait_recv()

    @pl.when(row >= 0)
    def _():
        acc[10] = tap_sum(xt, d1, 0)

    send_first(10)
    run(W1_PLAN[1])

    @pl.when(row >= 0)
    def _():
        acc[11] = tap_sum(xt, d1, 2)

    send_first(11)
    run(W1_PLAN[2])
    scope = mark(scope, "p_fwd1")
    frame_wait(d_frame, True)
    scope = mark(scope, "p_mend")
    shift_row(d1, d2, d0, 0, lhd, rhd)
    shift_row(d1, d2, d0, ROWS + 1, lhd, rhd)

    def mend(i, c):
        for k in range(8):
            mend_row(d2, d0, 1 + 8 * i + k, lhd, rhd)
        return c

    lax.fori_loop(0, ROWS // 8, mend, 0)

    w1_copy.wait()
    d_planes = (d0, d1, d2)

    def dx_pair(i):
        for n, total in enumerate(conv_pair(d_planes, w1, i)):
            at = STEP * (2 * i + n)
            total = total + g1[pl.ds(1 + at, STEP)].reshape(SPAN, CH).astype(F32)
            av[pl.ds(at, STEP)] = total.astype(BF16).reshape(STEP, COLS, CH)

    @pl.when(row >= 0)
    def _():
        dx_pair(0)

    run(W1_PLAN[3])

    def w1_left(i, c):
        acc[12 + i] = tap_sum(xt, d0, i)
        send_first(12 + i)
        run_at(i, W1_PLAN[4:7])
        return c

    def w1_right(i, c):
        acc[15 + i] = tap_sum(xt, d2, i)
        send_first(15 + i)
        run_at(i, W1_PLAN[7:10])
        return c

    scope = mark(scope, "p_w1l")
    lax.fori_loop(0, 3, w1_left, 0)
    scope = mark(scope, "p_w1r")
    lax.fori_loop(0, 3, w1_right, 0)

    def dx_step(i, c):
        dx_pair(i)
        run_at(i - 1, DX_PLAN[:CHUNKS // 2 - 1])
        return c

    lax.fori_loop(1, CHUNKS // 2, dx_step, 0)
    run(DX_PLAN[CHUNKS // 2 - 1])

    scope = mark(scope, "p_done")
    frame_done(g_frame)
    frame_done(d_frame)
    mark(scope, None)

def write_out(*refs):
    sem = refs[-1]
    copies = [pltpu.make_async_copy(src, dst, sem.at[k]) for k, (src, dst) in enumerate(zip(refs[:3], refs[3:6]))]
    for c in copies:
        c.start()
    for c in copies:
        c.wait()


def solution(mesh):
    n_row, n_col = mesh.shape["row"], mesh.shape["col"]

    def local_step(x_tile, a_tile, g_tile, w_one, w_two):
        units = 2 * TAPS
        hbm = pl.BlockSpec(memory_space=pl.ANY)
        frame = pltpu.VMEM((64, CH), F32)
        edge = pltpu.VMEM((ROWS, CH), F32)
        d_x, d_w1, d_w2 = pl.pallas_call(
            functools.partial(kernel, n_row, n_col),
            out_shape=(
                pltpu.VMEM((ROWS, COLS, CH), BF16),
                pltpu.VMEM((TAPS, CH, CH), F32),
                pltpu.VMEM((TAPS, CH, CH), F32),
            ),
            in_specs=[hbm] * 5,
            out_specs=(pl.BlockSpec(memory_space=pltpu.VMEM),) * 3,
            scratch_shapes=[
                pltpu.VMEM((6, ROWS + 2, COLS, CH), BF16),
                pltpu.VMEM((PIX // CH, CH, CH), BF16),
                pltpu.VMEM((PIX // CH, CH, CH), BF16),
                pltpu.VMEM((TAPS, CH, CH), BF16),
                pltpu.VMEM((TAPS, CH, CH), BF16),
                pltpu.VMEM((units, CH, CH), F32),
                pltpu.VMEM((units, 128, CH), F32),
                pltpu.VMEM((units, 64, CH), F32),
                pltpu.VMEM((units, 32, CH), F32),
                pltpu.VMEM((2, SPAN, CH), F32),
                frame, frame, frame, frame,
                edge, edge, edge, edge,
                pltpu.SemaphoreType.DMA((8,)),
                pltpu.SemaphoreType.DMA((2, 5)),
                pltpu.SemaphoreType.DMA((2, 5)),
                pltpu.SemaphoreType.DMA((units, 10)),
                pltpu.SemaphoreType.DMA((units, 10)),
            ],
            compiler_params=pltpu.CompilerParams(collective_id=0, has_side_effects=True, vmem_limit_bytes=VMEM_LIMIT),
        )(x_tile[0], a_tile[0], g_tile[0], w_one.reshape(TAPS, CH, CH), w_two.reshape(TAPS, CH, CH))
        held = [pltpu.with_memory_space_constraint(r, pltpu.VMEM) for r in (d_x, d_w1, d_w2)]
        d_x, d_w1, d_w2 = pl.pallas_call(
            write_out,
            out_shape=tuple(jax.ShapeDtypeStruct(r.shape, r.dtype) for r in (d_x, d_w1, d_w2)),
            in_specs=[pl.BlockSpec(memory_space=pltpu.VMEM)] * 3,
            out_specs=(hbm,) * 3,
            scratch_shapes=[pltpu.SemaphoreType.DMA((3,))],
            compiler_params=pltpu.CompilerParams(vmem_limit_bytes=2**20),
        )(*held)
        shape = (3, 3, CH, CH)
        return d_x[None], d_w1.reshape(shape), d_w2.reshape(shape)

    tile_spec = P(None, "row", "col", None)
    return jax.shard_map(local_step, mesh=mesh, in_specs=(tile_spec, tile_spec, tile_spec, P(), P()), out_specs=(tile_spec, P(), P()), check_vma=False)
```

```python
import functools

import jax
import jax.numpy as jnp
from jax import lax
from jax.experimental import pallas as pl
from jax.experimental.pallas import tpu as pltpu
from jax.sharding import PartitionSpec as P

MESH = pl.DeviceIdType.MESH
F32 = jnp.float32
BF16 = jnp.bfloat16
CH = 256
ROWS = 48
COLS = 192
PIX = ROWS * COLS
VMEM_LIMIT = 56000 * 2**10
PARTS = 12
STEP = 4
SPAN = STEP * COLS
CHUNKS = ROWS // STEP
TAPS = 9
TAP_ORDER = ((1, 1), (0, 1), (2, 1), (0, 0), (1, 0), (2, 0), (0, 2), (1, 2), (2, 2))
TAP_ORDER_TWO = ((1, 1), (0, 1), (2, 1), (0, 0), (0, 2), (1, 0), (1, 2), (2, 0), (2, 2))
W2_PLAN = (
    ((1, 2), (2, 0)),
    ((1, 3), (1, 4), (2, 1), (2, 2)),
    ((1, 5), (1, 6), (2, 3), (3, 0)),
)
DZ_PLAN = (
    ((1, 7), (1, 8), (2, 4), (2, 5), (3, 1), (3, 2)),
    ((2, 6), (3, 3), (4, 0), (4, 1)),
    ((2, 7), (2, 8), (3, 4), (3, 5), (4, 2)),
    ((3, 6), (4, 3), (4, 4), (5, 0), (5, 1)),
    ((3, 7), (3, 8), (4, 5), (5, 2), (6, 0)),
    ((4, 6), (5, 3), (5, 4), (6, 1)),
)
W1_PLAN = (
    ((4, 7), (4, 8), (5, 5), (6, 2)),
    ((1, 9), (5, 6), (6, 3), (6, 4)),
    ((1, 10), (6, 5)),
    ((1, 11), (2, 9), (2, 10), (5, 7), (5, 8), (6, 6)),
    (),
    ((2, 11), (1, 12), (3, 9), (6, 7)),
    ((3, 10), (1, 13), (6, 8)),
    ((3, 11), (2, 12), (1, 14), (4, 9)),
    ((2, 13), (1, 15), (4, 10)),
    ((3, 12), (2, 14), (1, 16), (4, 11)),
)
DX_PLAN = (
    ((3, 13), (2, 15), (7, 17), (5, 9), (5, 10)),
    ((3, 14), (4, 12), (2, 16), (3, 15), (5, 11), (6, 9)),
    ((4, 13), (8, 17), (3, 16), (6, 10)),
    ((4, 14), (4, 15), (5, 12), (4, 16), (6, 11)),
    ((5, 13), (9, 17), (6, 12)),
    ((5, 14), (5, 15), (5, 16), (6, 13), (6, 17), (6, 14), (6, 15), (6, 16)),
)
DIRECT = 17


def gelu_slope(a):
    scale = 0.7978845608028654
    square = (scale * 0.044715 * a) * a
    tanh_val = jnp.tanh(a * (scale + square))
    return (0.5 + 0.5 * tanh_val) + (0.5 * a * (1.0 - tanh_val * tanh_val)) * (scale + 3.0 * square)


def kernel(n_row, n_col, x_hbm, a_hbm, g_hbm, w1_hbm, w2_hbm, av, dw1, dw2,
           planes, zt, xt, w1, w2, acc, r0, r1, r2, dzs,
           lhg, rhg, lhd, rhd, clg, crg, cld, crd,
           in_sem, hs_sem, hr_sem, as_sem, ar_sem):
    row = lax.axis_index("row")
    col = lax.axis_index("col")
    by = jnp.where(col >= 2, 1, 0)
    bx = col - 2 * by
    other = 1 - row
    g0, g1, g2, d0, d1, d2 = (planes.at[k] for k in range(6))
    col_x = col + 1 - 2 * bx
    col_y = col + 2 - 4 * by
    has_left = col > 0
    has_right = col < n_col - 1

    a_copies = [pltpu.make_async_copy(a_hbm.at[pl.ds(12 * q, 12)], av.at[pl.ds(12 * q, 12)], in_sem.at[q]) for q in range(4)]
    g_copy = pltpu.make_async_copy(g_hbm, g1.at[pl.ds(1, ROWS)], in_sem.at[4])
    x_copy = pltpu.make_async_copy(x_hbm, d1.at[pl.ds(1, ROWS)], in_sem.at[5])
    w2_copy = pltpu.make_async_copy(w2_hbm, w2, in_sem.at[6])
    w1_copy = pltpu.make_async_copy(w1_hbm, w1, in_sem.at[7])
    a_copies[0].start()
    g_copy.start()
    for q in range(1, 4):
        a_copies[q].start()
    x_copy.start()
    w2_copy.start()
    w1_copy.start()

    for buf in (lhg, rhg, lhd, rhd):
        buf[...] = jnp.zeros_like(buf)
    for buf in (g1, d1):
        buf[0] = jnp.zeros((COLS, CH), BF16)
        buf[ROWS + 1] = jnp.zeros((COLS, CH), BF16)

    barrier = pltpu.get_barrier_semaphore()
    for dc in range(n_col):
        for dr in range(n_row):
            if dc or dr:
                pl.semaphore_signal(barrier, inc=1, device_id={"col": lax.rem(col + dc, n_col), "row": lax.rem(row + dr, n_row)}, device_id_type=MESH)
    pl.semaphore_wait(barrier, n_col * n_row - 1)

    def frame_copies(which, plane, cl, cr, lh, rh):
        def remote(src, dst, k, dev):
            return pltpu.make_async_remote_copy(src_ref=src, dst_ref=dst, send_sem=hs_sem.at[which, k], recv_sem=hr_sem.at[which, k], device_id=dev, device_id_type=MESH)

        left = jnp.maximum(col - 1, 0)
        right = jnp.minimum(col + 1, n_col - 1)
        src8 = pl.multiple_of(40 * other, 8)
        dst8 = pl.multiple_of(56 * row, 8)
        pair = remote(plane.at[ROWS - (ROWS - 1) * row], plane.at[(ROWS + 1) * row], 0, {"col": col, "row": other})
        to_left = [remote(cl, rh.at[pl.ds(8, ROWS)], 1, {"col": left, "row": row}), remote(cl.at[pl.ds(src8, 8)], rh.at[pl.ds(dst8, 8)], 2, {"col": left, "row": other})]
        to_right = [remote(cr, lh.at[pl.ds(8, ROWS)], 3, {"col": right, "row": row}), remote(cr.at[pl.ds(src8, 8)], lh.at[pl.ds(dst8, 8)], 4, {"col": right, "row": other})]
        return pair, to_left, to_right

    def frame_send(copies):
        pair, to_left, to_right = copies
        pair.start()

        @pl.when(has_left)
        def _():
            for c in to_left:
                c.start()

        @pl.when(has_right)
        def _():
            for c in to_right:
                c.start()

    def frame_wait(copies, columns_only=False):
        pair, to_left, to_right = copies
        if not columns_only:
            pair.wait_recv()

        @pl.when(has_right)
        def _():
            for c in to_left:
                c.wait_recv()

        @pl.when(has_left)
        def _():
            for c in to_right:
                c.wait_recv()

    def frame_done(copies):
        pair, to_left, to_right = copies
        pair.wait_send()

        @pl.when(has_left)
        def _():
            for c in to_left:
                c.wait_send()

        @pl.when(has_right)
        def _():
            for c in to_right:
                c.wait_send()

    def result_of(u, first):
        tap_row, tap_col = (TAP_ORDER_TWO if first else TAP_ORDER)[u % TAPS]
        return dw2 if first else dw1, 3 * tap_row + tap_col

    def unit_copies(u, j, first):
        half = 128 * row
        p_base, q_base = half, half + 64
        p_mine, q_mine = p_base + 32 * bx, q_base + 32 * by
        p_last, q_last = p_mine + 16 * by, q_mine + 16 * bx

        result, tap = result_of(u, first) if j else (None, None)

        def rows(ref, start, size):
            return ref.at[u, pl.ds(pl.multiple_of(start, 16), size)]

        def done(start, size):
            return result.at[tap, pl.ds(pl.multiple_of(start, 16), size)]

        def remote(src, dst, k, dev):
            return pltpu.make_async_remote_copy(src_ref=src, dst_ref=dst, send_sem=as_sem.at[u, k], recv_sem=ar_sem.at[u, k], device_id=dev, device_id_type=MESH)

        core = {"col": col, "row": other}
        dev_x = {"col": col_x, "row": row}
        dev_y = {"col": col_y, "row": row}
        if j == 0:
            return [remote(rows(acc, 128 * other, 128), r0.at[u], 0, core)]
        if j in (7, 8):
            mine = half + 32 * col
            peers = ((col_x, rows(r1, 0, 32)), (col_y, rows(r1, 32, 32)), (3 - col, rows(r2, 0, 32)))
            if j == 7:
                return [remote(rows(acc, half + 32 * peer, 32), slot, 1 + k, {"col": peer, "row": row}) for k, (peer, slot) in enumerate(peers)]
            return [remote(done(mine, 32), done(mine, 32), 4 + k, {"col": peer, "row": row}) for k, (peer, _) in enumerate(peers)]
        if j == 1:
            return [remote(rows(acc, p_base + 32 * (1 - bx), 32), rows(r1, 0, 32), 1, dev_x), remote(rows(acc, q_base + 32 * (1 - by), 32), rows(r1, 32, 32), 2, dev_y)]
        if j == 2:
            return [remote(rows(acc, p_mine + 16 * (1 - by), 16), rows(r2, 0, 16), 3, dev_y), remote(rows(acc, q_mine + 16 * (1 - bx), 16), rows(r2, 16, 16), 4, dev_x)]
        if j == 3:
            return [remote(done(p_last, 16), done(p_last, 16), 5, dev_y), remote(done(q_last, 16), done(q_last, 16), 6, dev_x)]
        if j == 4:
            return [remote(done(p_mine, 32), done(p_mine, 32), 7, dev_x), remote(done(q_mine, 32), done(q_mine, 32), 8, dev_y)]
        return [remote(done(half, 128), done(half, 128), 9, core)]

    def add_rows(dst, where, u, start, size, src, src_start):
        at = pl.ds(pl.multiple_of(start, 16), size)
        dst[where, at, :] = acc[u, at, :] + src[u, pl.ds(src_start, size), :]

    def stage(u, j, first=None):
        first = u < TAPS if first is None else first
        result, tap = result_of(u, first)
        direct = isinstance(u, int) and u >= DIRECT
        for c in unit_copies(u, {7: 0, 8: 7, 9: 8}.get(j, j - 1), first):
            c.wait_recv()
        half = 128 * row
        if j in (1, 7):
            add_rows(acc, u, u, half, 128, r0, 0)
        elif j == 2:
            add_rows(acc, u, u, half + 32 * bx, 32, r1, 0)
            add_rows(acc, u, u, half + 64 + 32 * by, 32, r1, 32)
        elif j == 3:
            add_rows(result, tap, u, half + 32 * bx + 16 * by, 16, r2, 0)
            add_rows(result, tap, u, half + 64 + 32 * by + 16 * bx, 16, r2, 16)
        elif j == 8:
            at = pl.ds(pl.multiple_of(half + 32 * col, 16), 32)
            result[tap, at, :] = (acc[u, at, :] + r1[u, 0:32, :]) + (r1[u, 32:64, :] + r2[u, 0:32, :])
        if j == 6:
            for k in (0, 7, 8, 5) if direct else range(6):
                for c in unit_copies(u, k, first):
                    c.wait_send()
        else:
            for c in unit_copies(u, {9: 5}.get(j, j), first):
                c.start()

    def run(plan):
        for j, u in plan:
            stage(u, j)

    def run_at(i, plans):
        for k, plan in enumerate(plans):
            @pl.when(i == k)
            def _(plan=plan):
                run(plan)

    def send_first(u):
        for c in unit_copies(u, 0, True):
            c.start()

    def tap_sum(lhs_t, plane, tap_row, fill=(), before=None):
        total = None
        blocks = SPAN // CH
        for q in range(CHUNKS):
            rhs = plane[pl.ds(2 - tap_row + STEP * q, STEP)].reshape(SPAN, CH)
            for m in range(blocks):
                for piece in fill[blocks * q + m::CHUNKS * blocks]:
                    piece()
                if before is not None and before[blocks * q + m] is not None:
                    before[blocks * q + m]()
                part = jnp.dot(lhs_t[blocks * q + m], rhs[CH * m:CH * (m + 1)], preferred_element_type=F32)
                total = part if total is None else total + part
        return total

    def tap_pair(lhs_t, pair, tap_row):
        totals = [None, None]
        blocks = SPAN // CH
        for q in range(CHUNKS):
            for m in range(blocks):
                for n in range(2):
                    rhs = pair[n][pl.ds(2 - tap_row + STEP * q, STEP)].reshape(SPAN, CH)[CH * m:CH * (m + 1)]
                    part = jnp.dot(lhs_t[blocks * q + m], rhs, preferred_element_type=F32)
                    totals[n] = part if totals[n] is None else totals[n] + part
        return totals

    def shift_row(center, minus, plus, r, lh=None, rh=None):
        v = center[r]
        first = v[:1] if lh is None else lh[pl.ds(r + 7, 1), :].astype(BF16)
        last = v[:1] if rh is None else rh[pl.ds(r + 7, 1), :].astype(BF16)
        minus[r] = jnp.concatenate([first, v[:COLS - 1]], axis=0)
        plus[r] = jnp.concatenate([v[1:], last], axis=0)

    def mend_row(minus, plus, r, lh, rh):
        at = lax.broadcasted_iota(jnp.int32, (8, CH), 0)
        minus[r, 0:8] = jnp.where(at == 0, lh[pl.ds(r + 7, 1), :], minus[r, 0:8].astype(F32)).astype(BF16)
        plus[r, COLS - 8:COLS] = jnp.where(at == 7, rh[pl.ds(r + 7, 1), :], plus[r, COLS - 8:COLS].astype(F32)).astype(BF16)

    def conv_pair(planes, w, i, fill=()):
        totals = [None, None]
        for k in range(TAPS):
            for n in range(2):
                lhs = planes[k % 3][pl.ds(STEP * (2 * i + n) + 2 - k // 3, STEP)].reshape(SPAN, CH)
                part = lax.dot_general(lhs, w[k], (((1,), (1,)), ((), ())), preferred_element_type=F32)
                totals[n] = part if k == 0 else totals[n] + part
            for piece in fill[len(fill) * k // TAPS:len(fill) * (k + 1) // TAPS]:
                piece()
        return totals

    def z_pieces(i):
        def one(m):
            for half in range(2):
                at = CH * m + 128 * half
                z = jax.nn.gelu(av[pl.ds(STEP * i, STEP)].reshape(SPAN, CH)[at:at + 128].astype(F32), approximate=True).astype(BF16)
                zt[SPAN // CH * i + m, :, 128 * half:128 * half + 128] = z.T

        return [functools.partial(one, m) for m in range(SPAN // CH)]

    def z_chunk(i):
        z = jax.nn.gelu(av[pl.ds(STEP * i, STEP)].reshape(SPAN, CH).astype(F32), approximate=True).astype(BF16)
        for m in range(SPAN // CH):
            zt[SPAN // CH * i + m] = z[CH * m:CH * (m + 1)].T

    def x_chunk(i):
        x = d1[pl.ds(1 + STEP * i, STEP)].reshape(SPAN, CH)
        for m in range(SPAN // CH):
            xt[SPAN // CH * i + m] = x[CH * m:CH * (m + 1)].T

    def z_loop(lo, hi):
        lax.fori_loop(lo, hi, lambda i, c: (z_chunk(i), c)[1], 0)

    a_copies[0].wait()
    z_loop(0, 3)
    g_copy.wait()

    def g_edge(i, c):
        for k in range(8):
            r = 8 * i + k
            clg[pl.ds(r, 1), :] = g1[r + 1, 0:8, :].astype(F32)[0:1]
            crg[pl.ds(r, 1), :] = g1[r + 1, COLS - 8:COLS, :].astype(F32)[7:8]
        return c

    lax.fori_loop(0, ROWS // 8, g_edge, 0)
    g_frame = frame_copies(0, g1, clg, crg, lhg, rhg)
    frame_send(g_frame)
    a_copies[1].wait()
    z_loop(3, 6)
    for q in range(2, 4):
        a_copies[q].wait()

    acc[0] = tap_sum(zt, g1, 1, before=[piece for i in range(CHUNKS) for piece in (z_pieces(i) if i >= 6 else [None] * 3)])
    send_first(0)
    frame_wait(g_frame)

    for i in range(2):
        @pl.when(row >= 0)
        def _(i=i):
            acc[1 + i] = tap_sum(zt, g1, 2 * i, [functools.partial(shift_row, g1, g2, g0, 25 * i + k, lhg, rhg) for k in range(25)])

        send_first(1 + i)
        stage(i, 1)

    x_copy.wait()

    def w2_side(i, c):
        for k in range(4):
            x_chunk(4 * i + k)
        totals = tap_pair(zt, (g0, g2), i)
        acc[3 + 2 * i] = totals[0]
        acc[4 + 2 * i] = totals[1]
        send_first(3 + 2 * i)
        send_first(4 + 2 * i)
        run_at(i, W2_PLAN)
        return c

    lax.fori_loop(0, 3, w2_side, 0)

    w2_copy.wait()
    g_planes = (g0, g1, g2)

    def da_chunk(i, dz):
        part = COLS // PARTS

        def one(k, third):
            r, at = STEP * i + k, part * third
            a_val = av[r, at:at + part].astype(F32)
            d_a = (dz[COLS * k + at:COLS * k + at + part] * gelu_slope(a_val)).astype(BF16)
            d1[1 + r, at:at + part] = d_a
            if third == 0:
                cld[pl.ds(r, 1), :] = d_a[0:8].astype(F32)[0:1]
            if third == PARTS - 1:
                crd[pl.ds(r, 1), :] = d_a[part - 8:].astype(F32)[7:8]

        pieces = []
        for k in range(STEP):
            pieces += [functools.partial(one, k, third) for third in range(PARTS)]
            pieces.append(functools.partial(shift_row, d1, d2, d0, 1 + STEP * i + k))
        return pieces

    dza, dzb = dzs.at[0], dzs.at[1]

    def dz_store(pair):
        dza[...], dzb[...] = pair

    def dz_step(i, c):
        dz_store(conv_pair(g_planes, w2, i, da_chunk(2 * i - 2, dza) + da_chunk(2 * i - 1, dzb)))
        run_at(i - 1, DZ_PLAN[1:])
        return c

    dz_store(conv_pair(g_planes, w2, 0))
    run(DZ_PLAN[0])
    lax.fori_loop(1, CHUNKS // 2, dz_step, 0)

    d_frame = frame_copies(1, d1, cld, crd, lhd, rhd)
    def da_last(i, c):
        for piece in da_chunk(CHUNKS - 2 + i, dzs.at[i]):
            piece()
        return c

    lax.fori_loop(0, 2, da_last, 0)
    frame_send(d_frame)
    acc[9] = tap_sum(xt, d1, 1)
    send_first(9)
    run(W1_PLAN[0])
    d_frame[0].wait_recv()

    @pl.when(row >= 0)
    def _():
        acc[10] = tap_sum(xt, d1, 0)

    send_first(10)
    run(W1_PLAN[1])

    @pl.when(row >= 0)
    def _():
        acc[11] = tap_sum(xt, d1, 2)

    send_first(11)
    run(W1_PLAN[2])
    frame_wait(d_frame, True)
    shift_row(d1, d2, d0, 0, lhd, rhd)
    shift_row(d1, d2, d0, ROWS + 1, lhd, rhd)

    def mend(i, c):
        for k in range(8):
            mend_row(d2, d0, 1 + 8 * i + k, lhd, rhd)
        return c

    lax.fori_loop(0, ROWS // 8, mend, 0)

    w1_copy.wait()
    d_planes = (d0, d1, d2)

    def dx_pair(i):
        for n, total in enumerate(conv_pair(d_planes, w1, i)):
            at = STEP * (2 * i + n)
            total = total + g1[pl.ds(1 + at, STEP)].reshape(SPAN, CH).astype(F32)
            av[pl.ds(at, STEP)] = total.astype(BF16).reshape(STEP, COLS, CH)

    @pl.when(row >= 0)
    def _():
        dx_pair(0)

    run(W1_PLAN[3])

    def w1_left(i, c):
        acc[12 + i] = tap_sum(xt, d0, i)
        send_first(12 + i)
        run_at(i, W1_PLAN[4:7])
        return c

    def w1_right(i, c):
        acc[15 + i] = tap_sum(xt, d2, i)
        send_first(15 + i)
        run_at(i, W1_PLAN[7:10])
        return c

    lax.fori_loop(0, 3, w1_left, 0)
    lax.fori_loop(0, 3, w1_right, 0)

    def dx_step(i, c):
        dx_pair(i)
        run_at(i - 1, DX_PLAN[:CHUNKS // 2 - 1])
        return c

    lax.fori_loop(1, CHUNKS // 2, dx_step, 0)
    run(DX_PLAN[CHUNKS // 2 - 1])

    frame_done(g_frame)
    frame_done(d_frame)

def write_out(*refs):
    sem = refs[-1]
    copies = [pltpu.make_async_copy(src, dst, sem.at[k]) for k, (src, dst) in enumerate(zip(refs[:3], refs[3:6]))]
    for c in copies:
        c.start()
    for c in copies:
        c.wait()


def solution(mesh):
    n_row, n_col = mesh.shape["row"], mesh.shape["col"]

    def local_step(x_tile, a_tile, g_tile, w_one, w_two):
        units = 2 * TAPS
        hbm = pl.BlockSpec(memory_space=pl.ANY)
        frame = pltpu.VMEM((64, CH), F32)
        edge = pltpu.VMEM((ROWS, CH), F32)
        d_x, d_w1, d_w2 = pl.pallas_call(
            functools.partial(kernel, n_row, n_col),
            out_shape=(
                pltpu.VMEM((ROWS, COLS, CH), BF16),
                pltpu.VMEM((TAPS, CH, CH), F32),
                pltpu.VMEM((TAPS, CH, CH), F32),
            ),
            in_specs=[hbm] * 5,
            out_specs=(pl.BlockSpec(memory_space=pltpu.VMEM),) * 3,
            scratch_shapes=[
                pltpu.VMEM((6, ROWS + 2, COLS, CH), BF16),
                pltpu.VMEM((PIX // CH, CH, CH), BF16),
                pltpu.VMEM((PIX // CH, CH, CH), BF16),
                pltpu.VMEM((TAPS, CH, CH), BF16),
                pltpu.VMEM((TAPS, CH, CH), BF16),
                pltpu.VMEM((units, CH, CH), F32),
                pltpu.VMEM((units, 128, CH), F32),
                pltpu.VMEM((units, 64, CH), F32),
                pltpu.VMEM((units, 32, CH), F32),
                pltpu.VMEM((2, SPAN, CH), F32),
                frame, frame, frame, frame,
                edge, edge, edge, edge,
                pltpu.SemaphoreType.DMA((8,)),
                pltpu.SemaphoreType.DMA((2, 5)),
                pltpu.SemaphoreType.DMA((2, 5)),
                pltpu.SemaphoreType.DMA((units, 10)),
                pltpu.SemaphoreType.DMA((units, 10)),
            ],
            compiler_params=pltpu.CompilerParams(collective_id=0, has_side_effects=True, vmem_limit_bytes=VMEM_LIMIT),
        )(x_tile[0], a_tile[0], g_tile[0], w_one.reshape(TAPS, CH, CH), w_two.reshape(TAPS, CH, CH))
        held = [pltpu.with_memory_space_constraint(r, pltpu.VMEM) for r in (d_x, d_w1, d_w2)]
        d_x, d_w1, d_w2 = pl.pallas_call(
            write_out,
            out_shape=tuple(jax.ShapeDtypeStruct(r.shape, r.dtype) for r in (d_x, d_w1, d_w2)),
            in_specs=[pl.BlockSpec(memory_space=pltpu.VMEM)] * 3,
            out_specs=(hbm,) * 3,
            scratch_shapes=[pltpu.SemaphoreType.DMA((3,))],
            compiler_params=pltpu.CompilerParams(vmem_limit_bytes=2**20),
        )(*held)
        shape = (3, 3, CH, CH)
        return d_x[None], d_w1.reshape(shape), d_w2.reshape(shape)

    tile_spec = P(None, "row", "col", None)
    return jax.shard_map(local_step, mesh=mesh, in_specs=(tile_spec, tile_spec, tile_spec, P(), P()), out_specs=(tile_spec, P(), P()), check_vma=False)
```

```python
import functools

import jax
import jax.numpy as jnp
from jax import lax
from jax.experimental import pallas as pl
from jax.experimental.pallas import tpu as pltpu
from jax.sharding import PartitionSpec as P

MESH = pl.DeviceIdType.MESH
F32 = jnp.float32
BF16 = jnp.bfloat16
CH = 256
ROWS = 48
COLS = 192
PIX = ROWS * COLS
VMEM_LIMIT = 56000 * 2**10
PARTS = 12
STEP = 4
SPAN = STEP * COLS
CHUNKS = ROWS // STEP
TAPS = 9
TAP_ORDER = ((1, 1), (0, 1), (2, 1), (0, 0), (1, 0), (2, 0), (0, 2), (1, 2), (2, 2))
TAP_ORDER_TWO = ((1, 1), (0, 1), (2, 1), (0, 0), (0, 2), (1, 0), (1, 2), (2, 0), (2, 2))
W2_PLAN = (
    ((1, 2), (2, 0)),
    ((1, 3), (1, 4), (2, 1), (2, 2)),
    ((1, 5), (1, 6), (2, 3), (3, 0)),
)
DZ_PLAN = (
    ((1, 7), (1, 8), (2, 4), (2, 5), (3, 1), (3, 2)),
    ((2, 6), (3, 3), (4, 0), (4, 1)),
    ((2, 7), (2, 8), (3, 4), (3, 5), (4, 2)),
    ((3, 6), (4, 3), (4, 4), (5, 0), (5, 1)),
    ((3, 7), (3, 8), (4, 5), (5, 2), (6, 0)),
    ((4, 6), (5, 3), (5, 4), (6, 1)),
)
W1_PLAN = (
    ((4, 7), (4, 8), (5, 5), (6, 2)),
    ((1, 9), (5, 6), (6, 3), (6, 4)),
    ((1, 10), (6, 5)),
    ((1, 11), (2, 9), (2, 10), (5, 7), (5, 8), (6, 6)),
    (),
    ((2, 11), (1, 12), (3, 9), (6, 7)),
    ((3, 10), (1, 13), (6, 8)),
    ((3, 11), (2, 12), (1, 14), (4, 9)),
    ((2, 13), (7, 15), (4, 10)),
    ((3, 12), (2, 14), (7, 16), (4, 11)),
)
DX_PLAN = (
    ((3, 13), (7, 17), (5, 9), (5, 10), (8, 15)),
    ((3, 14), (4, 12), (8, 16), (5, 11), (6, 9)),
    ((4, 13), (8, 17), (6, 10)),
    ((4, 14), (9, 15), (5, 12), (6, 11)),
    ((5, 13), (9, 16), (9, 17), (6, 12)),
    ((5, 14), (6, 13), (6, 15), (6, 16), (6, 17), (6, 14)),
)
DIRECT = 15


def gelu_slope(a):
    scale = 0.7978845608028654
    square = (scale * 0.044715 * a) * a
    tanh_val = jnp.tanh(a * (scale + square))
    return (0.5 + 0.5 * tanh_val) + (0.5 * a * (1.0 - tanh_val * tanh_val)) * (scale + 3.0 * square)


def mark(scope, name):
    if scope is not None:
        scope.__exit__(None, None, None)
    if name is None:
        return None
    scope = jax.named_scope(name)
    scope.__enter__()
    return scope


def kernel(n_row, n_col, x_hbm, a_hbm, g_hbm, w1_hbm, w2_hbm, av, dw1, dw2,
           planes, zt, xt, w1, w2, acc, r0, r1, r2, dzs,
           lhg, rhg, lhd, rhd, clg, crg, cld, crd,
           in_sem, hs_sem, hr_sem, as_sem, ar_sem):
    row = lax.axis_index("row")
    col = lax.axis_index("col")
    by = jnp.where(col >= 2, 1, 0)
    bx = col - 2 * by
    other = 1 - row
    g0, g1, g2, d0, d1, d2 = (planes.at[k] for k in range(6))
    col_x = col + 1 - 2 * bx
    col_y = col + 2 - 4 * by
    has_left = col > 0
    has_right = col < n_col - 1

    scope = None
    scope = mark(scope, "p_start")
    a_copies = [pltpu.make_async_copy(a_hbm.at[pl.ds(12 * q, 12)], av.at[pl.ds(12 * q, 12)], in_sem.at[q]) for q in range(4)]
    g_copy = pltpu.make_async_copy(g_hbm, g1.at[pl.ds(1, ROWS)], in_sem.at[4])
    x_copy = pltpu.make_async_copy(x_hbm, d1.at[pl.ds(1, ROWS)], in_sem.at[5])
    w2_copy = pltpu.make_async_copy(w2_hbm, w2, in_sem.at[6])
    w1_copy = pltpu.make_async_copy(w1_hbm, w1, in_sem.at[7])
    a_copies[0].start()
    g_copy.start()
    for q in range(1, 4):
        a_copies[q].start()
    x_copy.start()
    w2_copy.start()
    w1_copy.start()

    for buf in (lhg, rhg, lhd, rhd):
        buf[...] = jnp.zeros_like(buf)
    for buf in (g1, d1):
        buf[0] = jnp.zeros((COLS, CH), BF16)
        buf[ROWS + 1] = jnp.zeros((COLS, CH), BF16)

    scope = mark(scope, "p_barrier")
    barrier = pltpu.get_barrier_semaphore()
    for dc in range(n_col):
        for dr in range(n_row):
            if dc or dr:
                pl.semaphore_signal(barrier, inc=1, device_id={"col": lax.rem(col + dc, n_col), "row": lax.rem(row + dr, n_row)}, device_id_type=MESH)
    pl.semaphore_wait(barrier, n_col * n_row - 1)

    def frame_copies(which, plane, cl, cr, lh, rh):
        def remote(src, dst, k, dev):
            return pltpu.make_async_remote_copy(src_ref=src, dst_ref=dst, send_sem=hs_sem.at[which, k], recv_sem=hr_sem.at[which, k], device_id=dev, device_id_type=MESH)

        left = jnp.maximum(col - 1, 0)
        right = jnp.minimum(col + 1, n_col - 1)
        src8 = pl.multiple_of(40 * other, 8)
        dst8 = pl.multiple_of(56 * row, 8)
        pair = remote(plane.at[ROWS - (ROWS - 1) * row], plane.at[(ROWS + 1) * row], 0, {"col": col, "row": other})
        to_left = [remote(cl, rh.at[pl.ds(8, ROWS)], 1, {"col": left, "row": row}), remote(cl.at[pl.ds(src8, 8)], rh.at[pl.ds(dst8, 8)], 2, {"col": left, "row": other})]
        to_right = [remote(cr, lh.at[pl.ds(8, ROWS)], 3, {"col": right, "row": row}), remote(cr.at[pl.ds(src8, 8)], lh.at[pl.ds(dst8, 8)], 4, {"col": right, "row": other})]
        return pair, to_left, to_right

    def frame_send(copies):
        pair, to_left, to_right = copies
        pair.start()

        @pl.when(has_left)
        def _():
            for c in to_left:
                c.start()

        @pl.when(has_right)
        def _():
            for c in to_right:
                c.start()

    def frame_wait(copies, columns_only=False):
        pair, to_left, to_right = copies
        if not columns_only:
            pair.wait_recv()

        @pl.when(has_right)
        def _():
            for c in to_left:
                c.wait_recv()

        @pl.when(has_left)
        def _():
            for c in to_right:
                c.wait_recv()

    def frame_done(copies):
        pair, to_left, to_right = copies
        pair.wait_send()

        @pl.when(has_left)
        def _():
            for c in to_left:
                c.wait_send()

        @pl.when(has_right)
        def _():
            for c in to_right:
                c.wait_send()

    def result_of(u, first):
        tap_row, tap_col = (TAP_ORDER_TWO if first else TAP_ORDER)[u % TAPS]
        return dw2 if first else dw1, 3 * tap_row + tap_col

    def unit_copies(u, j, first):
        half = 128 * row
        p_base, q_base = half, half + 64
        p_mine, q_mine = p_base + 32 * bx, q_base + 32 * by
        p_last, q_last = p_mine + 16 * by, q_mine + 16 * bx

        result, tap = result_of(u, first) if j else (None, None)

        def rows(ref, start, size):
            return ref.at[u, pl.ds(pl.multiple_of(start, 16), size)]

        def done(start, size):
            return result.at[tap, pl.ds(pl.multiple_of(start, 16), size)]

        def remote(src, dst, k, dev):
            return pltpu.make_async_remote_copy(src_ref=src, dst_ref=dst, send_sem=as_sem.at[u, k], recv_sem=ar_sem.at[u, k], device_id=dev, device_id_type=MESH)

        core = {"col": col, "row": other}
        dev_x = {"col": col_x, "row": row}
        dev_y = {"col": col_y, "row": row}
        if j == 0:
            return [remote(rows(acc, 128 * other, 128), r0.at[u], 0, core)]
        if j in (7, 8):
            mine = half + 32 * col
            peers = ((col_x, rows(r1, 0, 32)), (col_y, rows(r1, 32, 32)), (3 - col, rows(r2, 0, 32)))
            if j == 7:
                return [remote(rows(acc, half + 32 * peer, 32), slot, 1 + k, {"col": peer, "row": row}) for k, (peer, slot) in enumerate(peers)]
            return [remote(done(mine, 32), done(mine, 32), 4 + k, {"col": peer, "row": row}) for k, (peer, _) in enumerate(peers)]
        if j == 1:
            return [remote(rows(acc, p_base + 32 * (1 - bx), 32), rows(r1, 0, 32), 1, dev_x), remote(rows(acc, q_base + 32 * (1 - by), 32), rows(r1, 32, 32), 2, dev_y)]
        if j == 2:
            return [remote(rows(acc, p_mine + 16 * (1 - by), 16), rows(r2, 0, 16), 3, dev_y), remote(rows(acc, q_mine + 16 * (1 - bx), 16), rows(r2, 16, 16), 4, dev_x)]
        if j == 3:
            return [remote(done(p_last, 16), done(p_last, 16), 5, dev_y), remote(done(q_last, 16), done(q_last, 16), 6, dev_x)]
        if j == 4:
            return [remote(done(p_mine, 32), done(p_mine, 32), 7, dev_x), remote(done(q_mine, 32), done(q_mine, 32), 8, dev_y)]
        return [remote(done(half, 128), done(half, 128), 9, core)]

    def add_rows(dst, where, u, start, size, src, src_start):
        at = pl.ds(pl.multiple_of(start, 16), size)
        dst[where, at, :] = acc[u, at, :] + src[u, pl.ds(src_start, size), :]

    def stage(u, j, first=None):
        first = u < TAPS if first is None else first
        result, tap = result_of(u, first)
        direct = isinstance(u, int) and u >= DIRECT
        with jax.named_scope(f"p_w{j}_{u}" if isinstance(u, int) else f"p_w{j}_dyn"):
            for c in unit_copies(u, {7: 0, 8: 7, 9: 8}.get(j, j - 1), first):
                c.wait_recv()
        half = 128 * row
        if j in (1, 7):
            add_rows(acc, u, u, half, 128, r0, 0)
        elif j == 2:
            add_rows(acc, u, u, half + 32 * bx, 32, r1, 0)
            add_rows(acc, u, u, half + 64 + 32 * by, 32, r1, 32)
        elif j == 3:
            add_rows(result, tap, u, half + 32 * bx + 16 * by, 16, r2, 0)
            add_rows(result, tap, u, half + 64 + 32 * by + 16 * bx, 16, r2, 16)
        elif j == 8:
            at = pl.ds(pl.multiple_of(half + 32 * col, 16), 32)
            result[tap, at, :] = (acc[u, at, :] + r1[u, 0:32, :]) + (r1[u, 32:64, :] + r2[u, 0:32, :])
        if j == 6:
            for k in (0, 7, 8, 5) if direct else range(6):
                for c in unit_copies(u, k, first):
                    c.wait_send()
        else:
            for c in unit_copies(u, {9: 5}.get(j, j), first):
                c.start()

    def run(plan):
        for j, u in plan:
            stage(u, j)

    def run_at(i, plans):
        for k, plan in enumerate(plans):
            @pl.when(i == k)
            def _(plan=plan):
                run(plan)

    def send_first(u):
        for c in unit_copies(u, 0, True):
            c.start()

    def tap_sum(lhs_t, plane, tap_row, fill=(), before=None):
        total = None
        blocks = SPAN // CH
        for q in range(CHUNKS):
            rhs = plane[pl.ds(2 - tap_row + STEP * q, STEP)].reshape(SPAN, CH)
            for m in range(blocks):
                for piece in fill[blocks * q + m::CHUNKS * blocks]:
                    piece()
                if before is not None and before[blocks * q + m] is not None:
                    before[blocks * q + m]()
                part = jnp.dot(lhs_t[blocks * q + m], rhs[CH * m:CH * (m + 1)], preferred_element_type=F32)
                total = part if total is None else total + part
        return total

    def tap_pair(lhs_t, pair, tap_row):
        totals = [None, None]
        blocks = SPAN // CH
        for q in range(CHUNKS):
            for m in range(blocks):
                for n in range(2):
                    rhs = pair[n][pl.ds(2 - tap_row + STEP * q, STEP)].reshape(SPAN, CH)[CH * m:CH * (m + 1)]
                    part = jnp.dot(lhs_t[blocks * q + m], rhs, preferred_element_type=F32)
                    totals[n] = part if totals[n] is None else totals[n] + part
        return totals

    def shift_row(center, minus, plus, r, lh=None, rh=None):
        v = center[r]
        first = v[:1] if lh is None else lh[pl.ds(r + 7, 1), :].astype(BF16)
        last = v[:1] if rh is None else rh[pl.ds(r + 7, 1), :].astype(BF16)
        minus[r] = jnp.concatenate([first, v[:COLS - 1]], axis=0)
        plus[r] = jnp.concatenate([v[1:], last], axis=0)

    def mend_row(minus, plus, r, lh, rh):
        at = lax.broadcasted_iota(jnp.int32, (8, CH), 0)
        minus[r, 0:8] = jnp.where(at == 0, lh[pl.ds(r + 7, 1), :], minus[r, 0:8].astype(F32)).astype(BF16)
        plus[r, COLS - 8:COLS] = jnp.where(at == 7, rh[pl.ds(r + 7, 1), :], plus[r, COLS - 8:COLS].astype(F32)).astype(BF16)

    def conv_pair(planes, w, i, fill=()):
        totals = [None, None]
        for k in range(TAPS):
            for n in range(2):
                lhs = planes[k % 3][pl.ds(STEP * (2 * i + n) + 2 - k // 3, STEP)].reshape(SPAN, CH)
                part = lax.dot_general(lhs, w[k], (((1,), (1,)), ((), ())), preferred_element_type=F32)
                totals[n] = part if k == 0 else totals[n] + part
            for piece in fill[len(fill) * k // TAPS:len(fill) * (k + 1) // TAPS]:
                piece()
        return totals

    def z_pieces(i):
        def one(m):
            for half in range(2):
                at = CH * m + 128 * half
                z = jax.nn.gelu(av[pl.ds(STEP * i, STEP)].reshape(SPAN, CH)[at:at + 128].astype(F32), approximate=True).astype(BF16)
                zt[SPAN // CH * i + m, :, 128 * half:128 * half + 128] = z.T

        return [functools.partial(one, m) for m in range(SPAN // CH)]

    def z_chunk(i):
        z = jax.nn.gelu(av[pl.ds(STEP * i, STEP)].reshape(SPAN, CH).astype(F32), approximate=True).astype(BF16)
        for m in range(SPAN // CH):
            zt[SPAN // CH * i + m] = z[CH * m:CH * (m + 1)].T

    def x_chunk(i):
        x = d1[pl.ds(1 + STEP * i, STEP)].reshape(SPAN, CH)
        for m in range(SPAN // CH):
            xt[SPAN // CH * i + m] = x[CH * m:CH * (m + 1)].T

    def z_loop(lo, hi):
        lax.fori_loop(lo, hi, lambda i, c: (z_chunk(i), c)[1], 0)

    scope = mark(scope, "p_z1")
    a_copies[0].wait()
    z_loop(0, 3)
    scope = mark(scope, "p_gwait")
    g_copy.wait()

    def g_edge(i, c):
        for k in range(8):
            r = 8 * i + k
            clg[pl.ds(r, 1), :] = g1[r + 1, 0:8, :].astype(F32)[0:1]
            crg[pl.ds(r, 1), :] = g1[r + 1, COLS - 8:COLS, :].astype(F32)[7:8]
        return c

    lax.fori_loop(0, ROWS // 8, g_edge, 0)
    g_frame = frame_copies(0, g1, clg, crg, lhg, rhg)
    frame_send(g_frame)
    a_copies[1].wait()
    z_loop(3, 6)
    for q in range(2, 4):
        a_copies[q].wait()

    scope = mark(scope, "p_s0")
    acc[0] = tap_sum(zt, g1, 1, before=[piece for i in range(CHUNKS) for piece in (z_pieces(i) if i >= 6 else [None] * 3)])
    send_first(0)
    scope = mark(scope, "p_fwg")
    frame_wait(g_frame)

    scope = mark(scope, "p_mid")
    for i in range(2):
        @pl.when(row >= 0)
        def _(i=i):
            acc[1 + i] = tap_sum(zt, g1, 2 * i, [functools.partial(shift_row, g1, g2, g0, 25 * i + k, lhg, rhg) for k in range(25)])

        send_first(1 + i)
        stage(i, 1)

    x_copy.wait()

    def w2_side(i, c):
        for k in range(4):
            x_chunk(4 * i + k)
        totals = tap_pair(zt, (g0, g2), i)
        acc[3 + 2 * i] = totals[0]
        acc[4 + 2 * i] = totals[1]
        send_first(3 + 2 * i)
        send_first(4 + 2 * i)
        run_at(i, W2_PLAN)
        return c

    lax.fori_loop(0, 3, w2_side, 0)

    w2_copy.wait()
    g_planes = (g0, g1, g2)

    def da_chunk(i, dz):
        part = COLS // PARTS

        def one(k, third):
            r, at = STEP * i + k, part * third
            a_val = av[r, at:at + part].astype(F32)
            d_a = (dz[COLS * k + at:COLS * k + at + part] * gelu_slope(a_val)).astype(BF16)
            d1[1 + r, at:at + part] = d_a
            if third == 0:
                cld[pl.ds(r, 1), :] = d_a[0:8].astype(F32)[0:1]
            if third == PARTS - 1:
                crd[pl.ds(r, 1), :] = d_a[part - 8:].astype(F32)[7:8]

        pieces = []
        for k in range(STEP):
            pieces += [functools.partial(one, k, third) for third in range(PARTS)]
            pieces.append(functools.partial(shift_row, d1, d2, d0, 1 + STEP * i + k))
        return pieces

    dza, dzb = dzs.at[0], dzs.at[1]

    def dz_store(pair):
        dza[...], dzb[...] = pair

    def dz_step(i, c):
        dz_store(conv_pair(g_planes, w2, i, da_chunk(2 * i - 2, dza) + da_chunk(2 * i - 1, dzb)))
        run_at(i - 1, DZ_PLAN[1:])
        return c

    scope = mark(scope, "p_dz0")
    dz_store(conv_pair(g_planes, w2, 0))
    run(DZ_PLAN[0])
    scope = mark(scope, "p_dz")
    lax.fori_loop(1, CHUNKS // 2, dz_step, 0)

    d_frame = frame_copies(1, d1, cld, crd, lhd, rhd)
    def da_last(i, c):
        for piece in da_chunk(CHUNKS - 2 + i, dzs.at[i]):
            piece()
        return c

    scope = mark(scope, "p_dal")
    lax.fori_loop(0, 2, da_last, 0)
    frame_send(d_frame)
    scope = mark(scope, "p_s9")
    acc[9] = tap_sum(xt, d1, 1)
    send_first(9)
    scope = mark(scope, "p_s9plan")
    run(W1_PLAN[0])
    scope = mark(scope, "p_fwd0")
    d_frame[0].wait_recv()

    @pl.when(row >= 0)
    def _():
        acc[10] = tap_sum(xt, d1, 0)

    send_first(10)
    run(W1_PLAN[1])

    @pl.when(row >= 0)
    def _():
        acc[11] = tap_sum(xt, d1, 2)

    send_first(11)
    run(W1_PLAN[2])
    scope = mark(scope, "p_fwd1")
    frame_wait(d_frame, True)
    scope = mark(scope, "p_mend")
    shift_row(d1, d2, d0, 0, lhd, rhd)
    shift_row(d1, d2, d0, ROWS + 1, lhd, rhd)

    def mend(i, c):
        for k in range(8):
            mend_row(d2, d0, 1 + 8 * i + k, lhd, rhd)
        return c

    lax.fori_loop(0, ROWS // 8, mend, 0)

    w1_copy.wait()
    d_planes = (d0, d1, d2)

    def dx_pair(i):
        for n, total in enumerate(conv_pair(d_planes, w1, i)):
            at = STEP * (2 * i + n)
            total = total + g1[pl.ds(1 + at, STEP)].reshape(SPAN, CH).astype(F32)
            av[pl.ds(at, STEP)] = total.astype(BF16).reshape(STEP, COLS, CH)

    @pl.when(row >= 0)
    def _():
        dx_pair(0)

    run(W1_PLAN[3])

    def w1_left(i, c):
        with jax.named_scope("p_tap"):
            acc[12 + i] = tap_sum(xt, d0, i)
        send_first(12 + i)
        run_at(i, W1_PLAN[4:7])
        return c

    def w1_right(i, c):
        with jax.named_scope("p_tap"):
            acc[15 + i] = tap_sum(xt, d2, i)
        send_first(15 + i)
        run_at(i, W1_PLAN[7:10])
        return c

    scope = mark(scope, "p_w1l")
    lax.fori_loop(0, 3, w1_left, 0)
    scope = mark(scope, "p_w1r")
    lax.fori_loop(0, 3, w1_right, 0)

    def dx_step(i, c):
        with jax.named_scope("p_dxc"):
            dx_pair(i)
        run_at(i - 1, DX_PLAN[:CHUNKS // 2 - 1])
        return c

    lax.fori_loop(1, CHUNKS // 2, dx_step, 0)
    run(DX_PLAN[CHUNKS // 2 - 1])

    scope = mark(scope, "p_done")
    frame_done(g_frame)
    frame_done(d_frame)
    mark(scope, None)

def write_out(*refs):
    sem = refs[-1]
    copies = [pltpu.make_async_copy(src, dst, sem.at[k]) for k, (src, dst) in enumerate(zip(refs[:3], refs[3:6]))]
    for c in copies:
        c.start()
    for c in copies:
        c.wait()


def solution(mesh):
    n_row, n_col = mesh.shape["row"], mesh.shape["col"]

    def local_step(x_tile, a_tile, g_tile, w_one, w_two):
        units = 2 * TAPS
        hbm = pl.BlockSpec(memory_space=pl.ANY)
        frame = pltpu.VMEM((64, CH), F32)
        edge = pltpu.VMEM((ROWS, CH), F32)
        d_x, d_w1, d_w2 = pl.pallas_call(
            functools.partial(kernel, n_row, n_col),
            out_shape=(
                pltpu.VMEM((ROWS, COLS, CH), BF16),
                pltpu.VMEM((TAPS, CH, CH), F32),
                pltpu.VMEM((TAPS, CH, CH), F32),
            ),
            in_specs=[hbm] * 5,
            out_specs=(pl.BlockSpec(memory_space=pltpu.VMEM),) * 3,
            scratch_shapes=[
                pltpu.VMEM((6, ROWS + 2, COLS, CH), BF16),
                pltpu.VMEM((PIX // CH, CH, CH), BF16),
                pltpu.VMEM((PIX // CH, CH, CH), BF16),
                pltpu.VMEM((TAPS, CH, CH), BF16),
                pltpu.VMEM((TAPS, CH, CH), BF16),
                pltpu.VMEM((units, CH, CH), F32),
                pltpu.VMEM((units, 128, CH), F32),
                pltpu.VMEM((units, 64, CH), F32),
                pltpu.VMEM((units, 32, CH), F32),
                pltpu.VMEM((2, SPAN, CH), F32),
                frame, frame, frame, frame,
                edge, edge, edge, edge,
                pltpu.SemaphoreType.DMA((8,)),
                pltpu.SemaphoreType.DMA((2, 5)),
                pltpu.SemaphoreType.DMA((2, 5)),
                pltpu.SemaphoreType.DMA((units, 10)),
                pltpu.SemaphoreType.DMA((units, 10)),
            ],
            compiler_params=pltpu.CompilerParams(collective_id=0, has_side_effects=True, vmem_limit_bytes=VMEM_LIMIT),
        )(x_tile[0], a_tile[0], g_tile[0], w_one.reshape(TAPS, CH, CH), w_two.reshape(TAPS, CH, CH))
        held = [pltpu.with_memory_space_constraint(r, pltpu.VMEM) for r in (d_x, d_w1, d_w2)]
        d_x, d_w1, d_w2 = pl.pallas_call(
            write_out,
            out_shape=tuple(jax.ShapeDtypeStruct(r.shape, r.dtype) for r in (d_x, d_w1, d_w2)),
            in_specs=[pl.BlockSpec(memory_space=pltpu.VMEM)] * 3,
            out_specs=(hbm,) * 3,
            scratch_shapes=[pltpu.SemaphoreType.DMA((3,))],
            compiler_params=pltpu.CompilerParams(vmem_limit_bytes=2**20),
        )(*held)
        shape = (3, 3, CH, CH)
        return d_x[None], d_w1.reshape(shape), d_w2.reshape(shape)

    tile_spec = P(None, "row", "col", None)
    return jax.shard_map(local_step, mesh=mesh, in_specs=(tile_spec, tile_spec, tile_spec, P(), P()), out_specs=(tile_spec, P(), P()), check_vma=False)
```

```python
import functools

import jax
import jax.numpy as jnp
from jax import lax
from jax.experimental import pallas as pl
from jax.experimental.pallas import tpu as pltpu
from jax.sharding import PartitionSpec as P

MESH = pl.DeviceIdType.MESH
F32 = jnp.float32
BF16 = jnp.bfloat16
CH = 256
ROWS = 48
COLS = 192
PIX = ROWS * COLS
VMEM_LIMIT = 56000 * 2**10
PARTS = 12
STEP = 4
SPAN = STEP * COLS
CHUNKS = ROWS // STEP
TAPS = 9
TAP_ORDER = ((1, 1), (0, 1), (2, 1), (0, 0), (1, 0), (2, 0), (0, 2), (1, 2), (2, 2))
TAP_ORDER_TWO = ((1, 1), (0, 1), (2, 1), (0, 0), (0, 2), (1, 0), (1, 2), (2, 0), (2, 2))
W2_PLAN = (
    ((2, 0), (1, 2)),
    ((2, 1), (1, 3), (1, 4)),
    ((2, 2), (3, 0), (1, 5), (1, 6)),
)
DZ_PLAN = (
    ((2, 3), (3, 1), (1, 7), (1, 8)),
    ((2, 4), (2, 5), (3, 2), (4, 0)),
    ((2, 6), (3, 3), (4, 1), (2, 7)),
    ((2, 8), (3, 4), (3, 5), (4, 2), (5, 0)),
    ((3, 6), (3, 7), (4, 3), (5, 1)),
    ((4, 4), (4, 5), (5, 2), (3, 8)),
)
W1_PLAN = (
    ((4, 6), (4, 7), (5, 3), (5, 4)),
    ((1, 9), (4, 8), (5, 5)),
    ((1, 10), (5, 6)),
    ((1, 11), (2, 9), (2, 10), (5, 7), (5, 8)),
    ((6, 0), (6, 1), (6, 2), (6, 3)),
    ((2, 11), (1, 12), (3, 9), (6, 4), (6, 5)),
    ((3, 10), (1, 13), (6, 6), (6, 7)),
    ((3, 11), (2, 12), (1, 14), (4, 9), (6, 8)),
    ((2, 13), (1, 15), (4, 10)),
    ((3, 12), (2, 14), (7, 16), (4, 11)),
)
DX_PLAN = (
    ((3, 13), (2, 15), (7, 17), (5, 9)),
    ((3, 14), (4, 12), (8, 16), (5, 10), (3, 15), (5, 11), (6, 9)),
    ((4, 13), (8, 17), (6, 10)),
    ((4, 14), (4, 15), (5, 12), (6, 11)),
    ((5, 13), (9, 16), (9, 17), (6, 12)),
    ((5, 14), (5, 15), (6, 13), (6, 16), (6, 17), (6, 14), (6, 15)),
)
DIRECT = 16


def gelu_slope(a):
    scale = 0.7978845608028654
    square = (scale * 0.044715 * a) * a
    tanh_val = jnp.tanh(a * (scale + square))
    return (0.5 + 0.5 * tanh_val) + (0.5 * a * (1.0 - tanh_val * tanh_val)) * (scale + 3.0 * square)


def kernel(n_row, n_col, x_hbm, a_hbm, g_hbm, w1_hbm, w2_hbm, av, dw1, dw2,
           planes, zt, xt, w1, w2, acc, r0, r1, r2, dzs,
           lhg, rhg, lhd, rhd, clg, crg, cld, crd,
           in_sem, hs_sem, hr_sem, as_sem, ar_sem):
    row = lax.axis_index("row")
    col = lax.axis_index("col")
    by = jnp.where(col >= 2, 1, 0)
    bx = col - 2 * by
    other = 1 - row
    g0, g1, g2, d0, d1, d2 = (planes.at[k] for k in range(6))
    col_x = col + 1 - 2 * bx
    col_y = col + 2 - 4 * by
    has_left = col > 0
    has_right = col < n_col - 1

    a_copies = [pltpu.make_async_copy(a_hbm.at[pl.ds(12 * q, 12)], av.at[pl.ds(12 * q, 12)], in_sem.at[q]) for q in range(4)]
    g_copy = pltpu.make_async_copy(g_hbm, g1.at[pl.ds(1, ROWS)], in_sem.at[4])
    x_copy = pltpu.make_async_copy(x_hbm, d1.at[pl.ds(1, ROWS)], in_sem.at[5])
    w2_copy = pltpu.make_async_copy(w2_hbm, w2, in_sem.at[6])
    w1_copy = pltpu.make_async_copy(w1_hbm, w1, in_sem.at[7])
    a_copies[0].start()
    g_copy.start()
    for q in range(1, 4):
        a_copies[q].start()
    x_copy.start()
    w2_copy.start()
    w1_copy.start()

    for buf in (lhg, rhg, lhd, rhd):
        buf[...] = jnp.zeros_like(buf)
    for buf in (g1, d1):
        buf[0] = jnp.zeros((COLS, CH), BF16)
        buf[ROWS + 1] = jnp.zeros((COLS, CH), BF16)

    barrier = pltpu.get_barrier_semaphore()
    for dc in range(n_col):
        for dr in range(n_row):
            if dc or dr:
                pl.semaphore_signal(barrier, inc=1, device_id={"col": lax.rem(col + dc, n_col), "row": lax.rem(row + dr, n_row)}, device_id_type=MESH)
    pl.semaphore_wait(barrier, n_col * n_row - 1)

    def frame_copies(which, plane, cl, cr, lh, rh):
        def remote(src, dst, k, dev):
            return pltpu.make_async_remote_copy(src_ref=src, dst_ref=dst, send_sem=hs_sem.at[which, k], recv_sem=hr_sem.at[which, k], device_id=dev, device_id_type=MESH)

        left = jnp.maximum(col - 1, 0)
        right = jnp.minimum(col + 1, n_col - 1)
        src8 = pl.multiple_of(40 * other, 8)
        dst8 = pl.multiple_of(56 * row, 8)
        pair = remote(plane.at[ROWS - (ROWS - 1) * row], plane.at[(ROWS + 1) * row], 0, {"col": col, "row": other})
        to_left = [remote(cl, rh.at[pl.ds(8, ROWS)], 1, {"col": left, "row": row}), remote(cl.at[pl.ds(src8, 8)], rh.at[pl.ds(dst8, 8)], 2, {"col": left, "row": other})]
        to_right = [remote(cr, lh.at[pl.ds(8, ROWS)], 3, {"col": right, "row": row}), remote(cr.at[pl.ds(src8, 8)], lh.at[pl.ds(dst8, 8)], 4, {"col": right, "row": other})]
        return pair, to_left, to_right

    def frame_send(copies):
        pair, to_left, to_right = copies
        pair.start()

        @pl.when(has_left)
        def _():
            for c in to_left:
                c.start()

        @pl.when(has_right)
        def _():
            for c in to_right:
                c.start()

    def frame_wait(copies, columns_only=False):
        pair, to_left, to_right = copies
        if not columns_only:
            pair.wait_recv()

        @pl.when(has_right)
        def _():
            for c in to_left:
                c.wait_recv()

        @pl.when(has_left)
        def _():
            for c in to_right:
                c.wait_recv()

    def frame_done(copies):
        pair, to_left, to_right = copies
        pair.wait_send()

        @pl.when(has_left)
        def _():
            for c in to_left:
                c.wait_send()

        @pl.when(has_right)
        def _():
            for c in to_right:
                c.wait_send()

    def result_of(u, first):
        tap_row, tap_col = (TAP_ORDER_TWO if first else TAP_ORDER)[u % TAPS]
        return dw2 if first else dw1, 3 * tap_row + tap_col

    def unit_copies(u, j, first):
        half = 128 * row
        p_base, q_base = half, half + 64
        p_mine, q_mine = p_base + 32 * bx, q_base + 32 * by
        p_last, q_last = p_mine + 16 * by, q_mine + 16 * bx

        result, tap = result_of(u, first) if j else (None, None)

        def rows(ref, start, size):
            return ref.at[u, pl.ds(pl.multiple_of(start, 16), size)]

        def done(start, size):
            return result.at[tap, pl.ds(pl.multiple_of(start, 16), size)]

        def remote(src, dst, k, dev):
            return pltpu.make_async_remote_copy(src_ref=src, dst_ref=dst, send_sem=as_sem.at[u, k], recv_sem=ar_sem.at[u, k], device_id=dev, device_id_type=MESH)

        core = {"col": col, "row": other}
        dev_x = {"col": col_x, "row": row}
        dev_y = {"col": col_y, "row": row}
        if j == 0:
            return [remote(rows(acc, 128 * other, 128), r0.at[u], 0, core)]
        if j in (7, 8):
            mine = half + 32 * col
            peers = ((col_x, rows(r1, 0, 32)), (col_y, rows(r1, 32, 32)), (3 - col, rows(r2, 0, 32)))
            if j == 7:
                return [remote(rows(acc, half + 32 * peer, 32), slot, 1 + k, {"col": peer, "row": row}) for k, (peer, slot) in enumerate(peers)]
            return [remote(done(mine, 32), done(mine, 32), 4 + k, {"col": peer, "row": row}) for k, (peer, _) in enumerate(peers)]
        if j == 1:
            return [remote(rows(acc, p_base + 32 * (1 - bx), 32), rows(r1, 0, 32), 1, dev_x), remote(rows(acc, q_base + 32 * (1 - by), 32), rows(r1, 32, 32), 2, dev_y)]
        if j == 2:
            return [remote(rows(acc, p_mine + 16 * (1 - by), 16), rows(r2, 0, 16), 3, dev_y), remote(rows(acc, q_mine + 16 * (1 - bx), 16), rows(r2, 16, 16), 4, dev_x)]
        if j == 3:
            return [remote(done(p_last, 16), done(p_last, 16), 5, dev_y), remote(done(q_last, 16), done(q_last, 16), 6, dev_x)]
        if j == 4:
            return [remote(done(p_mine, 32), done(p_mine, 32), 7, dev_x), remote(done(q_mine, 32), done(q_mine, 32), 8, dev_y)]
        return [remote(done(half, 128), done(half, 128), 9, core)]

    def add_rows(dst, where, u, start, size, src, src_start):
        at = pl.ds(pl.multiple_of(start, 16), size)
        dst[where, at, :] = acc[u, at, :] + src[u, pl.ds(src_start, size), :]

    def stage(u, j, first=None):
        first = u < TAPS if first is None else first
        result, tap = result_of(u, first)
        direct = isinstance(u, int) and u >= DIRECT
        for c in unit_copies(u, {7: 0, 8: 7, 9: 8}.get(j, j - 1), first):
            c.wait_recv()
        half = 128 * row
        if j in (1, 7):
            add_rows(acc, u, u, half, 128, r0, 0)
        elif j == 2:
            add_rows(acc, u, u, half + 32 * bx, 32, r1, 0)
            add_rows(acc, u, u, half + 64 + 32 * by, 32, r1, 32)
        elif j == 3:
            add_rows(result, tap, u, half + 32 * bx + 16 * by, 16, r2, 0)
            add_rows(result, tap, u, half + 64 + 32 * by + 16 * bx, 16, r2, 16)
        elif j == 8:
            at = pl.ds(pl.multiple_of(half + 32 * col, 16), 32)
            result[tap, at, :] = (acc[u, at, :] + r1[u, 0:32, :]) + (r1[u, 32:64, :] + r2[u, 0:32, :])
        if j == 6:
            for k in (0, 7, 8, 5) if direct else range(6):
                for c in unit_copies(u, k, first):
                    c.wait_send()
        else:
            for c in unit_copies(u, {9: 5}.get(j, j), first):
                c.start()

    def run(plan):
        for j, u in plan:
            stage(u, j)

    def run_at(i, plans):
        for k, plan in enumerate(plans):
            @pl.when(i == k)
            def _(plan=plan):
                run(plan)

    def send_first(u):
        for c in unit_copies(u, 0, True):
            c.start()

    def tap_sum(lhs_t, plane, tap_row, fill=(), before=None):
        total = None
        blocks = SPAN // CH
        for q in range(CHUNKS):
            rhs = plane[pl.ds(2 - tap_row + STEP * q, STEP)].reshape(SPAN, CH)
            for m in range(blocks):
                for piece in fill[blocks * q + m::CHUNKS * blocks]:
                    piece()
                if before is not None and before[blocks * q + m] is not None:
                    before[blocks * q + m]()
                part = jnp.dot(lhs_t[blocks * q + m], rhs[CH * m:CH * (m + 1)], preferred_element_type=F32)
                total = part if total is None else total + part
        return total

    def tap_pair(lhs_t, pair, tap_row):
        totals = [None, None]
        blocks = SPAN // CH
        for q in range(CHUNKS):
            for m in range(blocks):
                for n in range(2):
                    rhs = pair[n][pl.ds(2 - tap_row + STEP * q, STEP)].reshape(SPAN, CH)[CH * m:CH * (m + 1)]
                    part = jnp.dot(lhs_t[blocks * q + m], rhs, preferred_element_type=F32)
                    totals[n] = part if totals[n] is None else totals[n] + part
        return totals

    def shift_row(center, minus, plus, r, lh=None, rh=None):
        v = center[r]
        first = v[:1] if lh is None else lh[pl.ds(r + 7, 1), :].astype(BF16)
        last = v[:1] if rh is None else rh[pl.ds(r + 7, 1), :].astype(BF16)
        minus[r] = jnp.concatenate([first, v[:COLS - 1]], axis=0)
        plus[r] = jnp.concatenate([v[1:], last], axis=0)

    def mend_row(minus, plus, r, lh, rh):
        at = lax.broadcasted_iota(jnp.int32, (8, CH), 0)
        minus[r, 0:8] = jnp.where(at == 0, lh[pl.ds(r + 7, 1), :], minus[r, 0:8].astype(F32)).astype(BF16)
        plus[r, COLS - 8:COLS] = jnp.where(at == 7, rh[pl.ds(r + 7, 1), :], plus[r, COLS - 8:COLS].astype(F32)).astype(BF16)

    def conv_pair(planes, w, i, fill=()):
        totals = [None, None]
        for k in range(TAPS):
            for n in range(2):
                lhs = planes[k % 3][pl.ds(STEP * (2 * i + n) + 2 - k // 3, STEP)].reshape(SPAN, CH)
                part = lax.dot_general(lhs, w[k], (((1,), (1,)), ((), ())), preferred_element_type=F32)
                totals[n] = part if k == 0 else totals[n] + part
            for piece in fill[len(fill) * k // TAPS:len(fill) * (k + 1) // TAPS]:
                piece()
        return totals

    def z_pieces(i):
        def one(m):
            for half in range(2):
                at = CH * m + 128 * half
                z = jax.nn.gelu(av[pl.ds(STEP * i, STEP)].reshape(SPAN, CH)[at:at + 128].astype(F32), approximate=True).astype(BF16)
                zt[SPAN // CH * i + m, :, 128 * half:128 * half + 128] = z.T

        return [functools.partial(one, m) for m in range(SPAN // CH)]

    def z_chunk(i):
        z = jax.nn.gelu(av[pl.ds(STEP * i, STEP)].reshape(SPAN, CH).astype(F32), approximate=True).astype(BF16)
        for m in range(SPAN // CH):
            zt[SPAN // CH * i + m] = z[CH * m:CH * (m + 1)].T

    def x_chunk(i):
        x = d1[pl.ds(1 + STEP * i, STEP)].reshape(SPAN, CH)
        for m in range(SPAN // CH):
            xt[SPAN // CH * i + m] = x[CH * m:CH * (m + 1)].T

    def z_loop(lo, hi):
        lax.fori_loop(lo, hi, lambda i, c: (z_chunk(i), c)[1], 0)

    a_copies[0].wait()
    z_loop(0, 3)
    g_copy.wait()

    def g_edge(i, c):
        for k in range(8):
            r = 8 * i + k
            clg[pl.ds(r, 1), :] = g1[r + 1, 0:8, :].astype(F32)[0:1]
            crg[pl.ds(r, 1), :] = g1[r + 1, COLS - 8:COLS, :].astype(F32)[7:8]
        return c

    lax.fori_loop(0, ROWS // 8, g_edge, 0)
    g_frame = frame_copies(0, g1, clg, crg, lhg, rhg)
    frame_send(g_frame)
    a_copies[1].wait()
    z_loop(3, 6)
    for q in range(2, 4):
        a_copies[q].wait()

    acc[0] = tap_sum(zt, g1, 1, before=[piece for i in range(CHUNKS) for piece in (z_pieces(i) if i >= 6 else [None] * 3)])
    send_first(0)
    frame_wait(g_frame)

    for i in range(2):
        @pl.when(row >= 0)
        def _(i=i):
            acc[1 + i] = tap_sum(zt, g1, 2 * i, [functools.partial(shift_row, g1, g2, g0, 25 * i + k, lhg, rhg) for k in range(25)])

        send_first(1 + i)
        stage(i, 1)

    x_copy.wait()

    def w2_side(i, c):
        for k in range(4):
            x_chunk(4 * i + k)
        totals = tap_pair(zt, (g0, g2), i)
        acc[3 + 2 * i] = totals[0]
        acc[4 + 2 * i] = totals[1]
        send_first(3 + 2 * i)
        send_first(4 + 2 * i)
        run_at(i, W2_PLAN)
        return c

    lax.fori_loop(0, 3, w2_side, 0)

    w2_copy.wait()
    g_planes = (g0, g1, g2)

    def da_chunk(i, dz):
        part = COLS // PARTS

        def one(k, third):
            r, at = STEP * i + k, part * third
            a_val = av[r, at:at + part].astype(F32)
            d_a = (dz[COLS * k + at:COLS * k + at + part] * gelu_slope(a_val)).astype(BF16)
            d1[1 + r, at:at + part] = d_a
            if third == 0:
                cld[pl.ds(r, 1), :] = d_a[0:8].astype(F32)[0:1]
            if third == PARTS - 1:
                crd[pl.ds(r, 1), :] = d_a[part - 8:].astype(F32)[7:8]

        pieces = []
        for k in range(STEP):
            pieces += [functools.partial(one, k, third) for third in range(PARTS)]
            pieces.append(functools.partial(shift_row, d1, d2, d0, 1 + STEP * i + k))
        return pieces

    dza, dzb = dzs.at[0], dzs.at[1]

    def dz_store(pair):
        dza[...], dzb[...] = pair

    def dz_step(i, c):
        dz_store(conv_pair(g_planes, w2, i, da_chunk(2 * i - 2, dza) + da_chunk(2 * i - 1, dzb)))
        run_at(i - 1, DZ_PLAN[1:])
        return c

    dz_store(conv_pair(g_planes, w2, 0))
    run(DZ_PLAN[0])
    lax.fori_loop(1, CHUNKS // 2, dz_step, 0)

    d_frame = frame_copies(1, d1, cld, crd, lhd, rhd)
    def da_last(i, c):
        for piece in da_chunk(CHUNKS - 2 + i, dzs.at[i]):
            piece()
        return c

    lax.fori_loop(0, 2, da_last, 0)
    frame_send(d_frame)
    acc[9] = tap_sum(xt, d1, 1)
    send_first(9)
    run(W1_PLAN[0])
    d_frame[0].wait_recv()

    @pl.when(row >= 0)
    def _():
        acc[10] = tap_sum(xt, d1, 0)

    send_first(10)
    run(W1_PLAN[1])

    @pl.when(row >= 0)
    def _():
        acc[11] = tap_sum(xt, d1, 2)

    send_first(11)
    run(W1_PLAN[2])
    frame_wait(d_frame, True)
    shift_row(d1, d2, d0, 0, lhd, rhd)
    shift_row(d1, d2, d0, ROWS + 1, lhd, rhd)

    def mend(i, c):
        for k in range(8):
            mend_row(d2, d0, 1 + 8 * i + k, lhd, rhd)
        return c

    lax.fori_loop(0, ROWS // 8, mend, 0)

    w1_copy.wait()
    d_planes = (d0, d1, d2)

    def dx_pair(i):
        for n, total in enumerate(conv_pair(d_planes, w1, i)):
            at = STEP * (2 * i + n)
            total = total + g1[pl.ds(1 + at, STEP)].reshape(SPAN, CH).astype(F32)
            av[pl.ds(at, STEP)] = total.astype(BF16).reshape(STEP, COLS, CH)

    @pl.when(row >= 0)
    def _():
        dx_pair(0)

    run(W1_PLAN[3])

    def w1_left(i, c):
        acc[12 + i] = tap_sum(xt, d0, i)
        send_first(12 + i)
        run_at(i, W1_PLAN[4:7])
        return c

    def w1_right(i, c):
        acc[15 + i] = tap_sum(xt, d2, i)
        send_first(15 + i)
        run_at(i, W1_PLAN[7:10])
        return c

    lax.fori_loop(0, 3, w1_left, 0)
    lax.fori_loop(0, 3, w1_right, 0)

    def dx_step(i, c):
        dx_pair(i)
        run_at(i - 1, DX_PLAN[:CHUNKS // 2 - 1])
        return c

    lax.fori_loop(1, CHUNKS // 2, dx_step, 0)
    run(DX_PLAN[CHUNKS // 2 - 1])

    frame_done(g_frame)
    frame_done(d_frame)

def write_out(*refs):
    sem = refs[-1]
    copies = [pltpu.make_async_copy(src, dst, sem.at[k]) for k, (src, dst) in enumerate(zip(refs[:3], refs[3:6]))]
    for c in copies:
        c.start()
    for c in copies:
        c.wait()


def solution(mesh):
    n_row, n_col = mesh.shape["row"], mesh.shape["col"]

    def local_step(x_tile, a_tile, g_tile, w_one, w_two):
        units = 2 * TAPS
        hbm = pl.BlockSpec(memory_space=pl.ANY)
        frame = pltpu.VMEM((64, CH), F32)
        edge = pltpu.VMEM((ROWS, CH), F32)
        d_x, d_w1, d_w2 = pl.pallas_call(
            functools.partial(kernel, n_row, n_col),
            out_shape=(
                pltpu.VMEM((ROWS, COLS, CH), BF16),
                pltpu.VMEM((TAPS, CH, CH), F32),
                pltpu.VMEM((TAPS, CH, CH), F32),
            ),
            in_specs=[hbm] * 5,
            out_specs=(pl.BlockSpec(memory_space=pltpu.VMEM),) * 3,
            scratch_shapes=[
                pltpu.VMEM((6, ROWS + 2, COLS, CH), BF16),
                pltpu.VMEM((PIX // CH, CH, CH), BF16),
                pltpu.VMEM((PIX // CH, CH, CH), BF16),
                pltpu.VMEM((TAPS, CH, CH), BF16),
                pltpu.VMEM((TAPS, CH, CH), BF16),
                pltpu.VMEM((units, CH, CH), F32),
                pltpu.VMEM((units, 128, CH), F32),
                pltpu.VMEM((units, 64, CH), F32),
                pltpu.VMEM((units, 32, CH), F32),
                pltpu.VMEM((2, SPAN, CH), F32),
                frame, frame, frame, frame,
                edge, edge, edge, edge,
                pltpu.SemaphoreType.DMA((8,)),
                pltpu.SemaphoreType.DMA((2, 5)),
                pltpu.SemaphoreType.DMA((2, 5)),
                pltpu.SemaphoreType.DMA((units, 10)),
                pltpu.SemaphoreType.DMA((units, 10)),
            ],
            compiler_params=pltpu.CompilerParams(collective_id=0, has_side_effects=True, vmem_limit_bytes=VMEM_LIMIT),
        )(x_tile[0], a_tile[0], g_tile[0], w_one.reshape(TAPS, CH, CH), w_two.reshape(TAPS, CH, CH))
        held = [pltpu.with_memory_space_constraint(r, pltpu.VMEM) for r in (d_x, d_w1, d_w2)]
        d_x, d_w1, d_w2 = pl.pallas_call(
            write_out,
            out_shape=tuple(jax.ShapeDtypeStruct(r.shape, r.dtype) for r in (d_x, d_w1, d_w2)),
            in_specs=[pl.BlockSpec(memory_space=pltpu.VMEM)] * 3,
            out_specs=(hbm,) * 3,
            scratch_shapes=[pltpu.SemaphoreType.DMA((3,))],
            compiler_params=pltpu.CompilerParams(vmem_limit_bytes=2**20),
        )(*held)
        shape = (3, 3, CH, CH)
        return d_x[None], d_w1.reshape(shape), d_w2.reshape(shape)

    tile_spec = P(None, "row", "col", None)
    return jax.shard_map(local_step, mesh=mesh, in_specs=(tile_spec, tile_spec, tile_spec, P(), P()), out_specs=(tile_spec, P(), P()), check_vma=False)
```
